32 devices in a mesh: seq: 16 (over z, y, x), tp: 2 (over core).
Axes of the slice: x: 2, y: 2, z: 4, core: 2. Of those that a mesh axis runs over, the one named last changes fastest.
Arguments:
- latent: bfloat16 [2, 16, 256, 1152], P(None, 'seq', 'tp'), may hold values from -6 to 6
- modulation: float32 [2, 9, 1152], replicated, may hold values from -4 to 4
- qkv_spatial: bfloat16 [3, 1152, 1152], P(None, None, 'tp'), may hold values from -0.1875 to 0.1875
- gain_spatial: float32 [2, 72], replicated, may hold values from 0.5 to 1.7
- out_spatial: bfloat16 [1152, 1152], P('tp'), may hold values from -0.1875 to 0.1875
- qkv_temporal: bfloat16 [3, 1152, 1152], P(None, None, 'tp'), may hold values from -0.1875 to 0.1875
- gain_temporal: float32 [2, 72], replicated, may hold values from 0.5 to 1.7
- out_temporal: bfloat16 [1152, 1152], P('tp'), may hold values from -0.1875 to 0.1875
- fc_in: bfloat16 [1152, 4608], P(None, 'tp'), may hold values from -0.1875 to 0.1875
- fc_out: bfloat16 [4608, 1152], P('tp'), may hold values from -0.09375 to 0.09375
Outputs:
- result: bfloat16 [2, 16, 256, 1152], P(None, 'seq', 'tp')
The draws below stay inside these ranges and needn't reach their ends.
All inputs are finite; a program needn't handle non-finite values.
Results may differ from the reference program's by a relative error of at most 0.017.
Values may be sent and summed in bfloat16 or wider, within the bound.
No kernel may reach another device: no remote copies, remote signals or barrier semaphores. Data moves between devices by JAX's collectives and lax.ppermute only.
A program may use at most 64 MiB of HBM per device.

```python
import math
import jax
import jax.numpy as jnp
from jax import lax

D = 1152
H = 16
FF = 4608
HD = 72
B = 2
P_SIZE = 256
F = 16
N_TP = 2


def steps_of(rng, extent, split, low, top_value):
    def one(dim, shards_of):
        draws = jax.random.uniform(jax.random.fold_in(jax.random.fold_in(rng, 6), dim), (shards_of,), jnp.float32, low / len(split), top_value / len(split))
        return jnp.repeat(jnp.exp(draws), extent[dim] // shards_of).reshape((-1,) + (1,) * (len(extent) - dim - 1))

    loudness = one(*split[0])
    for cut in split[1:]:
        loudness = loudness * one(*cut)
    return loudness


def bell_draw(key, shape, width, reach, cuts=(), held_as=jnp.bfloat16):
    result = width * jax.random.normal(key, shape, jnp.float32)
    if cuts:
        result = result * steps_of(key, shape, cuts, -0.22, 0.18)
    return jnp.clip(result, -reach, reach).astype(held_as)


def setup_inputs(seed: int = 0) -> dict:
    seeds = jax.random.split(jax.random.key(seed), 11)
    return {
        "latent": bell_draw(seeds[0], (B, F, P_SIZE, D), 1.0, 6.0, ((1, 16), (2, 2))),
        "modulation": bell_draw(seeds[1], (B, 9, D), 0.7, 4.0, (), jnp.float32),
        "qkv_spatial": bell_draw(seeds[2], (3, D, D), D ** -0.5, 0.1875, ((2, 2),)),
        "gain_spatial": jnp.clip(jax.random.uniform(seeds[3], (2, HD), jnp.float32, 0.5, 1.7), 0.5, 1.7),
        "out_spatial": bell_draw(seeds[4], (D, D), D ** -0.5, 0.1875, ((0, 2),)),
        "qkv_temporal": bell_draw(seeds[5], (3, D, D), D ** -0.5, 0.1875, ((2, 2),)),
        "gain_temporal": jnp.clip(jax.random.uniform(seeds[6], (2, HD), jnp.float32, 0.5, 1.7), 0.5, 1.7),
        "out_temporal": bell_draw(seeds[7], (D, D), D ** -0.5, 0.1875, ((0, 2),)),
        "fc_in": bell_draw(seeds[8], (D, FF), D ** -0.5, 0.1875, ((1, 2),)),
        "fc_out": bell_draw(seeds[9], (FF, D), FF ** -0.5, 0.09375, ((0, 2),)),
    }


epsilon = 1e-06

def layer_norm(values):
    average = lax.optimization_barrier(jnp.mean(values, axis=-1, keepdims=True))
    centred = values - average
    variance = lax.optimization_barrier(jnp.mean(centred * centred, axis=-1, keepdims=True))
    return centred * lax.rsqrt(variance + epsilon)

def modulated(field, modulation, offset):
    shift_row = modulation[:, offset][:, None, None, :]
    scale_row = modulation[:, offset + 1][:, None, None, :]
    return (layer_norm(field) * (1.0 + scale_row) + shift_row).astype(jnp.bfloat16)

def project_rows(normed, table, gains, head_dim):
    flat = normed.reshape(-1, normed.shape[-1])
    results = []
    for which_part in range(3):
        projected = jnp.dot(flat, table[which_part], preferred_element_type=jnp.float32)
        if which_part < 2:
            shaped = projected.reshape(projected.shape[0], -1, head_dim)
            shaped = shaped * lax.rsqrt(lax.optimization_barrier(jnp.mean(shaped * shaped, axis=-1, keepdims=True)) + epsilon) * gains[which_part]
            projected = shaped.reshape(projected.shape)
        results.append(projected.astype(jnp.bfloat16).reshape(normed.shape[:-1] + (table.shape[-1],)))
    return results

def attend_one(members, head_dim):
    query_rows, key_rows, value_rows = members
    length, feature_width = query_rows.shape
    head_count = feature_width // head_dim
    query_heads = query_rows.astype(jnp.float32).reshape(length, head_count, head_dim)
    key_heads = key_rows.astype(jnp.float32).reshape(length, head_count, head_dim)
    value_heads = value_rows.astype(jnp.float32).reshape(length, head_count, head_dim)
    scores = jnp.einsum('qhe,khe->hqk', query_heads, key_heads) / math.sqrt(head_dim)
    weights = jnp.exp(scores)
    probabilities = (weights / lax.optimization_barrier(jnp.sum(weights, axis=-1, keepdims=True))).astype(jnp.bfloat16)
    probabilities = lax.optimization_barrier(probabilities).astype(jnp.float32)
    mixed_heads = jnp.einsum('hqk,khe->qhe', probabilities, value_heads)
    return mixed_heads.reshape(length, feature_width).astype(jnp.bfloat16)

def grouped_product(left, right):
    flat = left.reshape(-1, left.shape[-1])
    group_width = flat.shape[1] // N_TP
    total = jnp.zeros((flat.shape[0], right.shape[1]), jnp.float32)
    for group_index in range(N_TP):
        lower = group_index * group_width
        piece_sum = jnp.dot(flat[:, lower:lower + group_width], right[lower:lower + group_width], preferred_element_type=jnp.float32)
        rounded = lax.optimization_barrier(piece_sum.astype(jnp.bfloat16))
        total = total + rounded.astype(jnp.float32)
    return total.astype(jnp.bfloat16).reshape(left.shape[:-1] + (right.shape[1],))

def reference(latent, modulation, qkv_spatial, gain_spatial, out_spatial, qkv_temporal, gain_temporal, out_temporal, fc_in, fc_out):
    head_dim = D // H
    batches, frames, patches, feature_width = latent.shape
    running = latent.astype(jnp.float32)
    normed = modulated(running, modulation, 0)
    query_rows, key_rows, value_rows = project_rows(normed, qkv_spatial, gain_spatial, head_dim)
    grouped = tuple((item.reshape(batches * frames, patches, feature_width) for item in (query_rows, key_rows, value_rows)))
    mixed_heads = lax.map(lambda members: attend_one(members, head_dim), grouped).reshape(batches, frames, patches, feature_width)
    spatial_out = grouped_product(mixed_heads, out_spatial)
    running = running + modulation[:, 2][:, None, None, :] * spatial_out.astype(jnp.float32)
    normed = modulated(running, modulation, 3)
    query_rows, key_rows, value_rows = project_rows(normed, qkv_temporal, gain_temporal, head_dim)
    grouped = tuple((item.transpose(0, 2, 1, 3).reshape(batches * patches, frames, feature_width) for item in (query_rows, key_rows, value_rows)))
    mixed_heads = lax.map(lambda members: attend_one(members, head_dim), grouped)
    mixed_heads = mixed_heads.reshape(batches, patches, frames, feature_width).transpose(0, 2, 1, 3)
    temporal_out = grouped_product(mixed_heads, out_temporal)
    running = running + modulation[:, 5][:, None, None, :] * temporal_out.astype(jnp.float32)
    normed = modulated(running, modulation, 6)
    flat = normed.reshape(-1, feature_width)
    hidden = jax.nn.gelu(jnp.dot(flat, fc_in, preferred_element_type=jnp.float32), approximate=True).astype(jnp.bfloat16)
    mlp_out = grouped_product(hidden, fc_out).reshape(batches, frames, patches, feature_width)
    return (running + modulation[:, 8][:, None, None, :] * mlp_out.astype(jnp.float32)).astype(jnp.bfloat16)
```

```python
import functools
import math

import jax
import jax.numpy as jnp
from jax import lax
from jax.experimental import pallas as pl
from jax.experimental.pallas import tpu as pltpu
from jax.sharding import PartitionSpec as P

epsilon = 1e-06
F32 = jnp.float32
BF16 = jnp.bfloat16
VMEM = pl.BlockSpec(memory_space=pltpu.VMEM)
HBM = pl.BlockSpec(memory_space=pltpu.HBM)

NT = (((1,), (1,)), ((), ()))
TN = (((0,), (0,)), ((), ()))
NN = (((1,), (0,)), ((), ()))


def mm(a, b, dims):
    return lax.dot_general(a, b, dims, preferred_element_type=F32)


def norm_rows(values):
    average = jnp.mean(values, axis=-1, keepdims=True)
    centred = values - average
    variance = jnp.mean(centred * centred, axis=-1, keepdims=True)
    return centred * lax.rsqrt(variance + epsilon)


def head_norm(projected, gain):
    mean_square = jnp.mean(projected * projected, axis=1, keepdims=True)
    return projected * lax.rsqrt(mean_square + epsilon) * gain[None]


def attend_pair(q_ref, k_ref, v_ref, heads, cols, factor, mask):
    outs = []
    for h in heads:
        scores = mm(k_ref[h, :, cols], q_ref[h, :, cols], TN)
        weights = jnp.exp2(scores * factor)
        if mask is not None:
            weights = jnp.where(mask, weights, 0.0)
        total = jnp.sum(weights, axis=0, keepdims=True)
        mixed = mm(v_ref[h, :, cols], weights.astype(BF16), NN)
        outs.append(mixed * (1.0 / total))
    return jnp.concatenate(outs, axis=0)


def spatial_kernel(
    head_dim, x_own, x_oth, mod, w_hbm, gain, o_hbm, part_own, part_oth,
    w_ref, o_ref, n_ref, q_ref, k_ref, v_ref, a_ref, sems,
):
    videos, rows, width = x_own.shape
    patches = 2 * rows
    heads = w_ref.shape[1] // head_dim
    copies = [pltpu.make_async_copy(w_hbm.at[i], w_ref.at[i], sems.at[i]) for i in range(3)]
    copies.append(pltpu.make_async_copy(o_hbm, o_ref, sems.at[3]))
    for copy in copies:
        copy.start()
    for v in range(videos):
        for place, source in enumerate((x_own, x_oth)):
            normed = norm_rows(source[v].astype(F32))
            normed = normed * (1.0 + mod[v, 1:2, :]) + mod[v, 0:1, :]
            n_ref[v * patches + place * rows : v * patches + (place + 1) * rows, :] = normed.astype(BF16)
    for which, target in enumerate((q_ref, k_ref, v_ref)):
        copies[which].wait()
        projected = mm(w_ref[which], n_ref[...], NT)
        projected = projected.reshape(heads, head_dim, videos * patches)
        if which < 2:
            projected = head_norm(projected, gain[which])
        target[...] = projected.astype(BF16)
    factor = math.log2(math.e) / math.sqrt(head_dim)
    copies[3].wait()
    for v in range(videos):
        cols = slice(v * patches, (v + 1) * patches)
        for h in range(0, heads, 2):
            mixed = attend_pair(q_ref, k_ref, v_ref, (h, h + 1), cols, factor, None)
            a_ref[h * head_dim : (h + 2) * head_dim, :] = mixed.astype(BF16)
        part = mm(a_ref[...], o_ref[...], TN).astype(BF16)
        part_own[v] = part[:rows]
        part_oth[v] = part[rows:]


def spatial(x_own, x_oth, mod, w, gain, w_out, head_dim):
    videos, rows, width = x_own.shape
    inner = w.shape[1]
    heads = inner // head_dim
    tokens = 2 * rows * videos
    return pl.pallas_call(
        functools.partial(spatial_kernel, head_dim),
        out_shape=[jax.ShapeDtypeStruct((videos, rows, width), BF16)] * 2,
        in_specs=[VMEM, VMEM, VMEM, HBM, VMEM, HBM],
        out_specs=[VMEM, VMEM],
        scratch_shapes=[
            pltpu.VMEM(w.shape, BF16),
            pltpu.VMEM(w_out.shape, BF16),
            pltpu.VMEM((tokens, width), BF16),
            pltpu.VMEM((heads, head_dim, tokens), BF16),
            pltpu.VMEM((heads, head_dim, tokens), BF16),
            pltpu.VMEM((heads, head_dim, tokens), BF16),
            pltpu.VMEM((inner, 2 * rows), BF16),
            pltpu.SemaphoreType.DMA((4,)),
        ],
        compiler_params=pltpu.CompilerParams(vmem_limit_bytes=30 << 20),
        cost_estimate=pl.CostEstimate(flops=6 * 10**9, transcendentals=10**6, bytes_accessed=8 * 10**6),
        name="spatial",
    )(x_own, x_oth, mod, w, gain, w_out)


def middle_kernel(x_ref, own_ref, got_ref, mod, out_ref):
    videos, rows, width = x_ref.shape
    peers = out_ref.shape[0]
    share = rows // peers
    mids = []
    for v in range(videos):
        total = (own_ref[v].astype(F32) + got_ref[v].astype(F32)).astype(BF16).astype(F32)
        mids.append(x_ref[v].astype(F32) + mod[v, 2:3, :] * total)
    for d in range(peers):
        block = jnp.concatenate([m[d * share : (d + 1) * share] for m in mids], axis=0)
        out_ref[d] = block.astype(BF16)


def middle(x_own, own, got, mod, peers):
    videos, rows, width = x_own.shape
    return pl.pallas_call(
        middle_kernel,
        out_shape=jax.ShapeDtypeStruct((peers, videos * rows // peers, width), BF16),
        in_specs=[VMEM] * 4,
        out_specs=VMEM,
        compiler_params=pltpu.CompilerParams(vmem_limit_bytes=16 << 20),
        cost_estimate=pl.CostEstimate(flops=10**8, transcendentals=0, bytes_accessed=10**6),
        name="middle",
    )(x_own, own, got, mod)


def late_kernel(
    head_dim, x_ref, mod, qo_hbm, qr_hbm, gain, oo_hbm, or_hbm, io_hbm, ir_hbm, fo_hbm, fr_hbm, out_ref,
    w_ref, o_ref, i_ref, f_ref, n_ref, q_ref, k_ref, v_ref, a_ref, h_ref, sems,
):
    frames, group, width = x_ref.shape
    videos = mod.shape[0]
    share = group // videos
    tokens = frames * group
    heads = q_ref.shape[0]
    inner = w_ref.shape[2]
    half = heads // 2
    copies = []

    def fetch(source, target):
        copy = pltpu.make_async_copy(source, target, sems.at[len(copies)])
        copy.start()
        copies.append(copy)

    for side, source in enumerate((qo_hbm, qr_hbm)):
        for which in range(3):
            fetch(source.at[which], w_ref.at[side, which])
    fetch(oo_hbm, o_ref.at[0])
    fetch(or_hbm, o_ref.at[1])
    fetch(io_hbm, i_ref.at[0])
    fetch(fo_hbm, f_ref.at[0])
    fetch(ir_hbm, i_ref.at[1])
    fetch(fr_hbm, f_ref.at[1])

    def row(index):
        return mod[:, index : index + 1, :][None]

    running = x_ref[...].astype(F32).reshape(frames, videos, share, width)
    normed = norm_rows(running) * (1.0 + row(4)) + row(3)
    n_ref[...] = normed.reshape(tokens, width).astype(BF16)
    for side in range(2):
        for which, target in enumerate((q_ref, k_ref, v_ref)):
            copies[side * 3 + which].wait()
            projected = mm(w_ref[side, which], n_ref[...], NT)
            projected = projected.reshape(half, head_dim, tokens)
            if which < 2:
                projected = head_norm(projected, gain[which])
            target[side * half : (side + 1) * half] = projected.astype(BF16)
    factor = math.log2(math.e) / math.sqrt(head_dim)
    first = lax.broadcasted_iota(jnp.int32, (tokens, tokens), 0)
    second = lax.broadcasted_iota(jnp.int32, (tokens, tokens), 1)
    mask = lax.rem(first, group) == lax.rem(second, group)
    cols = slice(0, tokens)
    total = None
    for side in range(2):
        for h in range(0, half, 2):
            g = side * half + h
            mixed = attend_pair(q_ref, k_ref, v_ref, (g, g + 1), cols, factor, mask)
            a_ref[h * head_dim : (h + 2) * head_dim, :] = mixed.astype(BF16)
        copies[6 + side].wait()
        part = mm(a_ref[...], o_ref[side], TN).astype(BF16).astype(F32)
        total = part if total is None else total + part
    total = total.astype(BF16).astype(F32).reshape(frames, videos, share, width)
    running = x_ref[...].astype(F32).reshape(frames, videos, share, width) + row(5) * total
    normed = norm_rows(running) * (1.0 + row(7)) + row(6)
    n_ref[...] = normed.reshape(tokens, width).astype(BF16)
    hidden_width = i_ref.shape[2]
    chunk = hidden_width // 3 if hidden_width % 384 == 0 else hidden_width
    mlp = None
    for side in range(2):
        copies[8 + 2 * side].wait()
        for start in range(0, hidden_width, chunk):
            u = mm(n_ref[...], i_ref[side, :, start : start + chunk], NN)
            h_ref[:, start : start + chunk] = jax.nn.gelu(u, approximate=True).astype(BF16)
        copies[9 + 2 * side].wait()
        part = mm(h_ref[...], f_ref[side], NN).astype(BF16).astype(F32)
        mlp = part if mlp is None else mlp + part
    mlp = mlp.astype(BF16).astype(F32).reshape(frames, videos, share, width)
    result = running + row(8) * mlp
    out_ref[...] = result.reshape(frames, group, width).astype(BF16)


def late(x, mod, q_own, q_rem, gain, o_own, o_rem, i_own, i_rem, f_own, f_rem, head_dim):
    frames, group, width = x.shape
    tokens = frames * group
    inner = q_own.shape[1]
    heads = 2 * inner // head_dim
    return pl.pallas_call(
        functools.partial(late_kernel, head_dim),
        out_shape=jax.ShapeDtypeStruct(x.shape, BF16),
        in_specs=[VMEM, VMEM, HBM, HBM, VMEM] + [HBM] * 6,
        out_specs=VMEM,
        scratch_shapes=[
            pltpu.VMEM((2,) + q_own.shape, BF16),
            pltpu.VMEM((2,) + o_own.shape, BF16),
            pltpu.VMEM((2,) + i_own.shape, BF16),
            pltpu.VMEM((2,) + f_own.shape, BF16),
            pltpu.VMEM((tokens, width), BF16),
            pltpu.VMEM((heads, head_dim, tokens), BF16),
            pltpu.VMEM((heads, head_dim, tokens), BF16),
            pltpu.VMEM((heads, head_dim, tokens), BF16),
            pltpu.VMEM((inner, tokens), BF16),
            pltpu.VMEM((tokens, i_own.shape[1]), BF16),
            pltpu.SemaphoreType.DMA((12,)),
        ],
        compiler_params=pltpu.CompilerParams(vmem_limit_bytes=58 << 20),
        cost_estimate=pl.CostEstimate(flops=9 * 10**9, transcendentals=2 * 10**6, bytes_accessed=33 * 10**6),
        name="late",
    )(x, mod, q_own, q_rem, gain, o_own, o_rem, i_own, i_rem, f_own, f_rem)


def paired_body(
    seq_size,
    latent,
    modulation,
    qkv_spatial,
    gain_spatial,
    out_spatial,
    qkv_temporal,
    gain_temporal,
    out_temporal,
    fc_in,
    fc_out,
):
    head_dim = gain_spatial.shape[-1]
    videos, _, rows, width = latent.shape

    def swap(value):
        return lax.ppermute(value, "tp", [(0, 1), (1, 0)])

    x_own = latent.reshape(videos, rows, width)
    w_spatial = jnp.swapaxes(qkv_spatial, 1, 2)
    w_temporal = jnp.swapaxes(qkv_temporal, 1, 2)
    x_oth = swap(x_own)
    q_rem, o_rem, i_rem, f_rem = (swap(w) for w in (w_temporal, out_temporal, fc_in, fc_out))
    own, other = spatial(
        x_own, x_oth, modulation, w_spatial, gain_spatial[..., None], out_spatial, head_dim
    )
    got = swap(other)
    mid = middle(x_own, own, got, modulation, seq_size)
    moved = lax.all_to_all(mid, "seq", 0, 0, tiled=True)
    done = late(
        moved, modulation, w_temporal, q_rem, gain_temporal[..., None], out_temporal, o_rem,
        fc_in, i_rem, fc_out, f_rem, head_dim,
    )
    back = lax.all_to_all(done, "seq", 0, 0, tiled=True)
    back = back.reshape(seq_size, videos, rows // seq_size, width).transpose(1, 0, 2, 3)
    return back.reshape(latent.shape)


def layer_norm(values):
    average = jnp.mean(values, axis=-1, keepdims=True)
    centred = values - average
    variance = jnp.mean(centred * centred, axis=-1, keepdims=True)
    return centred * lax.rsqrt(variance + epsilon)


def modulated(field, modulation, offset):
    shift_row = modulation[:, offset][:, None, None, :]
    scale_row = modulation[:, offset + 1][:, None, None, :]
    return (layer_norm(field) * (1.0 + scale_row) + shift_row).astype(jnp.bfloat16)


def project_heads(rows_piece, table, gains, head_dim):
    results = []
    for which_part in range(3):
        projected = jnp.einsum(
            "bfpd,de->bfpe", rows_piece, table[which_part], preferred_element_type=jnp.float32
        )
        if which_part < 2:
            shaped = projected.reshape(
                projected.shape[:-1] + (projected.shape[-1] // head_dim, head_dim)
            )
            shaped = (
                shaped
                * lax.rsqrt(jnp.mean(shaped * shaped, axis=-1, keepdims=True) + epsilon)
                * gains[which_part]
            )
            projected = shaped.reshape(projected.shape)
        results.append(projected.astype(jnp.bfloat16))
    return jnp.stack(results)


def attend(query_rows, key_rows, value_rows, head_dim):
    groups, length, feature_width = query_rows.shape
    head_count = feature_width // head_dim
    query_heads = query_rows.reshape(groups, length, head_count, head_dim)
    key_heads = key_rows.reshape(groups, length, head_count, head_dim)
    value_heads = value_rows.reshape(groups, length, head_count, head_dim)
    block_rows = min(length, 512)

    def one_block(first_row):
        query_block = lax.dynamic_slice_in_dim(query_heads, first_row, block_rows, 1)
        scores = jnp.einsum(
            "gqhe,gkhe->ghqk", query_block, key_heads, preferred_element_type=jnp.float32
        ) / math.sqrt(head_dim)
        weights = jnp.exp(scores)
        probabilities = (weights / jnp.sum(weights, axis=-1, keepdims=True)).astype(jnp.bfloat16)
        return jnp.einsum(
            "ghqk,gkhe->gqhe", probabilities, value_heads, preferred_element_type=jnp.float32
        ).astype(jnp.bfloat16)

    starts = jnp.arange(length // block_rows, dtype=jnp.int32) * block_rows
    pieces = lax.map(one_block, starts)
    return pieces.transpose(1, 0, 2, 3, 4).reshape(groups, length, feature_width)


def frame_attention(query_rows, key_rows, value_rows, head_dim):
    batches, frames, patches, feature_width = query_rows.shape
    members = [
        item.transpose(0, 2, 1, 3).reshape(batches * patches, frames, feature_width)
        for item in (query_rows, key_rows, value_rows)
    ]
    mixed_heads = attend(members[0], members[1], members[2], head_dim)
    return mixed_heads.reshape(batches, patches, frames, feature_width).transpose(0, 2, 1, 3)


def body(
    latent,
    modulation,
    qkv_spatial,
    gain_spatial,
    out_spatial,
    qkv_temporal,
    gain_temporal,
    out_temporal,
    fc_in,
    fc_out,
):
    head_dim = gain_spatial.shape[-1]
    running = latent.astype(jnp.float32)
    normed = modulated(running, modulation, 0)
    packed = project_heads(
        lax.all_gather(normed, "tp", axis=2, tiled=True), qkv_spatial, gain_spatial, head_dim
    )
    batches, frames, patches, local_width = packed.shape[1:]
    mixed_heads = attend(
        packed[0].reshape(batches * frames, patches, local_width),
        packed[1].reshape(batches * frames, patches, local_width),
        packed[2].reshape(batches * frames, patches, local_width),
        head_dim,
    )
    mixed_heads = mixed_heads.reshape(batches, frames, patches, local_width)
    partial_value = jnp.einsum(
        "bfpe,ed->bfpd", mixed_heads, out_spatial, preferred_element_type=jnp.float32
    )
    spatial_out = lax.psum_scatter(
        partial_value.astype(jnp.bfloat16), "tp", scatter_dimension=2, tiled=True
    )
    running = running + modulation[:, 2][:, None, None, :] * spatial_out.astype(jnp.float32)
    normed = modulated(running, modulation, 3)
    moved_rows = lax.all_to_all(normed, "seq", split_axis=2, concat_axis=1, tiled=True)
    packed = project_heads(
        lax.all_gather(moved_rows, "tp", axis=2, tiled=True), qkv_temporal, gain_temporal, head_dim
    )
    mixed_heads = frame_attention(packed[0], packed[1], packed[2], head_dim)
    partial_value = jnp.einsum(
        "bfpe,ed->bfpd", mixed_heads, out_temporal, preferred_element_type=jnp.float32
    )
    shares = lax.psum_scatter(
        partial_value.astype(jnp.bfloat16), "tp", scatter_dimension=2, tiled=True
    )
    temporal_out = lax.all_to_all(shares, "seq", split_axis=1, concat_axis=2, tiled=True)
    running = running + modulation[:, 5][:, None, None, :] * temporal_out.astype(jnp.float32)
    normed = modulated(running, modulation, 6)
    projected = jnp.einsum(
        "bfpd,de->bfpe",
        lax.all_gather(normed, "tp", axis=2, tiled=True),
        fc_in,
        preferred_element_type=jnp.float32,
    )
    hidden = jax.nn.gelu(projected, approximate=True).astype(jnp.bfloat16)
    partial_value = jnp.einsum("bfpe,ed->bfpd", hidden, fc_out, preferred_element_type=jnp.float32)
    mlp_out = lax.psum_scatter(
        partial_value.astype(jnp.bfloat16), "tp", scatter_dimension=2, tiled=True
    )
    return (running + modulation[:, 8][:, None, None, :] * mlp_out.astype(jnp.float32)).astype(
        jnp.bfloat16
    )


def fits(mesh, local_frames, local_rows, heads_here):
    return (
        mesh.shape["tp"] == 2
        and local_frames == 1
        and local_rows % (8 * mesh.shape["seq"]) == 0
        and heads_here % 2 == 0
    )


def solution(mesh):
    placed = (
        P(None, "seq", "tp", None),
        P(),
        P(None, None, "tp"),
        P(),
        P("tp", None),
        P(None, None, "tp"),
        P(),
        P("tp", None),
        P(None, "tp"),
        P("tp", None),
    )

    def step(*args):
        latent, qkv, gain = args[0], args[2], args[3]
        if fits(mesh, latent.shape[1], latent.shape[2], qkv.shape[2] // gain.shape[1]):
            return paired_body(mesh.shape["seq"], *args)
        return body(*args)

    return jax.shard_map(
        step, mesh=mesh, in_specs=placed, out_specs=P(None, "seq", "tp", None), check_vma=False
    )
```

```python
import functools
import math

import jax
import jax.numpy as jnp
from jax import lax
from jax.experimental import pallas as pl
from jax.experimental.pallas import tpu as pltpu
from jax.sharding import PartitionSpec as P


epsilon = 1e-06
F32 = jnp.float32
BF16 = jnp.bfloat16
VMEM = pl.BlockSpec(memory_space=pltpu.VMEM)
HBM = pl.BlockSpec(memory_space=pltpu.HBM)

NT = (((1,), (1,)), ((), ()))
TN = (((0,), (0,)), ((), ()))
NN = (((1,), (0,)), ((), ()))


def mm(a, b, dims):
    return lax.dot_general(a, b, dims, preferred_element_type=F32)


def norm_rows(values):
    average = jnp.mean(values, axis=-1, keepdims=True)
    centred = values - average
    variance = jnp.mean(centred * centred, axis=-1, keepdims=True)
    return centred * lax.rsqrt(variance + epsilon)


def column(row):
    n = row.shape[1]
    diagonal = lax.broadcasted_iota(jnp.int32, (n, n), 0) == lax.broadcasted_iota(jnp.int32, (n, n), 1)
    return jnp.sum(jnp.where(diagonal, row, 0.0), axis=1, keepdims=True)


def head_norm(projected, gain):
    mean_square = jnp.mean(projected * projected, axis=1, keepdims=True)
    return projected * lax.rsqrt(mean_square + epsilon) * gain[None]


def attend_pair(q_ref, k_ref, v_ref, heads, cols, factor, mask):
    outs = []
    for h in heads:
        scores = mm(k_ref[h, :, cols], q_ref[h, :, cols], TN)
        weights = jnp.exp2(scores * factor)
        if mask is not None:
            weights = jnp.where(mask, weights, 0.0)
        total = jnp.sum(weights, axis=0, keepdims=True)
        mixed = mm(v_ref[h, :, cols], weights.astype(BF16), NN)
        outs.append(mixed * (1.0 / total))
    return jnp.concatenate(outs, axis=0)


def spatial_kernel(
    head_dim, x_own, x_oth, mod, w_hbm, gain, o_hbm, part_own, part_oth,
    w_ref, o_ref, n_ref, q_ref, k_ref, v_ref, a_ref, sems,
):
    videos, rows, _ = x_own.shape
    patches = 2 * rows
    heads = w_ref.shape[1] // head_dim
    copies = [pltpu.make_async_copy(w_hbm.at[i], w_ref.at[i], sems.at[i]) for i in range(3)]
    copies.append(pltpu.make_async_copy(o_hbm, o_ref, sems.at[3]))
    for copy in copies:
        copy.start()
    for v in range(videos):
        for place, source in enumerate((x_own, x_oth)):
            normed = norm_rows(source[v].astype(F32))
            normed = normed * (1.0 + mod[1, v : v + 1, :]) + mod[0, v : v + 1, :]
            n_ref[v * patches + place * rows : v * patches + (place + 1) * rows, :] = normed.astype(BF16)
    for which, target in enumerate((q_ref, k_ref, v_ref)):
        copies[which].wait()
        projected = mm(w_ref[which], n_ref[...], NT)
        projected = projected.reshape(heads, head_dim, videos * patches)
        if which < 2:
            projected = head_norm(projected, column(gain[which : which + 1, :]))
        target[...] = projected.astype(BF16)
    factor = math.log2(math.e) / math.sqrt(head_dim)
    copies[3].wait()
    for v in range(videos):
        cols = slice(v * patches, (v + 1) * patches)
        for h in range(0, heads, 2):
            mixed = attend_pair(q_ref, k_ref, v_ref, (h, h + 1), cols, factor, None)
            a_ref[h * head_dim : (h + 2) * head_dim, :] = mixed.astype(BF16)
        part = mm(a_ref[...], o_ref[...], TN).astype(BF16)
        part_own[v] = part[:rows]
        part_oth[v] = part[rows:]


def spatial(x_own, x_oth, mod, w, gain, w_out, head_dim):
    videos, rows, width = x_own.shape
    inner = w.shape[1]
    heads = inner // head_dim
    tokens = 2 * rows * videos
    return pl.pallas_call(
        functools.partial(spatial_kernel, head_dim),
        out_shape=[jax.ShapeDtypeStruct((videos, rows, width), BF16)] * 2,
        in_specs=[VMEM, VMEM, VMEM, HBM, VMEM, HBM],
        out_specs=[VMEM, VMEM],
        scratch_shapes=[
            pltpu.VMEM(w.shape, BF16),
            pltpu.VMEM(w_out.shape, BF16),
            pltpu.VMEM((tokens, width), BF16),
            pltpu.VMEM((heads, head_dim, tokens), BF16),
            pltpu.VMEM((heads, head_dim, tokens), BF16),
            pltpu.VMEM((heads, head_dim, tokens), BF16),
            pltpu.VMEM((inner, 2 * rows), BF16),
            pltpu.SemaphoreType.DMA((4,)),
        ],
        compiler_params=pltpu.CompilerParams(vmem_limit_bytes=60 << 20),
        cost_estimate=pl.CostEstimate(flops=6 * 10**9, transcendentals=10**6, bytes_accessed=8 * 10**6),
        name="spatial",
    )(x_own, x_oth, mod, w, gain, w_out)


def middle_kernel(x_ref, own_ref, got_ref, mod, out_ref):
    videos, rows, _ = x_ref.shape
    peers = out_ref.shape[0]
    share = rows // peers
    mids = []
    for v in range(videos):
        total = (own_ref[v].astype(F32) + got_ref[v].astype(F32)).astype(BF16).astype(F32)
        mids.append(x_ref[v].astype(F32) + mod[2, v : v + 1, :] * total)
    for d in range(peers):
        block = jnp.concatenate([m[d * share : (d + 1) * share] for m in mids], axis=0)
        out_ref[d] = block.astype(BF16)


def middle(x_own, own, got, mod, peers):
    videos, rows, width = x_own.shape
    return pl.pallas_call(
        middle_kernel,
        out_shape=jax.ShapeDtypeStruct((peers, videos * rows // peers, width), BF16),
        in_specs=[VMEM] * 4,
        out_specs=VMEM,
        compiler_params=pltpu.CompilerParams(vmem_limit_bytes=16 << 20),
        cost_estimate=pl.CostEstimate(flops=10**8, transcendentals=0, bytes_accessed=10**6),
        name="middle",
    )(x_own, own, got, mod)


def late_kernel(
    head_dim, x_ref, mod, qo_hbm, qr_hbm, gain, oo_hbm, or_hbm, io_hbm, ir_hbm, fo_hbm, fr_hbm, out_ref,
    w_ref, o_ref, i_ref, f_ref, n_ref, q_ref, k_ref, v_ref, a_ref, h_ref, sems,
):
    frames, group, width = x_ref.shape
    videos = mod.shape[1]
    share = group // videos
    tokens = frames * group
    heads = q_ref.shape[0]
    half = heads // 2
    copies = []

    def fetch(source, target):
        copy = pltpu.make_async_copy(source, target, sems.at[len(copies)])
        copy.start()
        copies.append(copy)

    for side, source in enumerate((qo_hbm, qr_hbm)):
        for which in range(3):
            fetch(source.at[which], w_ref.at[side, which])
    fetch(oo_hbm, o_ref.at[0])
    fetch(or_hbm, o_ref.at[1])
    fetch(io_hbm, i_ref.at[0])
    fetch(fo_hbm, f_ref.at[0])
    fetch(ir_hbm, i_ref.at[1])
    fetch(fr_hbm, f_ref.at[1])

    def row(index):
        return mod[index][None, :, None, :]

    running = x_ref[...].astype(F32).reshape(frames, videos, share, width)
    normed = norm_rows(running) * (1.0 + row(4)) + row(3)
    n_ref[...] = normed.reshape(tokens, width).astype(BF16)
    for side in range(2):
        for which, target in enumerate((q_ref, k_ref, v_ref)):
            copies[side * 3 + which].wait()
            projected = mm(w_ref[side, which], n_ref[...], NT)
            projected = projected.reshape(half, head_dim, tokens)
            if which < 2:
                projected = head_norm(projected, column(gain[which : which + 1, :]))
            target[side * half : (side + 1) * half] = projected.astype(BF16)
    factor = math.log2(math.e) / math.sqrt(head_dim)
    first = lax.broadcasted_iota(jnp.int32, (tokens, tokens), 0)
    second = lax.broadcasted_iota(jnp.int32, (tokens, tokens), 1)
    mask = lax.rem(first, group) == lax.rem(second, group)
    cols = slice(0, tokens)
    total = None
    for side in range(2):
        for h in range(0, half, 2):
            g = side * half + h
            mixed = attend_pair(q_ref, k_ref, v_ref, (g, g + 1), cols, factor, mask)
            a_ref[h * head_dim : (h + 2) * head_dim, :] = mixed.astype(BF16)
        copies[6 + side].wait()
        part = mm(a_ref[...], o_ref[side], TN).astype(BF16).astype(F32)
        total = part if total is None else total + part
    total = total.astype(BF16).astype(F32).reshape(frames, videos, share, width)
    running = x_ref[...].astype(F32).reshape(frames, videos, share, width) + row(5) * total
    normed = norm_rows(running) * (1.0 + row(7)) + row(6)
    n_ref[...] = normed.reshape(tokens, width).astype(BF16)
    hidden_width = i_ref.shape[2]
    chunk = hidden_width // 3 if hidden_width % 384 == 0 else hidden_width
    mlp = None
    for side in range(2):
        copies[8 + 2 * side].wait()
        for start in range(0, hidden_width, chunk):
            u = mm(n_ref[...], i_ref[side, :, start : start + chunk], NN)
            h_ref[:, start : start + chunk] = jax.nn.gelu(u, approximate=True).astype(BF16)
        copies[9 + 2 * side].wait()
        part = mm(h_ref[...], f_ref[side], NN).astype(BF16).astype(F32)
        mlp = part if mlp is None else mlp + part
    mlp = mlp.astype(BF16).astype(F32).reshape(frames, videos, share, width)
    result = running + row(8) * mlp
    out_ref[...] = result.reshape(frames, group, width).astype(BF16)


def late(x, mod, q_own, q_rem, gain, o_own, o_rem, i_own, i_rem, f_own, f_rem, head_dim):
    frames, group, width = x.shape
    tokens = frames * group
    inner = q_own.shape[1]
    heads = 2 * inner // head_dim
    return pl.pallas_call(
        functools.partial(late_kernel, head_dim),
        out_shape=jax.ShapeDtypeStruct(x.shape, BF16),
        in_specs=[VMEM, VMEM, HBM, HBM, VMEM] + [HBM] * 6,
        out_specs=VMEM,
        scratch_shapes=[
            pltpu.VMEM((2,) + q_own.shape, BF16),
            pltpu.VMEM((2,) + o_own.shape, BF16),
            pltpu.VMEM((2,) + i_own.shape, BF16),
            pltpu.VMEM((2,) + f_own.shape, BF16),
            pltpu.VMEM((tokens, width), BF16),
            pltpu.VMEM((heads, head_dim, tokens), BF16),
            pltpu.VMEM((heads, head_dim, tokens), BF16),
            pltpu.VMEM((heads, head_dim, tokens), BF16),
            pltpu.VMEM((inner, tokens), BF16),
            pltpu.VMEM((tokens, i_own.shape[1]), BF16),
            pltpu.SemaphoreType.DMA((12,)),
        ],
        compiler_params=pltpu.CompilerParams(vmem_limit_bytes=58 << 20),
        cost_estimate=pl.CostEstimate(flops=9 * 10**9, transcendentals=2 * 10**6, bytes_accessed=33 * 10**6),
        name="late",
    )(x, mod, q_own, q_rem, gain, o_own, o_rem, i_own, i_rem, f_own, f_rem)


def paired_body(
    seq_size,
    latent,
    modulation,
    qkv_spatial,
    gain_spatial,
    out_spatial,
    qkv_temporal,
    gain_temporal,
    out_temporal,
    fc_in,
    fc_out,
):
    head_dim = gain_spatial.shape[-1]
    videos, _, rows, width = latent.shape

    def swap(value):
        return lax.ppermute(value, "tp", [(0, 1), (1, 0)])

    x_own = latent.reshape(videos, rows, width)
    w_spatial = jnp.swapaxes(qkv_spatial, 1, 2)
    w_temporal = jnp.swapaxes(qkv_temporal, 1, 2)
    modulation = jnp.swapaxes(modulation, 0, 1)
    x_oth = swap(x_own)
    x_oth, w_sent, o_sent = lax.optimization_barrier((x_oth, w_temporal, out_temporal))
    q_rem = swap(w_sent)
    o_rem = swap(o_sent)
    own, other = spatial(x_own, x_oth, modulation, w_spatial, gain_spatial, out_spatial, head_dim)
    got = swap(other)
    got, i_sent, f_sent = lax.optimization_barrier((got, fc_in, fc_out))
    i_rem = swap(i_sent)
    f_rem = swap(f_sent)
    mid = middle(x_own, own, got, modulation, seq_size)
    moved = lax.all_to_all(mid, "seq", 0, 0, tiled=True)
    done = late(
        moved, modulation, w_temporal, q_rem, gain_temporal, out_temporal, o_rem,
        fc_in, i_rem, fc_out, f_rem, head_dim,
    )
    back = lax.all_to_all(done, "seq", 0, 0, tiled=True)
    back = back.reshape(seq_size, videos, rows // seq_size, width).transpose(1, 0, 2, 3)
    return back.reshape(latent.shape)


def layer_norm(values):
    average = jnp.mean(values, axis=-1, keepdims=True)
    centred = values - average
    variance = jnp.mean(centred * centred, axis=-1, keepdims=True)
    return centred * lax.rsqrt(variance + epsilon)


def modulated(field, modulation, offset):
    shift_row = modulation[:, offset][:, None, None, :]
    scale_row = modulation[:, offset + 1][:, None, None, :]
    return (layer_norm(field) * (1.0 + scale_row) + shift_row).astype(jnp.bfloat16)


def project_heads(rows_piece, table, gains, head_dim):
    results = []
    for which_part in range(3):
        projected = jnp.einsum(
            "bfpd,de->bfpe", rows_piece, table[which_part], preferred_element_type=jnp.float32
        )
        if which_part < 2:
            shaped = projected.reshape(
                projected.shape[:-1] + (projected.shape[-1] // head_dim, head_dim)
            )
            shaped = (
                shaped
                * lax.rsqrt(jnp.mean(shaped * shaped, axis=-1, keepdims=True) + epsilon)
                * gains[which_part]
            )
            projected = shaped.reshape(projected.shape)
        results.append(projected.astype(jnp.bfloat16))
    return jnp.stack(results)


def attend(query_rows, key_rows, value_rows, head_dim):
    groups, length, feature_width = query_rows.shape
    head_count = feature_width // head_dim
    query_heads = query_rows.reshape(groups, length, head_count, head_dim)
    key_heads = key_rows.reshape(groups, length, head_count, head_dim)
    value_heads = value_rows.reshape(groups, length, head_count, head_dim)
    block_rows = min(length, 512)

    def one_block(first_row):
        query_block = lax.dynamic_slice_in_dim(query_heads, first_row, block_rows, 1)
        scores = jnp.einsum(
            "gqhe,gkhe->ghqk", query_block, key_heads, preferred_element_type=jnp.float32
        ) / math.sqrt(head_dim)
        weights = jnp.exp(scores)
        probabilities = (weights / jnp.sum(weights, axis=-1, keepdims=True)).astype(jnp.bfloat16)
        return jnp.einsum(
            "ghqk,gkhe->gqhe", probabilities, value_heads, preferred_element_type=jnp.float32
        ).astype(jnp.bfloat16)

    starts = jnp.arange(length // block_rows, dtype=jnp.int32) * block_rows
    pieces = lax.map(one_block, starts)
    return pieces.transpose(1, 0, 2, 3, 4).reshape(groups, length, feature_width)


def frame_attention(query_rows, key_rows, value_rows, head_dim):
    batches, frames, patches, feature_width = query_rows.shape
    members = [
        item.transpose(0, 2, 1, 3).reshape(batches * patches, frames, feature_width)
        for item in (query_rows, key_rows, value_rows)
    ]
    mixed_heads = attend(members[0], members[1], members[2], head_dim)
    return mixed_heads.reshape(batches, patches, frames, feature_width).transpose(0, 2, 1, 3)


def body(
    latent,
    modulation,
    qkv_spatial,
    gain_spatial,
    out_spatial,
    qkv_temporal,
    gain_temporal,
    out_temporal,
    fc_in,
    fc_out,
):
    head_dim = gain_spatial.shape[-1]
    running = latent.astype(jnp.float32)
    normed = modulated(running, modulation, 0)
    packed = project_heads(
        lax.all_gather(normed, "tp", axis=2, tiled=True), qkv_spatial, gain_spatial, head_dim
    )
    batches, frames, patches, local_width = packed.shape[1:]
    mixed_heads = attend(
        packed[0].reshape(batches * frames, patches, local_width),
        packed[1].reshape(batches * frames, patches, local_width),
        packed[2].reshape(batches * frames, patches, local_width),
        head_dim,
    )
    mixed_heads = mixed_heads.reshape(batches, frames, patches, local_width)
    partial_value = jnp.einsum(
        "bfpe,ed->bfpd", mixed_heads, out_spatial, preferred_element_type=jnp.float32
    )
    spatial_out = lax.psum_scatter(
        partial_value.astype(jnp.bfloat16), "tp", scatter_dimension=2, tiled=True
    )
    running = running + modulation[:, 2][:, None, None, :] * spatial_out.astype(jnp.float32)
    normed = modulated(running, modulation, 3)
    moved_rows = lax.all_to_all(normed, "seq", split_axis=2, concat_axis=1, tiled=True)
    packed = project_heads(
        lax.all_gather(moved_rows, "tp", axis=2, tiled=True), qkv_temporal, gain_temporal, head_dim
    )
    mixed_heads = frame_attention(packed[0], packed[1], packed[2], head_dim)
    partial_value = jnp.einsum(
        "bfpe,ed->bfpd", mixed_heads, out_temporal, preferred_element_type=jnp.float32
    )
    shares = lax.psum_scatter(
        partial_value.astype(jnp.bfloat16), "tp", scatter_dimension=2, tiled=True
    )
    temporal_out = lax.all_to_all(shares, "seq", split_axis=1, concat_axis=2, tiled=True)
    running = running + modulation[:, 5][:, None, None, :] * temporal_out.astype(jnp.float32)
    normed = modulated(running, modulation, 6)
    projected = jnp.einsum(
        "bfpd,de->bfpe",
        lax.all_gather(normed, "tp", axis=2, tiled=True),
        fc_in,
        preferred_element_type=jnp.float32,
    )
    hidden = jax.nn.gelu(projected, approximate=True).astype(jnp.bfloat16)
    partial_value = jnp.einsum("bfpe,ed->bfpd", hidden, fc_out, preferred_element_type=jnp.float32)
    mlp_out = lax.psum_scatter(
        partial_value.astype(jnp.bfloat16), "tp", scatter_dimension=2, tiled=True
    )
    return (running + modulation[:, 8][:, None, None, :] * mlp_out.astype(jnp.float32)).astype(
        jnp.bfloat16
    )


def fits(mesh, local_frames, local_rows, heads_here):
    return (
        mesh.shape["tp"] == 2
        and local_frames == 1
        and local_rows % (8 * mesh.shape["seq"]) == 0
        and heads_here % 2 == 0
    )


def solution(mesh):
    placed = (
        P(None, "seq", "tp", None),
        P(),
        P(None, None, "tp"),
        P(),
        P("tp", None),
        P(None, None, "tp"),
        P(),
        P("tp", None),
        P(None, "tp"),
        P("tp", None),
    )

    def step(*args):
        latent, qkv, gain = args[0], args[2], args[3]
        if fits(mesh, latent.shape[1], latent.shape[2], qkv.shape[2] // gain.shape[1]):
            return paired_body(mesh.shape["seq"], *args)
        return body(*args)

    return jax.shard_map(
        step, mesh=mesh, in_specs=placed, out_specs=P(None, "seq", "tp", None), check_vma=False
    )
```

```python
import functools
import math

import jax
import jax.numpy as jnp
from jax import lax
from jax.experimental import pallas as pl
from jax.experimental.pallas import tpu as pltpu
from jax.sharding import PartitionSpec as P


epsilon = 1e-06
F32 = jnp.float32
BF16 = jnp.bfloat16
VMEM = pl.BlockSpec(memory_space=pltpu.VMEM)
HBM = pl.BlockSpec(memory_space=pltpu.HBM)

NT = (((1,), (1,)), ((), ()))
TN = (((0,), (0,)), ((), ()))
NN = (((1,), (0,)), ((), ()))


def mm(a, b, dims):
    return lax.dot_general(a, b, dims, preferred_element_type=F32)


def norm_rows(values):
    average = jnp.mean(values, axis=-1, keepdims=True)
    centred = values - average
    variance = jnp.mean(centred * centred, axis=-1, keepdims=True)
    return centred * lax.rsqrt(variance + epsilon)


def column(row):
    n = row.shape[1]
    diagonal = lax.broadcasted_iota(jnp.int32, (n, n), 0) == lax.broadcasted_iota(jnp.int32, (n, n), 1)
    return jnp.sum(jnp.where(diagonal, row, 0.0), axis=1, keepdims=True)


def head_norm(projected, gain):
    mean_square = jnp.mean(projected * projected, axis=1, keepdims=True)
    return projected * lax.rsqrt(mean_square + epsilon) * gain[None]


def padded_rows(head_dim):
    return -(-(head_dim + 1) // 16) * 16


def with_ones(values):
    heads, head_dim, tokens = values.shape
    extra = padded_rows(head_dim) - head_dim
    place = lax.broadcasted_iota(jnp.int32, (heads, extra, tokens), 1)
    return jnp.concatenate([values, jnp.where(place == 0, 1.0, 0.0)], axis=1)


def normalized(mixed, head_dim):
    return mixed[:head_dim] * (1.0 / mixed[head_dim : head_dim + 1])


def spatial_kernel(
    head_dim, x_own, x_oth, mod, w_hbm, gain, o_hbm, part_own, part_oth,
    w_ref, o_ref, n_ref, q_ref, k_ref, v_ref, s_ref, p_ref, a_ref, sems,
):
    videos, rows, _ = x_own.shape
    patches = 2 * rows
    heads = w_ref.shape[1] // head_dim
    copies = [pltpu.make_async_copy(w_hbm.at[i], w_ref.at[i], sems.at[i]) for i in range(3)]
    copies.append(pltpu.make_async_copy(o_hbm, o_ref, sems.at[3]))
    for copy in copies:
        copy.start()
    for v in range(videos):
        for place, source in enumerate((x_own, x_oth)):
            normed = norm_rows(source[v].astype(F32))
            normed = normed * (1.0 + mod[1, v : v + 1, :]) + mod[0, v : v + 1, :]
            n_ref[v * patches + place * rows : v * patches + (place + 1) * rows, :] = normed.astype(BF16)
    factor = math.log2(math.e) / math.sqrt(head_dim)
    for copy in copies:
        copy.wait()
    for which, target in enumerate((q_ref, k_ref, v_ref)):
        projected = mm(w_ref[which], n_ref[...], NT)
        projected = projected.reshape(heads, head_dim, videos * patches)
        if which < 2:
            gains = column(gain[which : which + 1, :])
            projected = head_norm(projected, gains * factor if which == 0 else gains)
        else:
            projected = with_ones(projected)
        target[...] = projected.astype(BF16)
    for v in range(videos):
        cols = slice(v * patches, (v + 1) * patches)
        for h in range(heads):
            s_ref[v, h] = mm(k_ref[h, :, cols], q_ref[h, :, cols], TN)
    for v in range(videos):
        for h in range(heads):
            p_ref[v, h] = jnp.exp2(s_ref[v, h]).astype(BF16)
    for v in range(videos):
        cols = slice(v * patches, (v + 1) * patches)
        for h in range(0, heads, 2):
            pair = [
                normalized(mm(v_ref[g, :, cols], p_ref[v, g], NN), head_dim) for g in (h, h + 1)
            ]
            a_ref[v, h * head_dim : (h + 2) * head_dim, :] = jnp.concatenate(pair, axis=0).astype(BF16)
    for v in range(videos):
        part = mm(a_ref[v], o_ref[...], TN).astype(BF16)
        part_own[v] = part[:rows]
        part_oth[v] = part[rows:]


def spatial(x_own, x_oth, mod, w, gain, w_out, head_dim):
    videos, rows, width = x_own.shape
    inner = w.shape[1]
    heads = inner // head_dim
    tokens = 2 * rows * videos
    return pl.pallas_call(
        functools.partial(spatial_kernel, head_dim),
        out_shape=[jax.ShapeDtypeStruct((videos, rows, width), BF16)] * 2,
        in_specs=[VMEM, VMEM, VMEM, HBM, VMEM, HBM],
        out_specs=[VMEM, VMEM],
        scratch_shapes=[
            pltpu.VMEM(w.shape, BF16),
            pltpu.VMEM(w_out.shape, BF16),
            pltpu.VMEM((tokens, width), BF16),
            pltpu.VMEM((heads, head_dim, tokens), BF16),
            pltpu.VMEM((heads, head_dim, tokens), BF16),
            pltpu.VMEM((heads, padded_rows(head_dim), tokens), BF16),
            pltpu.VMEM((videos, heads, 2 * rows, 2 * rows), F32),
            pltpu.VMEM((videos, heads, 2 * rows, 2 * rows), BF16),
            pltpu.VMEM((videos, inner, 2 * rows), BF16),
            pltpu.SemaphoreType.DMA((4,)),
        ],
        compiler_params=pltpu.CompilerParams(vmem_limit_bytes=60 << 20),
        cost_estimate=pl.CostEstimate(flops=6 * 10**9, transcendentals=10**6, bytes_accessed=8 * 10**6),
        name="spatial",
    )(x_own, x_oth, mod, w, gain, w_out)


def middle_kernel(x_ref, own_ref, got_ref, mod, out_ref):
    videos, rows, _ = x_ref.shape
    peers = out_ref.shape[0]
    share = rows // peers
    mids = []
    for v in range(videos):
        total = (own_ref[v].astype(F32) + got_ref[v].astype(F32)).astype(BF16).astype(F32)
        mids.append(x_ref[v].astype(F32) + mod[2, v : v + 1, :] * total)
    for d in range(peers):
        block = jnp.concatenate([m[d * share : (d + 1) * share] for m in mids], axis=0)
        out_ref[d] = block.astype(BF16)


def middle(x_own, own, got, mod, peers):
    videos, rows, width = x_own.shape
    return pl.pallas_call(
        middle_kernel,
        out_shape=jax.ShapeDtypeStruct((peers, videos * rows // peers, width), BF16),
        in_specs=[VMEM] * 4,
        out_specs=VMEM,
        compiler_params=pltpu.CompilerParams(vmem_limit_bytes=16 << 20),
        cost_estimate=pl.CostEstimate(flops=10**8, transcendentals=0, bytes_accessed=10**6),
        name="middle",
    )(x_own, own, got, mod)


def late_kernel(
    head_dim, x_ref, mod, qo_hbm, qr_hbm, gain, oo_hbm, or_hbm, io_hbm, ir_hbm, fo_hbm, fr_hbm, out_ref,
    w_ref, o_ref, i_ref, f_ref, n_ref, r_ref, q_ref, k_ref, v_ref, s_ref, p_ref, a_ref, h_ref, sems,
):
    frames, group, _ = x_ref.shape
    videos = mod.shape[1]
    share = group // videos
    tokens = frames * group
    heads = q_ref.shape[0]
    inner = w_ref.shape[2]
    half = heads // 2
    copies = []

    def fetch(source, target):
        copy = pltpu.make_async_copy(source, target, sems.at[len(copies)])
        copy.start()
        copies.append(copy)

    for side, source in enumerate((qo_hbm, qr_hbm)):
        for which in range(3):
            fetch(source.at[which], w_ref.at[side, which])
    fetch(oo_hbm, o_ref.at[0])
    fetch(or_hbm, o_ref.at[1])
    fetch(io_hbm, i_ref.at[0])
    fetch(fo_hbm, f_ref.at[0])
    fetch(ir_hbm, i_ref.at[1])
    fetch(fr_hbm, f_ref.at[1])

    def video_rows(v):
        picked = [x_ref[f].astype(F32)[v * share : (v + 1) * share] for f in range(frames)]
        return jnp.concatenate(picked, axis=0)

    each = frames * share
    for v in range(videos):
        normed = norm_rows(video_rows(v)) * (1.0 + mod[4, v : v + 1, :]) + mod[3, v : v + 1, :]
        n_ref[v * each : (v + 1) * each, :] = normed.astype(BF16)
    factor = math.log2(math.e) / math.sqrt(head_dim)
    columns = [column(gain[which : which + 1, :]) for which in range(2)]
    for copy in copies[:8]:
        copy.wait()
    for side in range(2):
        for which, target in enumerate((q_ref, k_ref, v_ref)):
            projected = mm(w_ref[side, which], n_ref[...], NT)
            projected = projected.reshape(half, head_dim, tokens)
            if which < 2:
                projected = head_norm(projected, columns[which] * factor if which == 0 else columns[which])
            else:
                projected = with_ones(projected)
            target[side * half : (side + 1) * half] = projected.astype(BF16)
    for h in range(heads):
        for v in range(videos):
            cols = slice(v * each, (v + 1) * each)
            s_ref[h, v] = mm(k_ref[h, :, cols], q_ref[h, :, cols], TN)
    first = lax.broadcasted_iota(jnp.int32, (share, each), 0)
    second = lax.broadcasted_iota(jnp.int32, (share, each), 1)
    same = (first == lax.rem(second, share))[None]
    for h in range(heads):
        for v in range(videos):
            weights = jnp.exp2(s_ref[h, v]).reshape(frames, share, each)
            p_ref[h, v] = jnp.where(same, weights, 0.0).reshape(each, each).astype(BF16)
    for h in range(0, heads, 2):
        for v in range(videos):
            cols = slice(v * each, (v + 1) * each)
            pair = [
                normalized(mm(v_ref[g, :, cols], p_ref[g, v], NN), head_dim) for g in (h, h + 1)
            ]
            a_ref[h * head_dim : (h + 2) * head_dim, cols] = jnp.concatenate(pair, axis=0).astype(BF16)
    total = None
    for side in range(2):
        part = mm(a_ref[side * inner : (side + 1) * inner, :], o_ref[side], TN)
        part = part.astype(BF16).astype(F32)
        total = part if total is None else total + part
    total = total.astype(BF16).astype(F32)
    for v in range(videos):
        there = slice(v * each, (v + 1) * each)
        running = video_rows(v) + mod[5, v : v + 1, :] * total[there]
        r_ref[there, :] = running
        normed = norm_rows(running) * (1.0 + mod[7, v : v + 1, :]) + mod[6, v : v + 1, :]
        n_ref[there, :] = normed.astype(BF16)
    for copy in copies[8:]:
        copy.wait()
    hidden_width = i_ref.shape[2]
    chunk = hidden_width // 3 if hidden_width % 384 == 0 else hidden_width
    for side in range(2):
        for start in range(0, hidden_width, chunk):
            u = mm(n_ref[...], i_ref[side, :, start : start + chunk], NN)
            h_ref[side, :, start : start + chunk] = jax.nn.gelu(u, approximate=True).astype(BF16)
    mlp = None
    for side in range(2):
        part = mm(h_ref[side], f_ref[side], NN).astype(BF16).astype(F32)
        mlp = part if mlp is None else mlp + part
    mlp = mlp.astype(BF16).astype(F32)
    results = []
    for v in range(videos):
        there = slice(v * each, (v + 1) * each)
        results.append(r_ref[there, :] + mod[8, v : v + 1, :] * mlp[there])
    for f in range(frames):
        block = [r[f * share : (f + 1) * share] for r in results]
        out_ref[f] = jnp.concatenate(block, axis=0).astype(BF16)


def late(x, mod, q_own, q_rem, gain, o_own, o_rem, i_own, i_rem, f_own, f_rem, head_dim):
    frames, group, width = x.shape
    tokens = frames * group
    inner = q_own.shape[1]
    heads = 2 * inner // head_dim
    videos = mod.shape[1]
    return pl.pallas_call(
        functools.partial(late_kernel, head_dim),
        out_shape=jax.ShapeDtypeStruct(x.shape, BF16),
        in_specs=[VMEM, VMEM, HBM, HBM, VMEM] + [HBM] * 6,
        out_specs=VMEM,
        scratch_shapes=[
            pltpu.VMEM((2,) + q_own.shape, BF16),
            pltpu.VMEM((2,) + o_own.shape, BF16),
            pltpu.VMEM((2,) + i_own.shape, BF16),
            pltpu.VMEM((2,) + f_own.shape, BF16),
            pltpu.VMEM((tokens, width), BF16),
            pltpu.VMEM((tokens, width), F32),
            pltpu.VMEM((heads, head_dim, tokens), BF16),
            pltpu.VMEM((heads, head_dim, tokens), BF16),
            pltpu.VMEM((heads, padded_rows(head_dim), tokens), BF16),
            pltpu.VMEM((heads, videos, tokens // videos, tokens // videos), F32),
            pltpu.VMEM((heads, videos, tokens // videos, tokens // videos), BF16),
            pltpu.VMEM((2 * inner, tokens), BF16),
            pltpu.VMEM((2, tokens, i_own.shape[1]), BF16),
            pltpu.SemaphoreType.DMA((12,)),
        ],
        compiler_params=pltpu.CompilerParams(vmem_limit_bytes=58 << 20),
        cost_estimate=pl.CostEstimate(flops=9 * 10**9, transcendentals=2 * 10**6, bytes_accessed=33 * 10**6),
        name="late",
    )(x, mod, q_own, q_rem, gain, o_own, o_rem, i_own, i_rem, f_own, f_rem)


def paired_body(
    seq_size,
    latent,
    modulation,
    qkv_spatial,
    gain_spatial,
    out_spatial,
    qkv_temporal,
    gain_temporal,
    out_temporal,
    fc_in,
    fc_out,
):
    head_dim = gain_spatial.shape[-1]
    videos, _, rows, width = latent.shape

    def swap(value):
        return lax.ppermute(value, "tp", [(0, 1), (1, 0)])

    x_own = latent.reshape(videos, rows, width)
    w_spatial = jnp.swapaxes(qkv_spatial, 1, 2)
    w_temporal = jnp.swapaxes(qkv_temporal, 1, 2)
    modulation = jnp.swapaxes(modulation, 0, 1)
    x_oth = swap(x_own)
    x_oth, w_sent, o_sent = lax.optimization_barrier((x_oth, w_temporal, out_temporal))
    q_rem = swap(w_sent)
    o_rem = swap(o_sent)
    own, other = spatial(x_own, x_oth, modulation, w_spatial, gain_spatial, out_spatial, head_dim)
    got = swap(other)
    got, i_sent, f_sent = lax.optimization_barrier((got, fc_in, fc_out))
    i_rem = swap(i_sent)
    f_rem = swap(f_sent)
    mid = middle(x_own, own, got, modulation, seq_size)
    moved = lax.all_to_all(mid, "seq", 0, 0, tiled=True)
    done = late(
        moved, modulation, w_temporal, q_rem, gain_temporal, out_temporal, o_rem,
        fc_in, i_rem, fc_out, f_rem, head_dim,
    )
    back = lax.all_to_all(done, "seq", 0, 0, tiled=True)
    back = back.reshape(seq_size, videos, rows // seq_size, width).transpose(1, 0, 2, 3)
    return back.reshape(latent.shape)


def layer_norm(values):
    average = jnp.mean(values, axis=-1, keepdims=True)
    centred = values - average
    variance = jnp.mean(centred * centred, axis=-1, keepdims=True)
    return centred * lax.rsqrt(variance + epsilon)


def modulated(field, modulation, offset):
    shift_row = modulation[:, offset][:, None, None, :]
    scale_row = modulation[:, offset + 1][:, None, None, :]
    return (layer_norm(field) * (1.0 + scale_row) + shift_row).astype(jnp.bfloat16)


def project_heads(rows_piece, table, gains, head_dim):
    results = []
    for which_part in range(3):
        projected = jnp.einsum(
            "bfpd,de->bfpe", rows_piece, table[which_part], preferred_element_type=jnp.float32
        )
        if which_part < 2:
            shaped = projected.reshape(
                projected.shape[:-1] + (projected.shape[-1] // head_dim, head_dim)
            )
            shaped = (
                shaped
                * lax.rsqrt(jnp.mean(shaped * shaped, axis=-1, keepdims=True) + epsilon)
                * gains[which_part]
            )
            projected = shaped.reshape(projected.shape)
        results.append(projected.astype(jnp.bfloat16))
    return jnp.stack(results)


def attend(query_rows, key_rows, value_rows, head_dim):
    groups, length, feature_width = query_rows.shape
    head_count = feature_width // head_dim
    query_heads = query_rows.reshape(groups, length, head_count, head_dim)
    key_heads = key_rows.reshape(groups, length, head_count, head_dim)
    value_heads = value_rows.reshape(groups, length, head_count, head_dim)
    block_rows = min(length, 512)

    def one_block(first_row):
        query_block = lax.dynamic_slice_in_dim(query_heads, first_row, block_rows, 1)
        scores = jnp.einsum(
            "gqhe,gkhe->ghqk", query_block, key_heads, preferred_element_type=jnp.float32
        ) / math.sqrt(head_dim)
        weights = jnp.exp(scores)
        probabilities = (weights / jnp.sum(weights, axis=-1, keepdims=True)).astype(jnp.bfloat16)
        return jnp.einsum(
            "ghqk,gkhe->gqhe", probabilities, value_heads, preferred_element_type=jnp.float32
        ).astype(jnp.bfloat16)

    starts = jnp.arange(length // block_rows, dtype=jnp.int32) * block_rows
    pieces = lax.map(one_block, starts)
    return pieces.transpose(1, 0, 2, 3, 4).reshape(groups, length, feature_width)


def frame_attention(query_rows, key_rows, value_rows, head_dim):
    batches, frames, patches, feature_width = query_rows.shape
    members = [
        item.transpose(0, 2, 1, 3).reshape(batches * patches, frames, feature_width)
        for item in (query_rows, key_rows, value_rows)
    ]
    mixed_heads = attend(members[0], members[1], members[2], head_dim)
    return mixed_heads.reshape(batches, patches, frames, feature_width).transpose(0, 2, 1, 3)


def body(
    latent,
    modulation,
    qkv_spatial,
    gain_spatial,
    out_spatial,
    qkv_temporal,
    gain_temporal,
    out_temporal,
    fc_in,
    fc_out,
):
    head_dim = gain_spatial.shape[-1]
    running = latent.astype(jnp.float32)
    normed = modulated(running, modulation, 0)
    packed = project_heads(
        lax.all_gather(normed, "tp", axis=2, tiled=True), qkv_spatial, gain_spatial, head_dim
    )
    batches, frames, patches, local_width = packed.shape[1:]
    mixed_heads = attend(
        packed[0].reshape(batches * frames, patches, local_width),
        packed[1].reshape(batches * frames, patches, local_width),
        packed[2].reshape(batches * frames, patches, local_width),
        head_dim,
    )
    mixed_heads = mixed_heads.reshape(batches, frames, patches, local_width)
    partial_value = jnp.einsum(
        "bfpe,ed->bfpd", mixed_heads, out_spatial, preferred_element_type=jnp.float32
    )
    spatial_out = lax.psum_scatter(
        partial_value.astype(jnp.bfloat16), "tp", scatter_dimension=2, tiled=True
    )
    running = running + modulation[:, 2][:, None, None, :] * spatial_out.astype(jnp.float32)
    normed = modulated(running, modulation, 3)
    moved_rows = lax.all_to_all(normed, "seq", split_axis=2, concat_axis=1, tiled=True)
    packed = project_heads(
        lax.all_gather(moved_rows, "tp", axis=2, tiled=True), qkv_temporal, gain_temporal, head_dim
    )
    mixed_heads = frame_attention(packed[0], packed[1], packed[2], head_dim)
    partial_value = jnp.einsum(
        "bfpe,ed->bfpd", mixed_heads, out_temporal, preferred_element_type=jnp.float32
    )
    shares = lax.psum_scatter(
        partial_value.astype(jnp.bfloat16), "tp", scatter_dimension=2, tiled=True
    )
    temporal_out = lax.all_to_all(shares, "seq", split_axis=1, concat_axis=2, tiled=True)
    running = running + modulation[:, 5][:, None, None, :] * temporal_out.astype(jnp.float32)
    normed = modulated(running, modulation, 6)
    projected = jnp.einsum(
        "bfpd,de->bfpe",
        lax.all_gather(normed, "tp", axis=2, tiled=True),
        fc_in,
        preferred_element_type=jnp.float32,
    )
    hidden = jax.nn.gelu(projected, approximate=True).astype(jnp.bfloat16)
    partial_value = jnp.einsum("bfpe,ed->bfpd", hidden, fc_out, preferred_element_type=jnp.float32)
    mlp_out = lax.psum_scatter(
        partial_value.astype(jnp.bfloat16), "tp", scatter_dimension=2, tiled=True
    )
    return (running + modulation[:, 8][:, None, None, :] * mlp_out.astype(jnp.float32)).astype(
        jnp.bfloat16
    )


def fits(mesh, local_frames, local_rows, heads_here):
    return (
        mesh.shape["tp"] == 2
        and local_frames == 1
        and local_rows % (8 * mesh.shape["seq"]) == 0
        and heads_here % 2 == 0
    )


def solution(mesh):
    placed = (
        P(None, "seq", "tp", None),
        P(),
        P(None, None, "tp"),
        P(),
        P("tp", None),
        P(None, None, "tp"),
        P(),
        P("tp", None),
        P(None, "tp"),
        P("tp", None),
    )

    def step(*args):
        latent, qkv, gain = args[0], args[2], args[3]
        if fits(mesh, latent.shape[1], latent.shape[2], qkv.shape[2] // gain.shape[1]):
            return paired_body(mesh.shape["seq"], *args)
        return body(*args)

    return jax.shard_map(
        step, mesh=mesh, in_specs=placed, out_specs=P(None, "seq", "tp", None), check_vma=False
    )
```

```python
import functools
import math

import jax
import jax.numpy as jnp
from jax import lax
from jax.experimental import pallas as pl
from jax.experimental.pallas import tpu as pltpu
from jax.sharding import PartitionSpec as P


epsilon = 1e-06
F32 = jnp.float32
BF16 = jnp.bfloat16
VMEM = pl.BlockSpec(memory_space=pltpu.VMEM)
HBM = pl.BlockSpec(memory_space=pltpu.HBM)

MIB = 1 << 20

NT = (((1,), (1,)), ((), ()))
TN = (((0,), (0,)), ((), ()))
NN = (((1,), (0,)), ((), ()))


def mm(a, b, dims):
    return lax.dot_general(a, b, dims, preferred_element_type=F32)


def hbm(value):
    return pltpu.with_memory_space_constraint(value, pltpu.HBM)


class Fetches:
    def __init__(self, sems):
        self.sems, self.made = sems, {}

    def start(self, name, source, target):
        copy = pltpu.make_async_copy(source, target, self.sems.at[len(self.made)])
        copy.start()
        self.made[name] = copy

    def wait(self, *names):
        for name in names:
            self.made[name].wait()


def norm_rows(values):
    average = jnp.mean(values, axis=-1, keepdims=True)
    centred = values - average
    variance = jnp.mean(centred * centred, axis=-1, keepdims=True)
    return centred * lax.rsqrt(variance + epsilon)


def column(row):
    n = row.shape[1]
    diagonal = lax.broadcasted_iota(jnp.int32, (n, n), 0) == lax.broadcasted_iota(jnp.int32, (n, n), 1)
    return jnp.sum(jnp.where(diagonal, row, 0.0), axis=1, keepdims=True)


def head_norm(projected, gain):
    mean_square = jnp.mean(projected * projected, axis=1, keepdims=True)
    return projected * lax.rsqrt(mean_square + epsilon) * gain[None]


def padded_rows(head_dim):
    return -(-(head_dim + 1) // 16) * 16


def with_ones(values):
    heads, head_dim, tokens = values.shape
    extra = padded_rows(head_dim) - head_dim
    place = lax.broadcasted_iota(jnp.int32, (heads, extra, tokens), 1)
    return jnp.concatenate([values, jnp.where(place == 0, 1.0, 0.0)], axis=1)


def normalized(mixed, head_dim):
    return mixed[:head_dim] * (1.0 / mixed[head_dim : head_dim + 1])


def spatial_kernel(
    head_dim, own_hbm, oth_hbm, mod_hbm, w_hbm, gain_hbm, o_hbm, part_own, part_oth,
    x_own, x_oth, mod, gain, w_ref, o_ref, n_ref, q_ref, k_ref, v_ref, s_ref, p_ref, a_ref, sems,
):
    videos, rows, _ = x_own.shape
    patches = 2 * rows
    heads = w_ref.shape[1] // head_dim
    fetch = Fetches(sems)
    fetch.start("own", own_hbm, x_own)
    fetch.start("mod", mod_hbm, mod)
    fetch.start("oth", oth_hbm, x_oth)
    fetch.start("gain", gain_hbm, gain)
    for which in range(3):
        fetch.start(which, w_hbm.at[which], w_ref.at[which])
    fetch.start("out", o_hbm, o_ref)
    fetch.wait("own", "mod", "oth", "gain")
    for v in range(videos):
        for place, source in enumerate((x_own, x_oth)):
            normed = norm_rows(source[v].astype(F32))
            normed = normed * (1.0 + mod[1, v : v + 1, :]) + mod[0, v : v + 1, :]
            n_ref[v * patches + place * rows : v * patches + (place + 1) * rows, :] = normed.astype(BF16)
    factor = math.log2(math.e) / math.sqrt(head_dim)
    for which, target in enumerate((q_ref, k_ref, v_ref)):
        fetch.wait(which)
        projected = mm(w_ref[which], n_ref[...], NT)
        projected = projected.reshape(heads, head_dim, videos * patches)
        if which < 2:
            gains = column(gain[which : which + 1, :])
            projected = head_norm(projected, gains * factor if which == 0 else gains)
        else:
            projected = with_ones(projected)
        target[...] = projected.astype(BF16)
    for v in range(videos):
        cols = slice(v * patches, (v + 1) * patches)
        for h in range(heads):
            s_ref[v, h] = mm(k_ref[h, :, cols], q_ref[h, :, cols], TN)
    for v in range(videos):
        for h in range(heads):
            p_ref[v, h] = jnp.exp2(s_ref[v, h]).astype(BF16)
    for v in range(videos):
        cols = slice(v * patches, (v + 1) * patches)
        for h in range(0, heads, 2):
            pair = [
                normalized(mm(v_ref[g, :, cols], p_ref[v, g], NN), head_dim) for g in (h, h + 1)
            ]
            a_ref[v, h * head_dim : (h + 2) * head_dim, :] = jnp.concatenate(pair, axis=0).astype(BF16)
    fetch.wait("out")
    for v in range(videos):
        part = mm(a_ref[v], o_ref[...], TN).astype(BF16)
        part_own[v] = part[:rows]
        part_oth[v] = part[rows:]


def spatial(x_own, x_oth, mod, w, gain, w_out, head_dim):
    videos, rows, width = x_own.shape
    inner = w.shape[1]
    heads = inner // head_dim
    tokens = 2 * rows * videos
    return pl.pallas_call(
        functools.partial(spatial_kernel, head_dim),
        out_shape=[jax.ShapeDtypeStruct((videos, rows, width), BF16)] * 2,
        in_specs=[HBM] * 6,
        out_specs=[VMEM, VMEM],
        scratch_shapes=[
            pltpu.VMEM(x_own.shape, BF16),
            pltpu.VMEM(x_own.shape, BF16),
            pltpu.VMEM(mod.shape, F32),
            pltpu.VMEM(gain.shape, F32),
            pltpu.VMEM(w.shape, BF16),
            pltpu.VMEM(w_out.shape, BF16),
            pltpu.VMEM((tokens, width), BF16),
            pltpu.VMEM((heads, head_dim, tokens), BF16),
            pltpu.VMEM((heads, head_dim, tokens), BF16),
            pltpu.VMEM((heads, padded_rows(head_dim), tokens), BF16),
            pltpu.VMEM((videos, heads, 2 * rows, 2 * rows), F32),
            pltpu.VMEM((videos, heads, 2 * rows, 2 * rows), BF16),
            pltpu.VMEM((videos, inner, 2 * rows), BF16),
            pltpu.SemaphoreType.DMA((8,)),
        ],
        compiler_params=pltpu.CompilerParams(vmem_limit_bytes=28 * MIB),
        cost_estimate=pl.CostEstimate(flops=6 * 10**9, transcendentals=10**6, bytes_accessed=8 * 10**6),
        name="spatial",
    )(hbm(x_own), x_oth, hbm(mod), hbm(w), hbm(gain), hbm(w_out))


def middle_kernel(x_hbm, own_ref, got_ref, mod_hbm, out_ref, x_ref, mod, sems):
    fetch = Fetches(sems)
    fetch.start("x", x_hbm, x_ref)
    fetch.start("mod", mod_hbm, mod)
    fetch.wait("x", "mod")
    videos, rows, _ = x_ref.shape
    peers = out_ref.shape[0]
    share = rows // peers
    mids = []
    for v in range(videos):
        total = (own_ref[v].astype(F32) + got_ref[v].astype(F32)).astype(BF16).astype(F32)
        mids.append(x_ref[v].astype(F32) + mod[2, v : v + 1, :] * total)
    for d in range(peers):
        block = jnp.concatenate([m[d * share : (d + 1) * share] for m in mids], axis=0)
        out_ref[d] = block.astype(BF16)


def middle(x_own, own, got, mod, peers):
    videos, rows, width = x_own.shape
    return pl.pallas_call(
        middle_kernel,
        out_shape=jax.ShapeDtypeStruct((peers, videos * rows // peers, width), BF16),
        in_specs=[HBM, VMEM, VMEM, HBM],
        out_specs=VMEM,
        scratch_shapes=[
            pltpu.VMEM(x_own.shape, BF16),
            pltpu.VMEM(mod.shape, F32),
            pltpu.SemaphoreType.DMA((2,)),
        ],
        compiler_params=pltpu.CompilerParams(vmem_limit_bytes=16 * MIB),
        cost_estimate=pl.CostEstimate(flops=10**8, transcendentals=0, bytes_accessed=10**6),
        name="middle",
    )(hbm(x_own), own, got, hbm(mod))


def late_kernel(
    head_dim, x_hbm, mod_hbm, qo_hbm, qr_hbm, gain_hbm, oo_hbm, or_hbm, io_hbm, ir_hbm, fo_hbm, fr_hbm, out_ref,
    x_ref, mod, gain, w_ref, o_ref, i_ref, f_ref, n_ref, r_ref, q_ref, k_ref, v_ref, s_ref, p_ref, a_ref, h_ref, sems,
):
    frames, group, _ = x_hbm.shape
    videos = mod_hbm.shape[1]
    share = group // videos
    tokens = frames * group
    heads = q_ref.shape[0]
    inner = w_ref.shape[2]
    half = heads // 2
    fetch = Fetches(sems)
    q_hbms, o_hbms, i_hbms, f_hbms = (qo_hbm, qr_hbm), (oo_hbm, or_hbm), (io_hbm, ir_hbm), (fo_hbm, fr_hbm)

    def fetch_heads(which):
        for side in range(2):
            fetch.start((which, side), q_hbms[side].at[which], w_ref.at[side, which])

    fetch.start("x", x_hbm, x_ref)
    fetch.start("mod", mod_hbm, mod)
    fetch.start("gain", gain_hbm, gain)
    fetch_heads(0)
    fetch_heads(1)
    fetch.wait("x", "mod", "gain")

    def video_rows(v):
        picked = [x_ref[f].astype(F32)[v * share : (v + 1) * share] for f in range(frames)]
        return jnp.concatenate(picked, axis=0)

    each = frames * share
    for v in range(videos):
        normed = norm_rows(video_rows(v)) * (1.0 + mod[4, v : v + 1, :]) + mod[3, v : v + 1, :]
        n_ref[v * each : (v + 1) * each, :] = normed.astype(BF16)
    factor = math.log2(math.e) / math.sqrt(head_dim)
    columns = [column(gain[which : which + 1, :]) for which in range(2)]
    for which, target in enumerate((q_ref, k_ref, v_ref)):
        fetch.wait((which, 0), (which, 1))
        if which == 0:
            fetch_heads(2)
        elif which == 1:
            fetch.start("out0", o_hbms[0], o_ref.at[0])
            fetch.start("out1", o_hbms[1], o_ref.at[1])
            fetch.start("in0", i_hbms[0], i_ref.at[0])
        else:
            fetch.start("in1", i_hbms[1], i_ref.at[1])
            fetch.start("down0", f_hbms[0], f_ref.at[0])
        for side in range(2):
            projected = mm(w_ref[side, which], n_ref[...], NT)
            projected = projected.reshape(half, head_dim, tokens)
            if which < 2:
                projected = head_norm(projected, columns[which] * factor if which == 0 else columns[which])
            else:
                projected = with_ones(projected)
            target[side * half : (side + 1) * half] = projected.astype(BF16)
    for h in range(heads):
        for v in range(videos):
            cols = slice(v * each, (v + 1) * each)
            s_ref[h, v] = mm(k_ref[h, :, cols], q_ref[h, :, cols], TN)
    first = lax.broadcasted_iota(jnp.int32, (share, each), 0)
    second = lax.broadcasted_iota(jnp.int32, (share, each), 1)
    same = (first == lax.rem(second, share))[None]
    for h in range(heads):
        for v in range(videos):
            weights = jnp.exp2(s_ref[h, v]).reshape(frames, share, each)
            p_ref[h, v] = jnp.where(same, weights, 0.0).reshape(each, each).astype(BF16)
    for h in range(0, heads, 2):
        for v in range(videos):
            cols = slice(v * each, (v + 1) * each)
            pair = [
                normalized(mm(v_ref[g, :, cols], p_ref[g, v], NN), head_dim) for g in (h, h + 1)
            ]
            a_ref[h * head_dim : (h + 2) * head_dim, cols] = jnp.concatenate(pair, axis=0).astype(BF16)
    fetch.wait("out0", "out1")
    fetch.start("down1", f_hbms[1], f_ref.at[1])
    total = None
    for side in range(2):
        part = mm(a_ref[side * inner : (side + 1) * inner, :], o_ref[side], TN)
        part = part.astype(BF16).astype(F32)
        total = part if total is None else total + part
    total = total.astype(BF16).astype(F32)
    for v in range(videos):
        there = slice(v * each, (v + 1) * each)
        running = video_rows(v) + mod[5, v : v + 1, :] * total[there]
        r_ref[there, :] = running
        normed = norm_rows(running) * (1.0 + mod[7, v : v + 1, :]) + mod[6, v : v + 1, :]
        n_ref[there, :] = normed.astype(BF16)
    fetch.wait("in0", "in1")
    hidden_width = i_ref.shape[2]
    chunk = hidden_width // 3 if hidden_width % 384 == 0 else hidden_width
    for side in range(2):
        for start in range(0, hidden_width, chunk):
            u = mm(n_ref[...], i_ref[side, :, start : start + chunk], NN)
            h_ref[side, :, start : start + chunk] = jax.nn.gelu(u, approximate=True).astype(BF16)
    fetch.wait("down0", "down1")
    mlp = None
    for side in range(2):
        part = mm(h_ref[side], f_ref[side], NN).astype(BF16).astype(F32)
        mlp = part if mlp is None else mlp + part
    mlp = mlp.astype(BF16).astype(F32)
    results = []
    for v in range(videos):
        there = slice(v * each, (v + 1) * each)
        results.append(r_ref[there, :] + mod[8, v : v + 1, :] * mlp[there])
    for f in range(frames):
        block = [r[f * share : (f + 1) * share] for r in results]
        out_ref[f] = jnp.concatenate(block, axis=0).astype(BF16)


def late(x, mod, q_own, q_rem, gain, o_own, o_rem, i_own, i_rem, f_own, f_rem, head_dim):
    frames, group, width = x.shape
    tokens = frames * group
    inner = q_own.shape[1]
    heads = 2 * inner // head_dim
    videos = mod.shape[1]
    return pl.pallas_call(
        functools.partial(late_kernel, head_dim),
        out_shape=jax.ShapeDtypeStruct(x.shape, BF16),
        in_specs=[HBM] * 11,
        out_specs=VMEM,
        scratch_shapes=[
            pltpu.VMEM(x.shape, BF16),
            pltpu.VMEM(mod.shape, F32),
            pltpu.VMEM(gain.shape, F32),
            pltpu.VMEM((2,) + q_own.shape, BF16),
            pltpu.VMEM((2,) + o_own.shape, BF16),
            pltpu.VMEM((2,) + i_own.shape, BF16),
            pltpu.VMEM((2,) + f_own.shape, BF16),
            pltpu.VMEM((tokens, width), BF16),
            pltpu.VMEM((tokens, width), F32),
            pltpu.VMEM((heads, head_dim, tokens), BF16),
            pltpu.VMEM((heads, head_dim, tokens), BF16),
            pltpu.VMEM((heads, padded_rows(head_dim), tokens), BF16),
            pltpu.VMEM((heads, videos, tokens // videos, tokens // videos), F32),
            pltpu.VMEM((heads, videos, tokens // videos, tokens // videos), BF16),
            pltpu.VMEM((2 * inner, tokens), BF16),
            pltpu.VMEM((2, tokens, i_own.shape[1]), BF16),
            pltpu.SemaphoreType.DMA((15,)),
        ],
        compiler_params=pltpu.CompilerParams(vmem_limit_bytes=52 * MIB),
        cost_estimate=pl.CostEstimate(flops=9 * 10**9, transcendentals=2 * 10**6, bytes_accessed=33 * 10**6),
        name="late",
    )(x, *(hbm(v) for v in (mod, q_own, q_rem, gain, o_own, o_rem, i_own, i_rem, f_own, f_rem)))


def paired_body(
    seq_size,
    latent,
    modulation,
    qkv_spatial,
    gain_spatial,
    out_spatial,
    qkv_temporal,
    gain_temporal,
    out_temporal,
    fc_in,
    fc_out,
):
    head_dim = gain_spatial.shape[-1]
    videos, _, rows, width = latent.shape

    def swap(value):
        return lax.ppermute(value, "tp", [(0, 1), (1, 0)])

    x_own = latent.reshape(videos, rows, width)
    w_spatial = jnp.swapaxes(qkv_spatial, 1, 2)
    w_temporal = jnp.swapaxes(qkv_temporal, 1, 2)
    modulation = jnp.swapaxes(modulation, 0, 1)
    x_oth = swap(x_own)
    x_oth, w_sent, o_sent = lax.optimization_barrier((x_oth, w_temporal, out_temporal))
    q_rem = swap(w_sent)
    o_rem = swap(o_sent)
    own, other = spatial(x_own, x_oth, modulation, w_spatial, gain_spatial, out_spatial, head_dim)
    got = swap(other)
    got, i_sent, f_sent = lax.optimization_barrier((got, fc_in, fc_out))
    i_rem = swap(i_sent)
    f_rem = swap(f_sent)
    mid = middle(x_own, own, got, modulation, seq_size)
    moved = lax.all_to_all(mid, "seq", 0, 0, tiled=True)
    done = late(
        moved, modulation, w_temporal, q_rem, gain_temporal, out_temporal, o_rem,
        fc_in, i_rem, fc_out, f_rem, head_dim,
    )
    back = lax.all_to_all(done, "seq", 0, 0, tiled=True)
    back = back.reshape(seq_size, videos, rows // seq_size, width).transpose(1, 0, 2, 3)
    return back.reshape(latent.shape)


def layer_norm(values):
    average = jnp.mean(values, axis=-1, keepdims=True)
    centred = values - average
    variance = jnp.mean(centred * centred, axis=-1, keepdims=True)
    return centred * lax.rsqrt(variance + epsilon)


def modulated(field, modulation, offset):
    shift_row = modulation[:, offset][:, None, None, :]
    scale_row = modulation[:, offset + 1][:, None, None, :]
    return (layer_norm(field) * (1.0 + scale_row) + shift_row).astype(jnp.bfloat16)


def project_heads(rows_piece, table, gains, head_dim):
    results = []
    for which_part in range(3):
        projected = jnp.einsum(
            "bfpd,de->bfpe", rows_piece, table[which_part], preferred_element_type=jnp.float32
        )
        if which_part < 2:
            shaped = projected.reshape(
                projected.shape[:-1] + (projected.shape[-1] // head_dim, head_dim)
            )
            shaped = (
                shaped
                * lax.rsqrt(jnp.mean(shaped * shaped, axis=-1, keepdims=True) + epsilon)
                * gains[which_part]
            )
            projected = shaped.reshape(projected.shape)
        results.append(projected.astype(jnp.bfloat16))
    return jnp.stack(results)


def attend(query_rows, key_rows, value_rows, head_dim):
    groups, length, feature_width = query_rows.shape
    head_count = feature_width // head_dim
    query_heads = query_rows.reshape(groups, length, head_count, head_dim)
    key_heads = key_rows.reshape(groups, length, head_count, head_dim)
    value_heads = value_rows.reshape(groups, length, head_count, head_dim)
    block_rows = min(length, 512)

    def one_block(first_row):
        query_block = lax.dynamic_slice_in_dim(query_heads, first_row, block_rows, 1)
        scores = jnp.einsum(
            "gqhe,gkhe->ghqk", query_block, key_heads, preferred_element_type=jnp.float32
        ) / math.sqrt(head_dim)
        weights = jnp.exp(scores)
        probabilities = (weights / jnp.sum(weights, axis=-1, keepdims=True)).astype(jnp.bfloat16)
        return jnp.einsum(
            "ghqk,gkhe->gqhe", probabilities, value_heads, preferred_element_type=jnp.float32
        ).astype(jnp.bfloat16)

    starts = jnp.arange(length // block_rows, dtype=jnp.int32) * block_rows
    pieces = lax.map(one_block, starts)
    return pieces.transpose(1, 0, 2, 3, 4).reshape(groups, length, feature_width)


def frame_attention(query_rows, key_rows, value_rows, head_dim):
    batches, frames, patches, feature_width = query_rows.shape
    members = [
        item.transpose(0, 2, 1, 3).reshape(batches * patches, frames, feature_width)
        for item in (query_rows, key_rows, value_rows)
    ]
    mixed_heads = attend(members[0], members[1], members[2], head_dim)
    return mixed_heads.reshape(batches, patches, frames, feature_width).transpose(0, 2, 1, 3)


def body(
    latent,
    modulation,
    qkv_spatial,
    gain_spatial,
    out_spatial,
    qkv_temporal,
    gain_temporal,
    out_temporal,
    fc_in,
    fc_out,
):
    head_dim = gain_spatial.shape[-1]
    running = latent.astype(jnp.float32)
    normed = modulated(running, modulation, 0)
    packed = project_heads(
        lax.all_gather(normed, "tp", axis=2, tiled=True), qkv_spatial, gain_spatial, head_dim
    )
    batches, frames, patches, local_width = packed.shape[1:]
    mixed_heads = attend(
        packed[0].reshape(batches * frames, patches, local_width),
        packed[1].reshape(batches * frames, patches, local_width),
        packed[2].reshape(batches * frames, patches, local_width),
        head_dim,
    )
    mixed_heads = mixed_heads.reshape(batches, frames, patches, local_width)
    partial_value = jnp.einsum(
        "bfpe,ed->bfpd", mixed_heads, out_spatial, preferred_element_type=jnp.float32
    )
    spatial_out = lax.psum_scatter(
        partial_value.astype(jnp.bfloat16), "tp", scatter_dimension=2, tiled=True
    )
    running = running + modulation[:, 2][:, None, None, :] * spatial_out.astype(jnp.float32)
    normed = modulated(running, modulation, 3)
    moved_rows = lax.all_to_all(normed, "seq", split_axis=2, concat_axis=1, tiled=True)
    packed = project_heads(
        lax.all_gather(moved_rows, "tp", axis=2, tiled=True), qkv_temporal, gain_temporal, head_dim
    )
    mixed_heads = frame_attention(packed[0], packed[1], packed[2], head_dim)
    partial_value = jnp.einsum(
        "bfpe,ed->bfpd", mixed_heads, out_temporal, preferred_element_type=jnp.float32
    )
    shares = lax.psum_scatter(
        partial_value.astype(jnp.bfloat16), "tp", scatter_dimension=2, tiled=True
    )
    temporal_out = lax.all_to_all(shares, "seq", split_axis=1, concat_axis=2, tiled=True)
    running = running + modulation[:, 5][:, None, None, :] * temporal_out.astype(jnp.float32)
    normed = modulated(running, modulation, 6)
    projected = jnp.einsum(
        "bfpd,de->bfpe",
        lax.all_gather(normed, "tp", axis=2, tiled=True),
        fc_in,
        preferred_element_type=jnp.float32,
    )
    hidden = jax.nn.gelu(projected, approximate=True).astype(jnp.bfloat16)
    partial_value = jnp.einsum("bfpe,ed->bfpd", hidden, fc_out, preferred_element_type=jnp.float32)
    mlp_out = lax.psum_scatter(
        partial_value.astype(jnp.bfloat16), "tp", scatter_dimension=2, tiled=True
    )
    return (running + modulation[:, 8][:, None, None, :] * mlp_out.astype(jnp.float32)).astype(
        jnp.bfloat16
    )


def fits(mesh, local_frames, local_rows, heads_here):
    return (
        mesh.shape["tp"] == 2
        and local_frames == 1
        and local_rows % (8 * mesh.shape["seq"]) == 0
        and heads_here % 2 == 0
    )


def solution(mesh):
    placed = (
        P(None, "seq", "tp", None),
        P(),
        P(None, None, "tp"),
        P(),
        P("tp", None),
        P(None, None, "tp"),
        P(),
        P("tp", None),
        P(None, "tp"),
        P("tp", None),
    )

    def step(*args):
        latent, qkv, gain = args[0], args[2], args[3]
        if fits(mesh, latent.shape[1], latent.shape[2], qkv.shape[2] // gain.shape[1]):
            return paired_body(mesh.shape["seq"], *args)
        return body(*args)

    return jax.shard_map(
        step, mesh=mesh, in_specs=placed, out_specs=P(None, "seq", "tp", None), check_vma=False
    )
```

```python
import functools
import math

import jax
import jax.numpy as jnp
from jax import lax
from jax.experimental import pallas as pl
from jax.experimental.pallas import tpu as pltpu
from jax.sharding import PartitionSpec as P


epsilon = 1e-06
F32 = jnp.float32
BF16 = jnp.bfloat16
VMEM = pl.BlockSpec(memory_space=pltpu.VMEM)
HBM = pl.BlockSpec(memory_space=pltpu.HBM)

MIB = 1 << 20

NT = (((1,), (1,)), ((), ()))
TN = (((0,), (0,)), ((), ()))
NN = (((1,), (0,)), ((), ()))


def mm(a, b, dims):
    return lax.dot_general(a, b, dims, preferred_element_type=F32)


def hbm(value):
    return pltpu.with_memory_space_constraint(value, pltpu.HBM)


class Fetches:
    def __init__(self, sems):
        self.sems, self.made = sems, {}

    def start(self, name, source, target):
        copy = pltpu.make_async_copy(source, target, self.sems.at[len(self.made)])
        copy.start()
        self.made[name] = copy

    def wait(self, *names):
        for name in names:
            self.made[name].wait()


def norm_rows(values):
    average = jnp.mean(values, axis=-1, keepdims=True)
    centred = values - average
    variance = jnp.mean(centred * centred, axis=-1, keepdims=True)
    return centred * lax.rsqrt(variance + epsilon)


def column(row):
    n = row.shape[1]
    diagonal = lax.broadcasted_iota(jnp.int32, (n, n), 0) == lax.broadcasted_iota(jnp.int32, (n, n), 1)
    return jnp.sum(jnp.where(diagonal, row, 0.0), axis=1, keepdims=True)


def head_norm(projected, gain):
    mean_square = jnp.mean(projected * projected, axis=1, keepdims=True)
    return projected * lax.rsqrt(mean_square + epsilon) * gain[None]


def padded_rows(head_dim):
    return -(-(head_dim + 1) // 16) * 16


def with_ones(values):
    heads, head_dim, tokens = values.shape
    extra = padded_rows(head_dim) - head_dim
    place = lax.broadcasted_iota(jnp.int32, (heads, extra, tokens), 1)
    return jnp.concatenate([values, jnp.where(place == 0, 1.0, 0.0)], axis=1)


def normalized(mixed, head_dim):
    return mixed[:head_dim] * (1.0 / mixed[head_dim : head_dim + 1])


def spatial_kernel(
    head_dim, own_hbm, oth_hbm, mod_hbm, w_hbm, gain_hbm, o_hbm, part_own, part_oth, x_out, gate_out,
    x_own, x_oth, mod, gain, w_ref, o_ref, n_ref, q_ref, k_ref, v_ref, s_ref, p_ref, a_ref, sems,
):
    videos, rows, _ = part_own.shape
    patches = 2 * rows
    heads = w_ref.shape[1] // head_dim
    fetch = Fetches(sems)
    fetch.start("own", own_hbm, x_own)
    fetch.start("mod", mod_hbm, mod)
    fetch.start("oth", oth_hbm, x_oth)
    fetch.start("gain", gain_hbm, gain)
    for which in range(3):
        fetch.start(which, w_hbm.at[which], w_ref.at[which])
    fetch.start("out", o_hbm, o_ref)
    block = 16 if rows % 16 == 0 else rows
    fetch.wait("own", "mod", "gain")
    x_out[...] = x_own[...]
    gate_out[...] = mod[2]
    for v in range(videos):
        for place, source in enumerate((x_own, x_oth)):
            if v == 0 and place == 1:
                fetch.wait("oth")
            base = v * patches + place * rows
            for start in range(0, rows, block):
                normed = norm_rows(source[v, start : start + block].astype(F32))
                normed = normed * (1.0 + mod[1, v : v + 1, :]) + mod[0, v : v + 1, :]
                n_ref[base + start : base + start + block, :] = normed.astype(BF16)
    factor = math.log2(math.e) / math.sqrt(head_dim)
    for which, target in enumerate((q_ref, k_ref, v_ref)):
        fetch.wait(which)
        projected = mm(w_ref[which], n_ref[...], NT)
        projected = projected.reshape(heads, head_dim, videos * patches)
        if which < 2:
            gains = column(gain[which : which + 1, :])
            projected = head_norm(projected, gains * factor if which == 0 else gains)
        else:
            projected = with_ones(projected)
        target[...] = projected.astype(BF16)
    for v in range(videos):
        cols = slice(v * patches, (v + 1) * patches)
        for h in range(heads):
            s_ref[v, h] = mm(k_ref[h, :, cols], q_ref[h, :, cols], TN)
    for v in range(videos):
        for h in range(heads):
            p_ref[v, h] = jnp.exp2(s_ref[v, h]).astype(BF16)
    for v in range(videos):
        cols = slice(v * patches, (v + 1) * patches)
        for h in range(0, heads, 2):
            pair = [
                normalized(mm(v_ref[g, :, cols], p_ref[v, g], NN), head_dim) for g in (h, h + 1)
            ]
            a_ref[v, h * head_dim : (h + 2) * head_dim, :] = jnp.concatenate(pair, axis=0).astype(BF16)
    fetch.wait("out")
    for v in range(videos):
        part = mm(a_ref[v], o_ref[...], TN).astype(BF16)
        part_own[v] = part[:rows]
        part_oth[v] = part[rows:]


def spatial(x_own, x_oth, mod, w, gain, w_out, head_dim):
    videos, rows, width = x_own.shape
    inner = w.shape[1]
    heads = inner // head_dim
    tokens = 2 * rows * videos
    return pl.pallas_call(
        functools.partial(spatial_kernel, head_dim),
        out_shape=[jax.ShapeDtypeStruct((videos, rows, width), BF16)] * 3
        + [jax.ShapeDtypeStruct((videos, width), F32)],
        in_specs=[HBM] * 6,
        out_specs=[VMEM] * 4,
        scratch_shapes=[
            pltpu.VMEM(x_own.shape, BF16),
            pltpu.VMEM(x_own.shape, BF16),
            pltpu.VMEM(mod.shape, F32),
            pltpu.VMEM(gain.shape, F32),
            pltpu.VMEM(w.shape, BF16),
            pltpu.VMEM(w_out.shape, BF16),
            pltpu.VMEM((tokens, width), BF16),
            pltpu.VMEM((heads, head_dim, tokens), BF16),
            pltpu.VMEM((heads, head_dim, tokens), BF16),
            pltpu.VMEM((heads, padded_rows(head_dim), tokens), BF16),
            pltpu.VMEM((videos, heads, 2 * rows, 2 * rows), F32),
            pltpu.VMEM((videos, heads, 2 * rows, 2 * rows), BF16),
            pltpu.VMEM((videos, inner, 2 * rows), BF16),
            pltpu.SemaphoreType.DMA((8,)),
        ],
        compiler_params=pltpu.CompilerParams(vmem_limit_bytes=28 * MIB),
        cost_estimate=pl.CostEstimate(flops=6 * 10**9, transcendentals=10**6, bytes_accessed=8 * 10**6),
        name="spatial",
    )(hbm(x_own), x_oth, hbm(mod), hbm(w), hbm(gain), hbm(w_out))


def middle_kernel(x_ref, own_ref, got_ref, gate_ref, out_ref):
    videos = x_ref.shape[0]
    peers, group, _ = out_ref.shape
    share = group // videos
    for d in range(peers):
        there = slice(d * share, (d + 1) * share)
        parts = []
        for v in range(videos):
            total = own_ref[v, there].astype(F32) + got_ref[v, there].astype(F32)
            total = total.astype(BF16).astype(F32)
            parts.append(x_ref[v, there].astype(F32) + gate_ref[v : v + 1, :] * total)
        out_ref[d] = jnp.concatenate(parts, axis=0).astype(BF16)


def middle(x_own, own, got, gate, peers):
    videos, rows, width = x_own.shape
    return pl.pallas_call(
        middle_kernel,
        out_shape=jax.ShapeDtypeStruct((peers, videos * rows // peers, width), BF16),
        in_specs=[VMEM] * 4,
        out_specs=VMEM,
        compiler_params=pltpu.CompilerParams(vmem_limit_bytes=16 * MIB),
        cost_estimate=pl.CostEstimate(flops=10**8, transcendentals=0, bytes_accessed=10**6),
        name="middle",
    )(x_own, own, got, gate)


def late_kernel(
    head_dim, x_hbm, mod_hbm, qo_hbm, qr_hbm, gain_hbm, oo_hbm, or_hbm, io_hbm, ir_hbm, fo_hbm, fr_hbm, out_ref,
    x_ref, mod, gain, w_ref, o_ref, i_ref, f_ref, n_ref, r_ref, q_ref, k_ref, v_ref, s_ref, p_ref, a_ref, h_ref, sems,
):
    frames, group, _ = x_hbm.shape
    videos = mod_hbm.shape[1]
    share = group // videos
    tokens = frames * group
    heads = q_ref.shape[0]
    inner = w_ref.shape[2]
    half = heads // 2
    fetch = Fetches(sems)
    q_hbms, o_hbms, i_hbms, f_hbms = (qo_hbm, qr_hbm), (oo_hbm, or_hbm), (io_hbm, ir_hbm), (fo_hbm, fr_hbm)

    def fetch_heads(which):
        for side in range(2):
            fetch.start((which, side), q_hbms[side].at[which], w_ref.at[side, which])

    fetch.start("x", x_hbm, x_ref)
    fetch.start("mod", mod_hbm, mod)
    fetch.start("gain", gain_hbm, gain)
    fetch_heads(0)
    fetch.wait("x", "mod", "gain")
    fetch_heads(1)

    each = frames * share
    step = 2 if frames % 2 == 0 else 1

    def pieces():
        for v in range(videos):
            for f in range(0, frames, step):
                rows = [x_ref[f + i].astype(F32)[v * share : (v + 1) * share] for i in range(step)]
                start = v * each + f * share
                yield v, slice(start, start + step * share), jnp.concatenate(rows, axis=0)

    for v, rows, values in pieces():
        normed = norm_rows(values) * (1.0 + mod[4, v : v + 1, :]) + mod[3, v : v + 1, :]
        n_ref[rows, :] = normed.astype(BF16)
    factor = math.log2(math.e) / math.sqrt(head_dim)
    columns = [column(gain[which : which + 1, :]) for which in range(2)]
    for which, target in enumerate((q_ref, k_ref, v_ref)):
        if which == 0:
            fetch.wait((0, 0), (0, 1))
            fetch_heads(2)
            fetch.start("out0", o_hbms[0], o_ref.at[0])
            fetch.start("out1", o_hbms[1], o_ref.at[1])
        elif which == 1:
            fetch.wait((1, 0), (1, 1), (2, 0), (2, 1))
            fetch.start("in0", i_hbms[0], i_ref.at[0])
            fetch.start("in1", i_hbms[1], i_ref.at[1])
            fetch.start("down0", f_hbms[0], f_ref.at[0])
        for side in range(2):
            projected = mm(w_ref[side, which], n_ref[...], NT)
            projected = projected.reshape(half, head_dim, tokens)
            if which < 2:
                projected = head_norm(projected, columns[which] * factor if which == 0 else columns[which])
            else:
                projected = with_ones(projected)
            target[side * half : (side + 1) * half] = projected.astype(BF16)
    for h in range(heads):
        for v in range(videos):
            cols = slice(v * each, (v + 1) * each)
            s_ref[h, v] = mm(k_ref[h, :, cols], q_ref[h, :, cols], TN)
    first = lax.broadcasted_iota(jnp.int32, (share, each), 0)
    second = lax.broadcasted_iota(jnp.int32, (share, each), 1)
    same = (first == lax.rem(second, share))[None]
    for h in range(heads):
        for v in range(videos):
            weights = jnp.exp2(s_ref[h, v]).reshape(frames, share, each)
            p_ref[h, v] = jnp.where(same, weights, 0.0).reshape(each, each).astype(BF16)
    for h in range(0, heads, 2):
        for v in range(videos):
            cols = slice(v * each, (v + 1) * each)
            pair = [
                normalized(mm(v_ref[g, :, cols], p_ref[g, v], NN), head_dim) for g in (h, h + 1)
            ]
            a_ref[h * head_dim : (h + 2) * head_dim, cols] = jnp.concatenate(pair, axis=0).astype(BF16)
    fetch.wait("out0", "out1")
    fetch.start("down1", f_hbms[1], f_ref.at[1])
    r_ref[...] = mm(a_ref[:inner, :], o_ref[0], TN) + mm(a_ref[inner:, :], o_ref[1], TN)
    for v, rows, values in pieces():
        running = values + mod[5, v : v + 1, :] * r_ref[rows, :].astype(BF16).astype(F32)
        r_ref[rows, :] = running
        normed = norm_rows(running) * (1.0 + mod[7, v : v + 1, :]) + mod[6, v : v + 1, :]
        n_ref[rows, :] = normed.astype(BF16)
    fetch.wait("in0", "in1")
    hidden_width = i_ref.shape[2]
    chunk = hidden_width // 3 if hidden_width % 384 == 0 else hidden_width
    for side in range(2):
        for start in range(0, hidden_width, chunk):
            u = mm(n_ref[...], i_ref[side, :, start : start + chunk], NN)
            h_ref[side, :, start : start + chunk] = jax.nn.gelu(u, approximate=True).astype(BF16)
    fetch.wait("down0", "down1")
    mlp = mm(h_ref[0], f_ref[0], NN) + mm(h_ref[1], f_ref[1], NN)
    mlp = mlp.astype(BF16).astype(F32)
    for f in range(frames):
        parts = []
        for v in range(videos):
            rows = slice(v * each + f * share, v * each + (f + 1) * share)
            parts.append(r_ref[rows, :] + mod[8, v : v + 1, :] * mlp[rows])
        out_ref[f] = jnp.concatenate(parts, axis=0).astype(BF16)


def late(x, mod, q_own, q_rem, gain, o_own, o_rem, i_own, i_rem, f_own, f_rem, head_dim):
    frames, group, width = x.shape
    tokens = frames * group
    inner = q_own.shape[1]
    heads = 2 * inner // head_dim
    videos = mod.shape[1]
    return pl.pallas_call(
        functools.partial(late_kernel, head_dim),
        out_shape=jax.ShapeDtypeStruct(x.shape, BF16),
        in_specs=[HBM] * 11,
        out_specs=VMEM,
        scratch_shapes=[
            pltpu.VMEM(x.shape, BF16),
            pltpu.VMEM(mod.shape, F32),
            pltpu.VMEM(gain.shape, F32),
            pltpu.VMEM((2,) + q_own.shape, BF16),
            pltpu.VMEM((2,) + o_own.shape, BF16),
            pltpu.VMEM((2,) + i_own.shape, BF16),
            pltpu.VMEM((2,) + f_own.shape, BF16),
            pltpu.VMEM((tokens, width), BF16),
            pltpu.VMEM((tokens, width), F32),
            pltpu.VMEM((heads, head_dim, tokens), BF16),
            pltpu.VMEM((heads, head_dim, tokens), BF16),
            pltpu.VMEM((heads, padded_rows(head_dim), tokens), BF16),
            pltpu.VMEM((heads, videos, tokens // videos, tokens // videos), F32),
            pltpu.VMEM((heads, videos, tokens // videos, tokens // videos), BF16),
            pltpu.VMEM((2 * inner, tokens), BF16),
            pltpu.VMEM((2, tokens, i_own.shape[1]), BF16),
            pltpu.SemaphoreType.DMA((15,)),
        ],
        compiler_params=pltpu.CompilerParams(vmem_limit_bytes=52 * MIB),
        cost_estimate=pl.CostEstimate(flops=9 * 10**9, transcendentals=2 * 10**6, bytes_accessed=33 * 10**6),
        name="late",
    )(x, *(hbm(v) for v in (mod, q_own, q_rem, gain, o_own, o_rem, i_own, i_rem, f_own, f_rem)))


def paired_body(
    seq_size,
    latent,
    modulation,
    qkv_spatial,
    gain_spatial,
    out_spatial,
    qkv_temporal,
    gain_temporal,
    out_temporal,
    fc_in,
    fc_out,
):
    head_dim = gain_spatial.shape[-1]
    videos, _, rows, width = latent.shape

    def swap(value):
        return lax.ppermute(value, "tp", [(0, 1), (1, 0)])

    x_own = latent.reshape(videos, rows, width)
    w_spatial = jnp.swapaxes(qkv_spatial, 1, 2)
    w_temporal = jnp.swapaxes(qkv_temporal, 1, 2)
    modulation = jnp.swapaxes(modulation, 0, 1)
    x_oth = swap(x_own)
    x_oth, w_sent, o_sent = lax.optimization_barrier((x_oth, w_temporal, out_temporal))
    q_rem = swap(w_sent)
    o_rem = swap(o_sent)
    own, other, x_kept, gate = spatial(
        x_own, x_oth, modulation, w_spatial, gain_spatial, out_spatial, head_dim
    )
    got = swap(other)
    got, i_sent, f_sent = lax.optimization_barrier((got, fc_in, fc_out))
    i_rem = swap(i_sent)
    f_rem = swap(f_sent)
    mid = middle(x_kept, own, got, gate, seq_size)
    moved = lax.all_to_all(mid, "seq", 0, 0, tiled=True)
    done = late(
        moved, modulation, w_temporal, q_rem, gain_temporal, out_temporal, o_rem,
        fc_in, i_rem, fc_out, f_rem, head_dim,
    )
    back = lax.all_to_all(done, "seq", 0, 0, tiled=True)
    back = back.reshape(seq_size, videos, rows // seq_size, width).transpose(1, 0, 2, 3)
    return back.reshape(latent.shape)


def layer_norm(values):
    average = jnp.mean(values, axis=-1, keepdims=True)
    centred = values - average
    variance = jnp.mean(centred * centred, axis=-1, keepdims=True)
    return centred * lax.rsqrt(variance + epsilon)


def modulated(field, modulation, offset):
    shift_row = modulation[:, offset][:, None, None, :]
    scale_row = modulation[:, offset + 1][:, None, None, :]
    return (layer_norm(field) * (1.0 + scale_row) + shift_row).astype(jnp.bfloat16)


def project_heads(rows_piece, table, gains, head_dim):
    results = []
    for which_part in range(3):
        projected = jnp.einsum(
            "bfpd,de->bfpe", rows_piece, table[which_part], preferred_element_type=jnp.float32
        )
        if which_part < 2:
            shaped = projected.reshape(
                projected.shape[:-1] + (projected.shape[-1] // head_dim, head_dim)
            )
            shaped = (
                shaped
                * lax.rsqrt(jnp.mean(shaped * shaped, axis=-1, keepdims=True) + epsilon)
                * gains[which_part]
            )
            projected = shaped.reshape(projected.shape)
        results.append(projected.astype(jnp.bfloat16))
    return jnp.stack(results)


def attend(query_rows, key_rows, value_rows, head_dim):
    groups, length, feature_width = query_rows.shape
    head_count = feature_width // head_dim
    query_heads = query_rows.reshape(groups, length, head_count, head_dim)
    key_heads = key_rows.reshape(groups, length, head_count, head_dim)
    value_heads = value_rows.reshape(groups, length, head_count, head_dim)
    block_rows = min(length, 512)

    def one_block(first_row):
        query_block = lax.dynamic_slice_in_dim(query_heads, first_row, block_rows, 1)
        scores = jnp.einsum(
            "gqhe,gkhe->ghqk", query_block, key_heads, preferred_element_type=jnp.float32
        ) / math.sqrt(head_dim)
        weights = jnp.exp(scores)
        probabilities = (weights / jnp.sum(weights, axis=-1, keepdims=True)).astype(jnp.bfloat16)
        return jnp.einsum(
            "ghqk,gkhe->gqhe", probabilities, value_heads, preferred_element_type=jnp.float32
        ).astype(jnp.bfloat16)

    starts = jnp.arange(length // block_rows, dtype=jnp.int32) * block_rows
    pieces = lax.map(one_block, starts)
    return pieces.transpose(1, 0, 2, 3, 4).reshape(groups, length, feature_width)


def frame_attention(query_rows, key_rows, value_rows, head_dim):
    batches, frames, patches, feature_width = query_rows.shape
    members = [
        item.transpose(0, 2, 1, 3).reshape(batches * patches, frames, feature_width)
        for item in (query_rows, key_rows, value_rows)
    ]
    mixed_heads = attend(members[0], members[1], members[2], head_dim)
    return mixed_heads.reshape(batches, patches, frames, feature_width).transpose(0, 2, 1, 3)


def body(
    latent,
    modulation,
    qkv_spatial,
    gain_spatial,
    out_spatial,
    qkv_temporal,
    gain_temporal,
    out_temporal,
    fc_in,
    fc_out,
):
    head_dim = gain_spatial.shape[-1]
    running = latent.astype(jnp.float32)
    normed = modulated(running, modulation, 0)
    packed = project_heads(
        lax.all_gather(normed, "tp", axis=2, tiled=True), qkv_spatial, gain_spatial, head_dim
    )
    batches, frames, patches, local_width = packed.shape[1:]
    mixed_heads = attend(
        packed[0].reshape(batches * frames, patches, local_width),
        packed[1].reshape(batches * frames, patches, local_width),
        packed[2].reshape(batches * frames, patches, local_width),
        head_dim,
    )
    mixed_heads = mixed_heads.reshape(batches, frames, patches, local_width)
    partial_value = jnp.einsum(
        "bfpe,ed->bfpd", mixed_heads, out_spatial, preferred_element_type=jnp.float32
    )
    spatial_out = lax.psum_scatter(
        partial_value.astype(jnp.bfloat16), "tp", scatter_dimension=2, tiled=True
    )
    running = running + modulation[:, 2][:, None, None, :] * spatial_out.astype(jnp.float32)
    normed = modulated(running, modulation, 3)
    moved_rows = lax.all_to_all(normed, "seq", split_axis=2, concat_axis=1, tiled=True)
    packed = project_heads(
        lax.all_gather(moved_rows, "tp", axis=2, tiled=True), qkv_temporal, gain_temporal, head_dim
    )
    mixed_heads = frame_attention(packed[0], packed[1], packed[2], head_dim)
    partial_value = jnp.einsum(
        "bfpe,ed->bfpd", mixed_heads, out_temporal, preferred_element_type=jnp.float32
    )
    shares = lax.psum_scatter(
        partial_value.astype(jnp.bfloat16), "tp", scatter_dimension=2, tiled=True
    )
    temporal_out = lax.all_to_all(shares, "seq", split_axis=1, concat_axis=2, tiled=True)
    running = running + modulation[:, 5][:, None, None, :] * temporal_out.astype(jnp.float32)
    normed = modulated(running, modulation, 6)
    projected = jnp.einsum(
        "bfpd,de->bfpe",
        lax.all_gather(normed, "tp", axis=2, tiled=True),
        fc_in,
        preferred_element_type=jnp.float32,
    )
    hidden = jax.nn.gelu(projected, approximate=True).astype(jnp.bfloat16)
    partial_value = jnp.einsum("bfpe,ed->bfpd", hidden, fc_out, preferred_element_type=jnp.float32)
    mlp_out = lax.psum_scatter(
        partial_value.astype(jnp.bfloat16), "tp", scatter_dimension=2, tiled=True
    )
    return (running + modulation[:, 8][:, None, None, :] * mlp_out.astype(jnp.float32)).astype(
        jnp.bfloat16
    )


def fits(mesh, local_frames, local_rows, heads_here):
    return (
        mesh.shape["tp"] == 2
        and local_frames == 1
        and local_rows % (8 * mesh.shape["seq"]) == 0
        and heads_here % 2 == 0
    )


def solution(mesh):
    placed = (
        P(None, "seq", "tp", None),
        P(),
        P(None, None, "tp"),
        P(),
        P("tp", None),
        P(None, None, "tp"),
        P(),
        P("tp", None),
        P(None, "tp"),
        P("tp", None),
    )

    def step(*args):
        latent, qkv, gain = args[0], args[2], args[3]
        if fits(mesh, latent.shape[1], latent.shape[2], qkv.shape[2] // gain.shape[1]):
            return paired_body(mesh.shape["seq"], *args)
        return body(*args)

    return jax.shard_map(
        step, mesh=mesh, in_specs=placed, out_specs=P(None, "seq", "tp", None), check_vma=False
    )
```

```python
import functools
import math

import jax
import jax.numpy as jnp
from jax import lax
from jax.experimental import pallas as pl
from jax.experimental.pallas import tpu as pltpu
from jax.sharding import PartitionSpec as P


epsilon = 1e-06
F32 = jnp.float32
BF16 = jnp.bfloat16
VMEM = pl.BlockSpec(memory_space=pltpu.VMEM)
HBM = pl.BlockSpec(memory_space=pltpu.HBM)

MIB = 1 << 20

NT = (((1,), (1,)), ((), ()))
TN = (((0,), (0,)), ((), ()))
NN = (((1,), (0,)), ((), ()))


def mm(a, b, dims):
    return lax.dot_general(a, b, dims, preferred_element_type=F32)


def hbm(value):
    return pltpu.with_memory_space_constraint(value, pltpu.HBM)


class Fetches:
    def __init__(self, sems):
        self.sems, self.made = sems, {}

    def start(self, name, source, target):
        copy = pltpu.make_async_copy(source, target, self.sems.at[len(self.made)])
        copy.start()
        self.made[name] = copy

    def wait(self, *names):
        for name in names:
            self.made[name].wait()


def norm_rows(values):
    average = jnp.mean(values, axis=-1, keepdims=True)
    centred = values - average
    variance = jnp.mean(centred * centred, axis=-1, keepdims=True)
    return centred * lax.rsqrt(variance + epsilon)


def column(row):
    n = row.shape[1]
    diagonal = lax.broadcasted_iota(jnp.int32, (n, n), 0) == lax.broadcasted_iota(jnp.int32, (n, n), 1)
    return jnp.sum(jnp.where(diagonal, row, 0.0), axis=1, keepdims=True)


def head_norm(projected, gain):
    mean_square = jnp.mean(projected * projected, axis=1, keepdims=True)
    return projected * lax.rsqrt(mean_square + epsilon) * gain[None]


def padded_rows(head_dim):
    return -(-(head_dim + 1) // 16) * 16


def with_ones(values):
    heads, head_dim, tokens = values.shape
    extra = padded_rows(head_dim) - head_dim
    place = lax.broadcasted_iota(jnp.int32, (heads, extra, tokens), 1)
    return jnp.concatenate([values, jnp.where(place == 0, 1.0, 0.0)], axis=1)


def normalized(mixed, head_dim):
    return mixed[:head_dim] * (1.0 / mixed[head_dim : head_dim + 1])


def spatial_kernel(
    head_dim, own_hbm, oth_hbm, mod_hbm, w_hbm, gain_hbm, o_hbm, part_own, part_oth, x_out, gate_out,
    x_own, x_oth, mod, gain, w_ref, o_ref, n_ref, q_ref, k_ref, v_ref, s_ref, p_ref, a_ref, sems,
):
    videos, rows, _ = part_own.shape
    patches = 2 * rows
    heads = w_ref.shape[1] // head_dim
    fetch = Fetches(sems)
    fetch.start("own", own_hbm, x_own)
    fetch.start("mod", mod_hbm, mod)
    fetch.start("oth", oth_hbm, x_oth)
    fetch.start("gain", gain_hbm, gain)
    for which in range(3):
        fetch.start(which, w_hbm.at[which], w_ref.at[which])
    fetch.start("out", o_hbm, o_ref)
    block = 16 if rows % 16 == 0 else rows
    fetch.wait("own", "mod", "gain")
    x_out[...] = x_own[...]
    gate_out[...] = mod[2]
    for v in range(videos):
        for place, source in enumerate((x_own, x_oth)):
            if v == 0 and place == 1:
                fetch.wait("oth")
            base = v * patches + place * rows
            for start in range(0, rows, block):
                normed = norm_rows(source[v, start : start + block].astype(F32))
                normed = normed * (1.0 + mod[1, v : v + 1, :]) + mod[0, v : v + 1, :]
                n_ref[base + start : base + start + block, :] = normed.astype(BF16)
    factor = math.log2(math.e) / math.sqrt(head_dim)
    for which, target in enumerate((q_ref, k_ref, v_ref)):
        fetch.wait(which)
        projected = mm(w_ref[which], n_ref[...], NT)
        projected = projected.reshape(heads, head_dim, videos * patches)
        if which < 2:
            gains = column(gain[which : which + 1, :])
            projected = head_norm(projected, gains * factor if which == 0 else gains)
        else:
            projected = with_ones(projected)
        target[...] = projected.astype(BF16)
    for v in range(videos):
        cols = slice(v * patches, (v + 1) * patches)
        for h in range(heads):
            s_ref[v, h] = mm(k_ref[h, :, cols], q_ref[h, :, cols], TN)
    for v in range(videos):
        for h in range(heads):
            p_ref[v, h] = jnp.exp2(s_ref[v, h]).astype(BF16)
    for v in range(videos):
        cols = slice(v * patches, (v + 1) * patches)
        for h in range(0, heads, 2):
            pair = [
                normalized(mm(v_ref[g, :, cols], p_ref[v, g], NN), head_dim) for g in (h, h + 1)
            ]
            a_ref[v, h * head_dim : (h + 2) * head_dim, :] = jnp.concatenate(pair, axis=0).astype(BF16)
    fetch.wait("out")
    for v in range(videos):
        part = mm(a_ref[v], o_ref[...], TN).astype(BF16)
        part_own[v] = part[:rows]
        part_oth[v] = part[rows:]


def spatial(x_own, x_oth, mod, w, gain, w_out, head_dim):
    videos, rows, width = x_own.shape
    inner = w.shape[1]
    heads = inner // head_dim
    tokens = 2 * rows * videos
    return pl.pallas_call(
        functools.partial(spatial_kernel, head_dim),
        out_shape=[jax.ShapeDtypeStruct((videos, rows, width), BF16)] * 3
        + [jax.ShapeDtypeStruct((videos, width), F32)],
        in_specs=[HBM] * 6,
        out_specs=[VMEM] * 4,
        scratch_shapes=[
            pltpu.VMEM(x_own.shape, BF16),
            pltpu.VMEM(x_own.shape, BF16),
            pltpu.VMEM(mod.shape, F32),
            pltpu.VMEM(gain.shape, F32),
            pltpu.VMEM(w.shape, BF16),
            pltpu.VMEM(w_out.shape, BF16),
            pltpu.VMEM((tokens, width), BF16),
            pltpu.VMEM((heads, head_dim, tokens), BF16),
            pltpu.VMEM((heads, head_dim, tokens), BF16),
            pltpu.VMEM((heads, padded_rows(head_dim), tokens), BF16),
            pltpu.VMEM((videos, heads, 2 * rows, 2 * rows), F32),
            pltpu.VMEM((videos, heads, 2 * rows, 2 * rows), BF16),
            pltpu.VMEM((videos, inner, 2 * rows), BF16),
            pltpu.SemaphoreType.DMA((8,)),
        ],
        compiler_params=pltpu.CompilerParams(vmem_limit_bytes=28 * MIB),
        cost_estimate=pl.CostEstimate(flops=6 * 10**9, transcendentals=10**6, bytes_accessed=8 * 10**6),
        name="spatial",
    )(hbm(x_own), x_oth, hbm(mod), hbm(w), hbm(gain), hbm(w_out))


def middle_kernel(x_ref, own_ref, got_ref, gate_ref, out_ref):
    videos = x_ref.shape[0]
    peers, group, _ = out_ref.shape
    share = group // videos
    for d in range(peers):
        there = slice(d * share, (d + 1) * share)
        parts = []
        for v in range(videos):
            total = own_ref[v, there].astype(F32) + got_ref[v, there].astype(F32)
            total = total.astype(BF16).astype(F32)
            parts.append(x_ref[v, there].astype(F32) + gate_ref[v : v + 1, :] * total)
        out_ref[d] = jnp.concatenate(parts, axis=0).astype(BF16)


def middle(x_own, own, got, gate, peers):
    videos, rows, width = x_own.shape
    return pl.pallas_call(
        middle_kernel,
        out_shape=jax.ShapeDtypeStruct((peers, videos * rows // peers, width), BF16),
        in_specs=[VMEM] * 4,
        out_specs=VMEM,
        compiler_params=pltpu.CompilerParams(vmem_limit_bytes=16 * MIB),
        cost_estimate=pl.CostEstimate(flops=10**8, transcendentals=0, bytes_accessed=10**6),
        name="middle",
    )(x_own, own, got, gate)


def late_kernel(
    head_dim, parts, x_ref, mod, gain, qo_hbm, qr_hbm, oo_hbm, or_hbm, io_hbm, ir_hbm, fo_hbm, fr_hbm, out_ref,
    w_ref, o_ref, i_ref, f_ref, n_ref, r_ref, q_ref, k_ref, v_ref, s_ref, p_ref, a_ref, h_ref, sems,
):
    frames, group, _ = x_ref.shape
    share = group // parts
    tokens = frames * group
    heads = q_ref.shape[0]
    inner = w_ref.shape[2]
    half = heads // 2
    fetch = Fetches(sems)
    q_hbms, o_hbms, i_hbms, f_hbms = (qo_hbm, qr_hbm), (oo_hbm, or_hbm), (io_hbm, ir_hbm), (fo_hbm, fr_hbm)

    for side in range(2):
        fetch.start(f"q{side}", q_hbms[side].at[0], w_ref.at[side, 0])

    each = frames * share
    step = 2 if frames % 2 == 0 else 1

    def pieces():
        for v in range(parts):
            for f in range(0, frames, step):
                rows = [x_ref[f + i].astype(F32)[v * share : (v + 1) * share] for i in range(step)]
                start = v * each + f * share
                yield slice(start, start + step * share), jnp.concatenate(rows, axis=0)

    for index, (rows, values) in enumerate(pieces()):
        if index == tokens // (2 * step * share):
            for side in range(2):
                fetch.start(f"k{side}", q_hbms[side].at[1], w_ref.at[side, 1])
        normed = norm_rows(values) * (1.0 + mod[4:5, :]) + mod[3:4, :]
        n_ref[rows, :] = normed.astype(BF16)
    factor = math.log2(math.e) / math.sqrt(head_dim)
    columns = [column(gain[which : which + 1, :]) for which in range(2)]
    quarter = half // 2

    def project(side, which, target):
        for part in range(2):
            rows = slice(part * quarter * head_dim, (part + 1) * quarter * head_dim)
            projected = mm(w_ref[side, which, rows], n_ref[...], NT).reshape(quarter, head_dim, tokens)
            if which < 2:
                projected = head_norm(projected, columns[which] * factor if which == 0 else columns[which])
            else:
                projected = with_ones(projected)
            at = side * half + part * quarter
            target[at : at + quarter] = projected.astype(BF16)

    fetch.wait("q0", "q1")
    for side in range(2):
        fetch.start(f"v{side}", q_hbms[side].at[2], w_ref.at[side, 2])
        fetch.start(f"out{side}", o_hbms[side], o_ref.at[side])
    project(0, 0, q_ref)
    project(1, 0, q_ref)
    fetch.wait("k0", "k1")
    for side in range(2):
        fetch.start(f"in{side}", i_hbms[side], i_ref.at[side])
    project(0, 1, k_ref)
    project(1, 1, k_ref)
    for h in range(heads):
        for v in range(parts):
            cols = slice(v * each, (v + 1) * each)
            s_ref[h, v] = mm(k_ref[h, :, cols], q_ref[h, :, cols], TN)
    first = lax.broadcasted_iota(jnp.int32, (share, each), 0)
    second = lax.broadcasted_iota(jnp.int32, (share, each), 1)
    same = (first == lax.rem(second, share))[None]
    for h in range(heads):
        for v in range(parts):
            weights = jnp.exp2(s_ref[h, v]).reshape(frames, share, each)
            p_ref[h, v] = jnp.where(same, weights, 0.0).reshape(each, each).astype(BF16)
    fetch.wait("v0", "v1", "out0", "out1")
    for side in range(2):
        fetch.start(f"down{side}", f_hbms[side], f_ref.at[side])
    project(0, 2, v_ref)
    project(1, 2, v_ref)
    for h in range(0, heads, 2):
        for v in range(parts):
            cols = slice(v * each, (v + 1) * each)
            pair = [
                normalized(mm(v_ref[g, :, cols], p_ref[g, v], NN), head_dim) for g in (h, h + 1)
            ]
            a_ref[h * head_dim : (h + 2) * head_dim, cols] = jnp.concatenate(pair, axis=0).astype(BF16)
    r_ref[...] = mm(a_ref[:inner, :], o_ref[0], TN) + mm(a_ref[inner:, :], o_ref[1], TN)
    for rows, values in pieces():
        running = values + mod[5:6, :] * r_ref[rows, :].astype(BF16).astype(F32)
        r_ref[rows, :] = running
        normed = norm_rows(running) * (1.0 + mod[7:8, :]) + mod[6:7, :]
        n_ref[rows, :] = normed.astype(BF16)
    fetch.wait("in0", "in1")
    hidden_width = i_ref.shape[2]
    chunk = hidden_width // 3 if hidden_width % 384 == 0 else hidden_width
    for side in range(2):
        for start in range(0, hidden_width, chunk):
            u = mm(n_ref[...], i_ref[side, :, start : start + chunk], NN)
            h_ref[side, :, start : start + chunk] = jax.nn.gelu(u, approximate=True).astype(BF16)
    fetch.wait("down0", "down1")
    mlp = mm(h_ref[0], f_ref[0], NN) + mm(h_ref[1], f_ref[1], NN)
    mlp = mlp.astype(BF16).astype(F32)
    for f in range(frames):
        blocks = []
        for v in range(parts):
            rows = slice(v * each + f * share, v * each + (f + 1) * share)
            blocks.append(r_ref[rows, :] + mod[8:9, :] * mlp[rows])
        out_ref[f] = jnp.concatenate(blocks, axis=0).astype(BF16)


def late(x, early, q_own, q_rem, o_own, o_rem, i_own, i_rem, f_own, f_rem, head_dim, parts):
    frames, group, width = x.shape
    tokens = frames * group
    inner = q_own.shape[1]
    heads = 2 * inner // head_dim
    return pl.pallas_call(
        functools.partial(late_kernel, head_dim, parts),
        out_shape=jax.ShapeDtypeStruct(x.shape, BF16),
        in_specs=[VMEM] * 3 + [HBM] * 8,
        out_specs=VMEM,
        scratch_shapes=[
            pltpu.VMEM((2,) + q_own.shape, BF16),
            pltpu.VMEM((2,) + o_own.shape, BF16),
            pltpu.VMEM((2,) + i_own.shape, BF16),
            pltpu.VMEM((2,) + f_own.shape, BF16),
            pltpu.VMEM((tokens, width), BF16),
            pltpu.VMEM((tokens, width), F32),
            pltpu.VMEM((heads, head_dim, tokens), BF16),
            pltpu.VMEM((heads, head_dim, tokens), BF16),
            pltpu.VMEM((heads, padded_rows(head_dim), tokens), BF16),
            pltpu.VMEM((heads, parts, tokens // parts, tokens // parts), F32),
            pltpu.VMEM((heads, parts, tokens // parts, tokens // parts), BF16),
            pltpu.VMEM((2 * inner, tokens), BF16),
            pltpu.VMEM((2, tokens, i_own.shape[1]), BF16),
            pltpu.SemaphoreType.DMA((12,)),
        ],
        compiler_params=pltpu.CompilerParams(vmem_limit_bytes=52 * MIB),
        cost_estimate=pl.CostEstimate(flops=9 * 10**9, transcendentals=2 * 10**6, bytes_accessed=33 * 10**6),
        name="late",
    )(x, *early, *(hbm(v) for v in (q_own, q_rem, o_own, o_rem, i_own, i_rem, f_own, f_rem)))


def early_kernel(mod_hbm, gain_hbm, mod, gain, sems):
    fetch = Fetches(sems)
    fetch.start("mod", mod_hbm.at[lax.axis_index("tp")], mod)
    fetch.start("gain", gain_hbm, gain)
    fetch.wait("mod", "gain")


def early_loads(mod, gain):
    return pl.pallas_call(
        early_kernel,
        out_shape=[
            jax.ShapeDtypeStruct(mod.shape[1:], F32),
            jax.ShapeDtypeStruct(gain.shape, F32),
        ],
        in_specs=[HBM] * 2,
        out_specs=[VMEM] * 2,
        scratch_shapes=[pltpu.SemaphoreType.DMA((2,))],
        compiler_params=pltpu.CompilerParams(vmem_limit_bytes=4 * MIB),
        cost_estimate=pl.CostEstimate(flops=10**9, transcendentals=0, bytes_accessed=10**5),
        name="early",
    )(hbm(mod), hbm(gain))


def paired_body(
    seq_size,
    latent,
    modulation,
    qkv_spatial,
    gain_spatial,
    out_spatial,
    qkv_temporal,
    gain_temporal,
    out_temporal,
    fc_in,
    fc_out,
):
    head_dim = gain_spatial.shape[-1]
    videos, _, rows, width = latent.shape

    def swap(value):
        return lax.ppermute(value, "tp", [(0, 1), (1, 0)])

    x_own = latent.reshape(videos, rows, width)
    w_spatial = jnp.swapaxes(qkv_spatial, 1, 2)
    w_temporal = jnp.swapaxes(qkv_temporal, 1, 2)
    latent_modulation = modulation
    modulation = jnp.swapaxes(modulation, 0, 1)
    x_oth = swap(x_own)
    x_oth, w_sent, o_sent = lax.optimization_barrier((x_oth, w_temporal, out_temporal))
    q_rem = swap(w_sent)
    o_rem = swap(o_sent)
    own, other, x_kept, gate = spatial(
        x_own, x_oth, modulation, w_spatial, gain_spatial, out_spatial, head_dim
    )
    got = swap(other)
    got, i_sent, f_sent = lax.optimization_barrier((got, fc_in, fc_out))
    i_rem = swap(i_sent)
    f_rem = swap(f_sent)
    mid = middle(x_kept, own, got, gate, seq_size)
    both = ("seq", "tp")
    share = rows // seq_size
    moved = lax.all_to_all(mid.reshape(-1, share, width), both, 0, 0, tiled=True)
    early = early_loads(latent_modulation, gain_temporal)
    done = late(
        moved.reshape(mid.shape), early, w_temporal, q_rem, out_temporal, o_rem,
        fc_in, i_rem, fc_out, f_rem, head_dim, mid.shape[1] // share,
    )
    back = lax.all_to_all(done.reshape(-1, share, width), both, 0, 0, tiled=True)
    back = back.reshape(seq_size, videos, share, width).transpose(1, 0, 2, 3)
    return back.reshape(latent.shape)


def layer_norm(values):
    average = jnp.mean(values, axis=-1, keepdims=True)
    centred = values - average
    variance = jnp.mean(centred * centred, axis=-1, keepdims=True)
    return centred * lax.rsqrt(variance + epsilon)


def modulated(field, modulation, offset):
    shift_row = modulation[:, offset][:, None, None, :]
    scale_row = modulation[:, offset + 1][:, None, None, :]
    return (layer_norm(field) * (1.0 + scale_row) + shift_row).astype(jnp.bfloat16)


def project_heads(rows_piece, table, gains, head_dim):
    results = []
    for which_part in range(3):
        projected = jnp.einsum(
            "bfpd,de->bfpe", rows_piece, table[which_part], preferred_element_type=jnp.float32
        )
        if which_part < 2:
            shaped = projected.reshape(
                projected.shape[:-1] + (projected.shape[-1] // head_dim, head_dim)
            )
            shaped = (
                shaped
                * lax.rsqrt(jnp.mean(shaped * shaped, axis=-1, keepdims=True) + epsilon)
                * gains[which_part]
            )
            projected = shaped.reshape(projected.shape)
        results.append(projected.astype(jnp.bfloat16))
    return jnp.stack(results)


def attend(query_rows, key_rows, value_rows, head_dim):
    groups, length, feature_width = query_rows.shape
    head_count = feature_width // head_dim
    query_heads = query_rows.reshape(groups, length, head_count, head_dim)
    key_heads = key_rows.reshape(groups, length, head_count, head_dim)
    value_heads = value_rows.reshape(groups, length, head_count, head_dim)
    block_rows = min(length, 512)

    def one_block(first_row):
        query_block = lax.dynamic_slice_in_dim(query_heads, first_row, block_rows, 1)
        scores = jnp.einsum(
            "gqhe,gkhe->ghqk", query_block, key_heads, preferred_element_type=jnp.float32
        ) / math.sqrt(head_dim)
        weights = jnp.exp(scores)
        probabilities = (weights / jnp.sum(weights, axis=-1, keepdims=True)).astype(jnp.bfloat16)
        return jnp.einsum(
            "ghqk,gkhe->gqhe", probabilities, value_heads, preferred_element_type=jnp.float32
        ).astype(jnp.bfloat16)

    starts = jnp.arange(length // block_rows, dtype=jnp.int32) * block_rows
    pieces = lax.map(one_block, starts)
    return pieces.transpose(1, 0, 2, 3, 4).reshape(groups, length, feature_width)


def frame_attention(query_rows, key_rows, value_rows, head_dim):
    batches, frames, patches, feature_width = query_rows.shape
    members = [
        item.transpose(0, 2, 1, 3).reshape(batches * patches, frames, feature_width)
        for item in (query_rows, key_rows, value_rows)
    ]
    mixed_heads = attend(members[0], members[1], members[2], head_dim)
    return mixed_heads.reshape(batches, patches, frames, feature_width).transpose(0, 2, 1, 3)


def body(
    latent,
    modulation,
    qkv_spatial,
    gain_spatial,
    out_spatial,
    qkv_temporal,
    gain_temporal,
    out_temporal,
    fc_in,
    fc_out,
):
    head_dim = gain_spatial.shape[-1]
    running = latent.astype(jnp.float32)
    normed = modulated(running, modulation, 0)
    packed = project_heads(
        lax.all_gather(normed, "tp", axis=2, tiled=True), qkv_spatial, gain_spatial, head_dim
    )
    batches, frames, patches, local_width = packed.shape[1:]
    mixed_heads = attend(
        packed[0].reshape(batches * frames, patches, local_width),
        packed[1].reshape(batches * frames, patches, local_width),
        packed[2].reshape(batches * frames, patches, local_width),
        head_dim,
    )
    mixed_heads = mixed_heads.reshape(batches, frames, patches, local_width)
    partial_value = jnp.einsum(
        "bfpe,ed->bfpd", mixed_heads, out_spatial, preferred_element_type=jnp.float32
    )
    spatial_out = lax.psum_scatter(
        partial_value.astype(jnp.bfloat16), "tp", scatter_dimension=2, tiled=True
    )
    running = running + modulation[:, 2][:, None, None, :] * spatial_out.astype(jnp.float32)
    normed = modulated(running, modulation, 3)
    moved_rows = lax.all_to_all(normed, "seq", split_axis=2, concat_axis=1, tiled=True)
    packed = project_heads(
        lax.all_gather(moved_rows, "tp", axis=2, tiled=True), qkv_temporal, gain_temporal, head_dim
    )
    mixed_heads = frame_attention(packed[0], packed[1], packed[2], head_dim)
    partial_value = jnp.einsum(
        "bfpe,ed->bfpd", mixed_heads, out_temporal, preferred_element_type=jnp.float32
    )
    shares = lax.psum_scatter(
        partial_value.astype(jnp.bfloat16), "tp", scatter_dimension=2, tiled=True
    )
    temporal_out = lax.all_to_all(shares, "seq", split_axis=1, concat_axis=2, tiled=True)
    running = running + modulation[:, 5][:, None, None, :] * temporal_out.astype(jnp.float32)
    normed = modulated(running, modulation, 6)
    projected = jnp.einsum(
        "bfpd,de->bfpe",
        lax.all_gather(normed, "tp", axis=2, tiled=True),
        fc_in,
        preferred_element_type=jnp.float32,
    )
    hidden = jax.nn.gelu(projected, approximate=True).astype(jnp.bfloat16)
    partial_value = jnp.einsum("bfpe,ed->bfpd", hidden, fc_out, preferred_element_type=jnp.float32)
    mlp_out = lax.psum_scatter(
        partial_value.astype(jnp.bfloat16), "tp", scatter_dimension=2, tiled=True
    )
    return (running + modulation[:, 8][:, None, None, :] * mlp_out.astype(jnp.float32)).astype(
        jnp.bfloat16
    )


def fits(mesh, videos, local_frames, local_rows, heads_here):
    return (
        mesh.shape["tp"] == 2
        and videos == 2
        and local_frames == 1
        and local_rows % (8 * mesh.shape["seq"]) == 0
        and heads_here % 2 == 0
    )


def solution(mesh):
    placed = (
        P(None, "seq", "tp", None),
        P(),
        P(None, None, "tp"),
        P(),
        P("tp", None),
        P(None, None, "tp"),
        P(),
        P("tp", None),
        P(None, "tp"),
        P("tp", None),
    )

    def step(*args):
        latent, qkv, gain = args[0], args[2], args[3]
        if fits(mesh, latent.shape[0], latent.shape[1], latent.shape[2], qkv.shape[2] // gain.shape[1]):
            return paired_body(mesh.shape["seq"], *args)
        return body(*args)

    return jax.shard_map(
        step, mesh=mesh, in_specs=placed, out_specs=P(None, "seq", "tp", None), check_vma=False
    )
```

```python
import functools
import math

import jax
import jax.numpy as jnp
from jax import lax
from jax.experimental import pallas as pl
from jax.experimental.pallas import tpu as pltpu
from jax.sharding import PartitionSpec as P


epsilon = 1e-06
F32 = jnp.float32
BF16 = jnp.bfloat16
VMEM = pl.BlockSpec(memory_space=pltpu.VMEM)
HBM = pl.BlockSpec(memory_space=pltpu.HBM)

MIB = 1 << 20

NT = (((1,), (1,)), ((), ()))
TN = (((0,), (0,)), ((), ()))
NN = (((1,), (0,)), ((), ()))


def mm(a, b, dims):
    return lax.dot_general(a, b, dims, preferred_element_type=F32)


def hbm(value):
    return pltpu.with_memory_space_constraint(value, pltpu.HBM)


class Fetches:
    def __init__(self, sems):
        self.sems, self.made = sems, {}

    def start(self, name, source, target):
        copy = pltpu.make_async_copy(source, target, self.sems.at[len(self.made)])
        copy.start()
        self.made[name] = copy

    def wait(self, *names):
        for name in names:
            self.made[name].wait()


def norm_rows(values):
    average = jnp.mean(values, axis=-1, keepdims=True)
    centred = values - average
    variance = jnp.mean(centred * centred, axis=-1, keepdims=True)
    return centred * lax.rsqrt(variance + epsilon)


def column(row):
    n = row.shape[1]
    diagonal = lax.broadcasted_iota(jnp.int32, (n, n), 0) == lax.broadcasted_iota(jnp.int32, (n, n), 1)
    return jnp.sum(jnp.where(diagonal, row, 0.0), axis=1, keepdims=True)


def head_norm(projected, gain):
    mean_square = jnp.mean(projected * projected, axis=1, keepdims=True)
    return projected * lax.rsqrt(mean_square + epsilon) * gain[None]


def padded_rows(head_dim):
    return -(-(head_dim + 1) // 16) * 16


def with_ones(values):
    heads, head_dim, tokens = values.shape
    extra = padded_rows(head_dim) - head_dim
    place = lax.broadcasted_iota(jnp.int32, (heads, extra, tokens), 1)
    return jnp.concatenate([values, jnp.where(place == 0, 1.0, 0.0)], axis=1)


def normalized(mixed, head_dim):
    return mixed[:head_dim] * (1.0 / mixed[head_dim : head_dim + 1])


def spatial_kernel(
    head_dim, own_hbm, oth_hbm, mod_hbm, w_hbm, gain_hbm, o_hbm, part_own, part_oth, x_out, gate_out,
    x_own, x_oth, mod, gain, w_ref, o_ref, n_ref, q_ref, k_ref, v_ref, s_ref, p_ref, a_ref, sems,
):
    videos, rows, _ = part_own.shape
    patches = 2 * rows
    heads = w_ref.shape[1] // head_dim
    fetch = Fetches(sems)
    fetch.start("own", own_hbm, x_own)
    fetch.start("mod", mod_hbm, mod)
    fetch.start("oth", oth_hbm, x_oth)
    fetch.start("gain", gain_hbm, gain)
    for which in range(3):
        fetch.start(which, w_hbm.at[which], w_ref.at[which])
    fetch.start("out", o_hbm, o_ref)
    block = 16 if rows % 16 == 0 else rows
    fetch.wait("own", "mod", "gain")
    x_out[...] = x_own[...]
    gate_out[...] = mod[2]
    for v in range(videos):
        for place, source in enumerate((x_own, x_oth)):
            if v == 0 and place == 1:
                fetch.wait("oth")
            base = v * patches + place * rows
            for start in range(0, rows, block):
                normed = norm_rows(source[v, start : start + block].astype(F32))
                normed = normed * (1.0 + mod[1, v : v + 1, :]) + mod[0, v : v + 1, :]
                n_ref[base + start : base + start + block, :] = normed.astype(BF16)
    factor = math.log2(math.e) / math.sqrt(head_dim)
    for which, target in enumerate((q_ref, k_ref, v_ref)):
        fetch.wait(which)
        projected = mm(w_ref[which], n_ref[...], NT)
        projected = projected.reshape(heads, head_dim, videos * patches)
        if which < 2:
            gains = column(gain[which : which + 1, :])
            projected = head_norm(projected, gains * factor if which == 0 else gains)
        else:
            projected = with_ones(projected)
        target[...] = projected.astype(BF16)
    for v in range(videos):
        cols = slice(v * patches, (v + 1) * patches)
        for h in range(heads):
            s_ref[v, h] = mm(k_ref[h, :, cols], q_ref[h, :, cols], TN)
    for v in range(videos):
        for h in range(heads):
            p_ref[v, h] = jnp.exp2(s_ref[v, h]).astype(BF16)
    for v in range(videos):
        cols = slice(v * patches, (v + 1) * patches)
        for h in range(0, heads, 2):
            pair = [
                normalized(mm(v_ref[g, :, cols], p_ref[v, g], NN), head_dim) for g in (h, h + 1)
            ]
            a_ref[v, h * head_dim : (h + 2) * head_dim, :] = jnp.concatenate(pair, axis=0).astype(BF16)
    fetch.wait("out")
    for v in range(videos):
        part = mm(a_ref[v], o_ref[...], TN).astype(BF16)
        part_own[v] = part[:rows]
        part_oth[v] = part[rows:]


def spatial(x_own, x_oth, mod, w, gain, w_out, head_dim):
    videos, rows, width = x_own.shape
    inner = w.shape[1]
    heads = inner // head_dim
    tokens = 2 * rows * videos
    return pl.pallas_call(
        functools.partial(spatial_kernel, head_dim),
        out_shape=[jax.ShapeDtypeStruct((videos, rows, width), BF16)] * 3
        + [jax.ShapeDtypeStruct((videos, width), F32)],
        in_specs=[HBM] * 6,
        out_specs=[VMEM] * 4,
        scratch_shapes=[
            pltpu.VMEM(x_own.shape, BF16),
            pltpu.VMEM(x_own.shape, BF16),
            pltpu.VMEM(mod.shape, F32),
            pltpu.VMEM(gain.shape, F32),
            pltpu.VMEM(w.shape, BF16),
            pltpu.VMEM(w_out.shape, BF16),
            pltpu.VMEM((tokens, width), BF16),
            pltpu.VMEM((heads, head_dim, tokens), BF16),
            pltpu.VMEM((heads, head_dim, tokens), BF16),
            pltpu.VMEM((heads, padded_rows(head_dim), tokens), BF16),
            pltpu.VMEM((videos, heads, 2 * rows, 2 * rows), F32),
            pltpu.VMEM((videos, heads, 2 * rows, 2 * rows), BF16),
            pltpu.VMEM((videos, inner, 2 * rows), BF16),
            pltpu.SemaphoreType.DMA((8,)),
        ],
        compiler_params=pltpu.CompilerParams(vmem_limit_bytes=28 * MIB),
        cost_estimate=pl.CostEstimate(flops=6 * 10**9, transcendentals=10**6, bytes_accessed=8 * 10**6),
        name="spatial",
    )(hbm(x_own), x_oth, hbm(mod), hbm(w), hbm(gain), hbm(w_out))


def middle_kernel(x_ref, own_ref, got_ref, gate_ref, out_ref):
    videos, rows, _ = x_ref.shape
    block = 16 if rows % 16 == 0 else rows
    for v in range(videos):
        for start in range(0, rows, block):
            there = slice(start, start + block)
            total = own_ref[v, there].astype(F32) + got_ref[v, there].astype(F32)
            total = total.astype(BF16).astype(F32)
            mid = x_ref[v, there].astype(F32) + gate_ref[v : v + 1, :] * total
            out_ref[v, there] = mid.astype(BF16)


def middle(x_own, own, got, gate):
    return pl.pallas_call(
        middle_kernel,
        out_shape=jax.ShapeDtypeStruct(x_own.shape, BF16),
        in_specs=[VMEM] * 4,
        out_specs=VMEM,
        compiler_params=pltpu.CompilerParams(vmem_limit_bytes=16 * MIB),
        cost_estimate=pl.CostEstimate(flops=10**8, transcendentals=0, bytes_accessed=10**6),
        name="middle",
    )(x_own, own, got, gate)


def late_kernel(
    head_dim, parts, frames, x_ref, mod, gain, qo_hbm, qr_hbm, oo_hbm, or_hbm, io_hbm, ir_hbm, fo_hbm, fr_hbm, out_ref,
    w_ref, o_ref, i_ref, f_ref, n_ref, r_ref, q_ref, k_ref, v_ref, s_ref, p_ref, a_ref, h_ref, sems,
):
    tokens, _ = x_ref.shape
    each = tokens // parts
    share = each // frames
    heads = q_ref.shape[0]
    inner = w_ref.shape[2]
    half = heads // 2
    fetch = Fetches(sems)
    q_hbms, o_hbms, i_hbms, f_hbms = (qo_hbm, qr_hbm), (oo_hbm, or_hbm), (io_hbm, ir_hbm), (fo_hbm, fr_hbm)

    for side in range(2):
        fetch.start(f"q{side}", q_hbms[side].at[0], w_ref.at[side, 0])

    block = 16 if tokens % 32 == 0 else tokens // 2

    def pieces():
        for start in range(0, tokens, block):
            rows = slice(start, start + block)
            yield rows, x_ref[rows, :].astype(F32)

    for index, (rows, values) in enumerate(pieces()):
        if index == tokens // (2 * block):
            for side in range(2):
                fetch.start(f"k{side}", q_hbms[side].at[1], w_ref.at[side, 1])
        normed = norm_rows(values) * (1.0 + mod[4:5, :]) + mod[3:4, :]
        n_ref[rows, :] = normed.astype(BF16)
    factor = math.log2(math.e) / math.sqrt(head_dim)
    columns = [column(gain[which : which + 1, :]) for which in range(2)]
    quarter = half // 2

    def project(side, which, target):
        for part in range(2):
            rows = slice(part * quarter * head_dim, (part + 1) * quarter * head_dim)
            projected = mm(w_ref[side, which, rows], n_ref[...], NT).reshape(quarter, head_dim, tokens)
            if which < 2:
                projected = head_norm(projected, columns[which] * factor if which == 0 else columns[which])
            else:
                projected = with_ones(projected)
            at = side * half + part * quarter
            target[at : at + quarter] = projected.astype(BF16)

    fetch.wait("q0", "q1")
    for side in range(2):
        fetch.start(f"v{side}", q_hbms[side].at[2], w_ref.at[side, 2])
        fetch.start(f"out{side}", o_hbms[side], o_ref.at[side])
    project(0, 0, q_ref)
    project(1, 0, q_ref)
    fetch.wait("k0", "k1")
    for side in range(2):
        fetch.start(f"in{side}", i_hbms[side], i_ref.at[side])
    project(0, 1, k_ref)
    project(1, 1, k_ref)
    for h in range(heads):
        for v in range(parts):
            cols = slice(v * each, (v + 1) * each)
            s_ref[h, v] = mm(k_ref[h, :, cols], q_ref[h, :, cols], TN)
    first = lax.broadcasted_iota(jnp.int32, (share, each), 0)
    second = lax.broadcasted_iota(jnp.int32, (share, each), 1)
    same = (first == lax.rem(second, share))[None]
    for h in range(heads):
        for v in range(parts):
            weights = jnp.exp2(s_ref[h, v]).reshape(frames, share, each)
            p_ref[h, v] = jnp.where(same, weights, 0.0).reshape(each, each).astype(BF16)
    fetch.wait("v0", "v1", "out0", "out1")
    for side in range(2):
        fetch.start(f"down{side}", f_hbms[side], f_ref.at[side])
    project(0, 2, v_ref)
    project(1, 2, v_ref)
    for h in range(0, heads, 2):
        for v in range(parts):
            cols = slice(v * each, (v + 1) * each)
            pair = [
                normalized(mm(v_ref[g, :, cols], p_ref[g, v], NN), head_dim) for g in (h, h + 1)
            ]
            a_ref[h * head_dim : (h + 2) * head_dim, cols] = jnp.concatenate(pair, axis=0).astype(BF16)
    r_ref[...] = mm(a_ref[:inner, :], o_ref[0], TN) + mm(a_ref[inner:, :], o_ref[1], TN)
    for rows, values in pieces():
        running = values + mod[5:6, :] * r_ref[rows, :].astype(BF16).astype(F32)
        r_ref[rows, :] = running
        normed = norm_rows(running) * (1.0 + mod[7:8, :]) + mod[6:7, :]
        n_ref[rows, :] = normed.astype(BF16)
    fetch.wait("in0", "in1")
    hidden_width = i_ref.shape[2]
    chunk = hidden_width // 3 if hidden_width % 384 == 0 else hidden_width
    for side in range(2):
        for start in range(0, hidden_width, chunk):
            u = mm(n_ref[...], i_ref[side, :, start : start + chunk], NN)
            h_ref[side, :, start : start + chunk] = jax.nn.gelu(u, approximate=True).astype(BF16)
    fetch.wait("down0", "down1")
    mlp = mm(h_ref[0], f_ref[0], NN) + mm(h_ref[1], f_ref[1], NN)
    mlp = mlp.astype(BF16).astype(F32)
    out_ref[...] = (r_ref[...] + mod[8:9, :] * mlp).astype(BF16)


def late(x, early, q_own, q_rem, o_own, o_rem, i_own, i_rem, f_own, f_rem, head_dim, parts, frames):
    tokens, width = x.shape
    inner = q_own.shape[1]
    heads = 2 * inner // head_dim
    return pl.pallas_call(
        functools.partial(late_kernel, head_dim, parts, frames),
        out_shape=jax.ShapeDtypeStruct(x.shape, BF16),
        in_specs=[VMEM] * 3 + [HBM] * 8,
        out_specs=VMEM,
        scratch_shapes=[
            pltpu.VMEM((2,) + q_own.shape, BF16),
            pltpu.VMEM((2,) + o_own.shape, BF16),
            pltpu.VMEM((2,) + i_own.shape, BF16),
            pltpu.VMEM((2,) + f_own.shape, BF16),
            pltpu.VMEM((tokens, width), BF16),
            pltpu.VMEM((tokens, width), F32),
            pltpu.VMEM((heads, head_dim, tokens), BF16),
            pltpu.VMEM((heads, head_dim, tokens), BF16),
            pltpu.VMEM((heads, padded_rows(head_dim), tokens), BF16),
            pltpu.VMEM((heads, parts, tokens // parts, tokens // parts), F32),
            pltpu.VMEM((heads, parts, tokens // parts, tokens // parts), BF16),
            pltpu.VMEM((2 * inner, tokens), BF16),
            pltpu.VMEM((2, tokens, i_own.shape[1]), BF16),
            pltpu.SemaphoreType.DMA((12,)),
        ],
        compiler_params=pltpu.CompilerParams(vmem_limit_bytes=52 * MIB),
        cost_estimate=pl.CostEstimate(flops=9 * 10**9, transcendentals=2 * 10**6, bytes_accessed=33 * 10**6),
        name="late",
    )(x, *early, *(hbm(v) for v in (q_own, q_rem, o_own, o_rem, i_own, i_rem, f_own, f_rem)))


def early_kernel(mod_hbm, gain_hbm, mod, gain, sems):
    fetch = Fetches(sems)
    fetch.start("mod", mod_hbm.at[lax.axis_index("tp")], mod)
    fetch.start("gain", gain_hbm, gain)
    fetch.wait("mod", "gain")


def early_loads(mod, gain):
    return pl.pallas_call(
        early_kernel,
        out_shape=[
            jax.ShapeDtypeStruct(mod.shape[1:], F32),
            jax.ShapeDtypeStruct(gain.shape, F32),
        ],
        in_specs=[HBM] * 2,
        out_specs=[VMEM] * 2,
        scratch_shapes=[pltpu.SemaphoreType.DMA((2,))],
        compiler_params=pltpu.CompilerParams(vmem_limit_bytes=4 * MIB),
        cost_estimate=pl.CostEstimate(flops=10**9, transcendentals=0, bytes_accessed=10**5),
        name="early",
    )(hbm(mod), hbm(gain))


def paired_body(
    seq_size,
    latent,
    modulation,
    qkv_spatial,
    gain_spatial,
    out_spatial,
    qkv_temporal,
    gain_temporal,
    out_temporal,
    fc_in,
    fc_out,
):
    head_dim = gain_spatial.shape[-1]
    videos, _, rows, width = latent.shape

    def swap(value):
        return lax.ppermute(value, "tp", [(0, 1), (1, 0)])

    x_own = latent.reshape(videos, rows, width)
    w_spatial = jnp.swapaxes(qkv_spatial, 1, 2)
    w_temporal = jnp.swapaxes(qkv_temporal, 1, 2)
    mod_rows = jnp.swapaxes(modulation, 0, 1)
    x_oth = swap(x_own)
    q_rem = swap(w_temporal)
    o_rem = swap(out_temporal)
    own, other, x_kept, gate = spatial(
        x_own, x_oth, mod_rows, w_spatial, gain_spatial, out_spatial, head_dim
    )
    other, i_sent, f_sent = lax.optimization_barrier((other, fc_in, fc_out))
    got = swap(other)
    i_rem = swap(i_sent)
    f_rem = swap(f_sent)
    mid = middle(x_kept, own, got, gate)
    both = ("tp", "seq")
    share = rows // seq_size
    moved = lax.all_to_all(mid.reshape(-1, share, width), both, 0, 0, tiled=True)
    early = early_loads(modulation, gain_temporal)
    done = late(
        moved.reshape(-1, width), early, w_temporal, q_rem, out_temporal, o_rem,
        fc_in, i_rem, fc_out, f_rem, head_dim, videos, seq_size,
    )
    back = lax.all_to_all(done.reshape(-1, share, width), both, 0, 0, tiled=True)
    return back.reshape(latent.shape)


def layer_norm(values):
    average = jnp.mean(values, axis=-1, keepdims=True)
    centred = values - average
    variance = jnp.mean(centred * centred, axis=-1, keepdims=True)
    return centred * lax.rsqrt(variance + epsilon)


def modulated(field, modulation, offset):
    shift_row = modulation[:, offset][:, None, None, :]
    scale_row = modulation[:, offset + 1][:, None, None, :]
    return (layer_norm(field) * (1.0 + scale_row) + shift_row).astype(jnp.bfloat16)


def project_heads(rows_piece, table, gains, head_dim):
    results = []
    for which_part in range(3):
        projected = jnp.einsum(
            "bfpd,de->bfpe", rows_piece, table[which_part], preferred_element_type=jnp.float32
        )
        if which_part < 2:
            shaped = projected.reshape(
                projected.shape[:-1] + (projected.shape[-1] // head_dim, head_dim)
            )
            shaped = (
                shaped
                * lax.rsqrt(jnp.mean(shaped * shaped, axis=-1, keepdims=True) + epsilon)
                * gains[which_part]
            )
            projected = shaped.reshape(projected.shape)
        results.append(projected.astype(jnp.bfloat16))
    return jnp.stack(results)


def attend(query_rows, key_rows, value_rows, head_dim):
    groups, length, feature_width = query_rows.shape
    head_count = feature_width // head_dim
    query_heads = query_rows.reshape(groups, length, head_count, head_dim)
    key_heads = key_rows.reshape(groups, length, head_count, head_dim)
    value_heads = value_rows.reshape(groups, length, head_count, head_dim)
    block_rows = min(length, 512)

    def one_block(first_row):
        query_block = lax.dynamic_slice_in_dim(query_heads, first_row, block_rows, 1)
        scores = jnp.einsum(
            "gqhe,gkhe->ghqk", query_block, key_heads, preferred_element_type=jnp.float32
        ) / math.sqrt(head_dim)
        weights = jnp.exp(scores)
        probabilities = (weights / jnp.sum(weights, axis=-1, keepdims=True)).astype(jnp.bfloat16)
        return jnp.einsum(
            "ghqk,gkhe->gqhe", probabilities, value_heads, preferred_element_type=jnp.float32
        ).astype(jnp.bfloat16)

    starts = jnp.arange(length // block_rows, dtype=jnp.int32) * block_rows
    pieces = lax.map(one_block, starts)
    return pieces.transpose(1, 0, 2, 3, 4).reshape(groups, length, feature_width)


def frame_attention(query_rows, key_rows, value_rows, head_dim):
    batches, frames, patches, feature_width = query_rows.shape
    members = [
        item.transpose(0, 2, 1, 3).reshape(batches * patches, frames, feature_width)
        for item in (query_rows, key_rows, value_rows)
    ]
    mixed_heads = attend(members[0], members[1], members[2], head_dim)
    return mixed_heads.reshape(batches, patches, frames, feature_width).transpose(0, 2, 1, 3)


def body(
    latent,
    modulation,
    qkv_spatial,
    gain_spatial,
    out_spatial,
    qkv_temporal,
    gain_temporal,
    out_temporal,
    fc_in,
    fc_out,
):
    head_dim = gain_spatial.shape[-1]
    running = latent.astype(jnp.float32)
    normed = modulated(running, modulation, 0)
    packed = project_heads(
        lax.all_gather(normed, "tp", axis=2, tiled=True), qkv_spatial, gain_spatial, head_dim
    )
    batches, frames, patches, local_width = packed.shape[1:]
    mixed_heads = attend(
        packed[0].reshape(batches * frames, patches, local_width),
        packed[1].reshape(batches * frames, patches, local_width),
        packed[2].reshape(batches * frames, patches, local_width),
        head_dim,
    )
    mixed_heads = mixed_heads.reshape(batches, frames, patches, local_width)
    partial_value = jnp.einsum(
        "bfpe,ed->bfpd", mixed_heads, out_spatial, preferred_element_type=jnp.float32
    )
    spatial_out = lax.psum_scatter(
        partial_value.astype(jnp.bfloat16), "tp", scatter_dimension=2, tiled=True
    )
    running = running + modulation[:, 2][:, None, None, :] * spatial_out.astype(jnp.float32)
    normed = modulated(running, modulation, 3)
    moved_rows = lax.all_to_all(normed, "seq", split_axis=2, concat_axis=1, tiled=True)
    packed = project_heads(
        lax.all_gather(moved_rows, "tp", axis=2, tiled=True), qkv_temporal, gain_temporal, head_dim
    )
    mixed_heads = frame_attention(packed[0], packed[1], packed[2], head_dim)
    partial_value = jnp.einsum(
        "bfpe,ed->bfpd", mixed_heads, out_temporal, preferred_element_type=jnp.float32
    )
    shares = lax.psum_scatter(
        partial_value.astype(jnp.bfloat16), "tp", scatter_dimension=2, tiled=True
    )
    temporal_out = lax.all_to_all(shares, "seq", split_axis=1, concat_axis=2, tiled=True)
    running = running + modulation[:, 5][:, None, None, :] * temporal_out.astype(jnp.float32)
    normed = modulated(running, modulation, 6)
    projected = jnp.einsum(
        "bfpd,de->bfpe",
        lax.all_gather(normed, "tp", axis=2, tiled=True),
        fc_in,
        preferred_element_type=jnp.float32,
    )
    hidden = jax.nn.gelu(projected, approximate=True).astype(jnp.bfloat16)
    partial_value = jnp.einsum("bfpe,ed->bfpd", hidden, fc_out, preferred_element_type=jnp.float32)
    mlp_out = lax.psum_scatter(
        partial_value.astype(jnp.bfloat16), "tp", scatter_dimension=2, tiled=True
    )
    return (running + modulation[:, 8][:, None, None, :] * mlp_out.astype(jnp.float32)).astype(
        jnp.bfloat16
    )


def fits(mesh, videos, local_frames, local_rows, heads_here):
    return (
        mesh.shape["tp"] == 2
        and videos == 2
        and local_frames == 1
        and local_rows % (8 * mesh.shape["seq"]) == 0
        and heads_here % 2 == 0
    )


def solution(mesh):
    placed = (
        P(None, "seq", "tp", None),
        P(),
        P(None, None, "tp"),
        P(),
        P("tp", None),
        P(None, None, "tp"),
        P(),
        P("tp", None),
        P(None, "tp"),
        P("tp", None),
    )

    def step(*args):
        latent, qkv, gain = args[0], args[2], args[3]
        if fits(mesh, latent.shape[0], latent.shape[1], latent.shape[2], qkv.shape[2] // gain.shape[1]):
            return paired_body(mesh.shape["seq"], *args)
        return body(*args)

    return jax.shard_map(
        step, mesh=mesh, in_specs=placed, out_specs=P(None, "seq", "tp", None), check_vma=False
    )
```

```python
import functools
import math

import jax
import jax.numpy as jnp
from jax import lax
from jax.experimental import pallas as pl
from jax.experimental.pallas import tpu as pltpu
from jax.sharding import PartitionSpec as P


epsilon = 1e-06
F32 = jnp.float32
BF16 = jnp.bfloat16
VMEM = pl.BlockSpec(memory_space=pltpu.VMEM)
HBM = pl.BlockSpec(memory_space=pltpu.HBM)

MIB = 1 << 20

NT = (((1,), (1,)), ((), ()))
TN = (((0,), (0,)), ((), ()))
NN = (((1,), (0,)), ((), ()))


def mm(a, b, dims):
    return lax.dot_general(a, b, dims, preferred_element_type=F32)


def hbm(value):
    return pltpu.with_memory_space_constraint(value, pltpu.HBM)


class Fetches:
    def __init__(self, sems):
        self.sems, self.made = sems, {}

    def start(self, name, source, target):
        copy = pltpu.make_async_copy(source, target, self.sems.at[len(self.made)])
        copy.start()
        self.made[name] = copy

    def wait(self, *names):
        for name in names:
            self.made[name].wait()


def norm_rows(values):
    average = jnp.mean(values, axis=-1, keepdims=True)
    centred = values - average
    variance = jnp.mean(centred * centred, axis=-1, keepdims=True)
    return centred * lax.rsqrt(variance + epsilon)


def column(row):
    n = row.shape[1]
    diagonal = lax.broadcasted_iota(jnp.int32, (n, n), 0) == lax.broadcasted_iota(jnp.int32, (n, n), 1)
    return jnp.sum(jnp.where(diagonal, row, 0.0), axis=1, keepdims=True)


def head_norm(projected, gain):
    mean_square = jnp.mean(projected * projected, axis=1, keepdims=True)
    return projected * lax.rsqrt(mean_square + epsilon) * gain[None]


def padded_rows(head_dim):
    return -(-(head_dim + 1) // 16) * 16


def with_ones(values):
    heads, head_dim, tokens = values.shape
    extra = padded_rows(head_dim) - head_dim
    place = lax.broadcasted_iota(jnp.int32, (heads, extra, tokens), 1)
    return jnp.concatenate([values, jnp.where(place == 0, 1.0, 0.0)], axis=1)


def normalized(mixed, head_dim):
    return mixed[:head_dim] * (1.0 / mixed[head_dim : head_dim + 1])


def spatial_kernel(
    head_dim, own_hbm, oth_hbm, mod_hbm, w_hbm, gain_hbm, o_hbm, part_own, part_oth, x_out, gate_out,
    x_own, x_oth, mod, gain, w_ref, o_ref, n_ref, q_ref, k_ref, v_ref, s_ref, p_ref, a_ref, sems,
):
    videos, rows, _ = part_own.shape
    patches = 2 * rows
    heads = w_ref.shape[1] // head_dim
    fetch = Fetches(sems)
    fetch.start("own", own_hbm, x_own)
    fetch.start("mod", mod_hbm, mod)
    fetch.start("oth", oth_hbm, x_oth)
    fetch.start("gain", gain_hbm, gain)
    for which in range(3):
        fetch.start(which, w_hbm.at[which], w_ref.at[which])
    fetch.start("out", o_hbm, o_ref)
    block = 16 if rows % 16 == 0 else rows
    fetch.wait("own", "mod", "gain")
    x_out[...] = x_own[...]
    gate_out[...] = mod[2]
    for v in range(videos):
        for place, source in enumerate((x_own, x_oth)):
            if v == 0 and place == 1:
                fetch.wait("oth")
            base = v * patches + place * rows
            for start in range(0, rows, block):
                normed = norm_rows(source[v, start : start + block].astype(F32))
                normed = normed * (1.0 + mod[1, v : v + 1, :]) + mod[0, v : v + 1, :]
                n_ref[base + start : base + start + block, :] = normed.astype(BF16)
    factor = math.log2(math.e) / math.sqrt(head_dim)
    for which, target in enumerate((q_ref, k_ref, v_ref)):
        if which == 0:
            fetch.wait(0)
        elif which == 1:
            fetch.wait(1, 2, "out")
        projected = mm(w_ref[which], n_ref[...], NT)
        projected = projected.reshape(heads, head_dim, videos * patches)
        if which < 2:
            gains = column(gain[which : which + 1, :])
            projected = head_norm(projected, gains * factor if which == 0 else gains)
        else:
            projected = with_ones(projected)
        target[...] = projected.astype(BF16)
    for v in range(videos):
        cols = slice(v * patches, (v + 1) * patches)
        for h in range(heads):
            s_ref[v, h] = mm(k_ref[h, :, cols], q_ref[h, :, cols], TN)
    for v in range(videos):
        for h in range(heads):
            p_ref[v, h] = jnp.exp2(s_ref[v, h]).astype(BF16)
    for v in range(videos):
        cols = slice(v * patches, (v + 1) * patches)
        for h in range(0, heads, 2):
            pair = [
                normalized(mm(v_ref[g, :, cols], p_ref[v, g], NN), head_dim) for g in (h, h + 1)
            ]
            a_ref[v, h * head_dim : (h + 2) * head_dim, :] = jnp.concatenate(pair, axis=0).astype(BF16)
    for v in range(videos):
        part = mm(a_ref[v], o_ref[...], TN).astype(BF16)
        part_own[v] = part[:rows]
        part_oth[v] = part[rows:]


def spatial(x_own, x_oth, mod, w, gain, w_out, head_dim):
    videos, rows, width = x_own.shape
    inner = w.shape[1]
    heads = inner // head_dim
    tokens = 2 * rows * videos
    return pl.pallas_call(
        functools.partial(spatial_kernel, head_dim),
        out_shape=[jax.ShapeDtypeStruct((videos, rows, width), BF16)] * 3
        + [jax.ShapeDtypeStruct((videos, width), F32)],
        in_specs=[HBM] * 6,
        out_specs=[VMEM] * 4,
        scratch_shapes=[
            pltpu.VMEM(x_own.shape, BF16),
            pltpu.VMEM(x_own.shape, BF16),
            pltpu.VMEM(mod.shape, F32),
            pltpu.VMEM(gain.shape, F32),
            pltpu.VMEM(w.shape, BF16),
            pltpu.VMEM(w_out.shape, BF16),
            pltpu.VMEM((tokens, width), BF16),
            pltpu.VMEM((heads, head_dim, tokens), BF16),
            pltpu.VMEM((heads, head_dim, tokens), BF16),
            pltpu.VMEM((heads, padded_rows(head_dim), tokens), BF16),
            pltpu.VMEM((videos, heads, 2 * rows, 2 * rows), F32),
            pltpu.VMEM((videos, heads, 2 * rows, 2 * rows), BF16),
            pltpu.VMEM((videos, inner, 2 * rows), BF16),
            pltpu.SemaphoreType.DMA((8,)),
        ],
        compiler_params=pltpu.CompilerParams(vmem_limit_bytes=28 * MIB),
        cost_estimate=pl.CostEstimate(flops=6 * 10**9, transcendentals=10**6, bytes_accessed=8 * 10**6),
        name="spatial",
    )(hbm(x_own), x_oth, hbm(mod), hbm(w), hbm(gain), hbm(w_out))


def middle(x_own, own, got, gate):
    total = (own.astype(F32) + got.astype(F32)).astype(BF16).astype(F32)
    return (x_own.astype(F32) + gate[:, None, :] * total).astype(BF16)


def late_kernel(
    head_dim, parts, frames, x_ref, mod, gain, qo_hbm, qr_hbm, oo_hbm, or_hbm, io_hbm, ir_hbm, fo_hbm, fr_hbm, out_ref,
    w_ref, o_ref, i_ref, f_ref, n_ref, r_ref, q_ref, k_ref, v_ref, s_ref, p_ref, a_ref, h_ref, sems,
):
    tokens, _ = x_ref.shape
    each = tokens // parts
    share = each // frames
    heads = q_ref.shape[0]
    inner = w_ref.shape[2]
    half = heads // 2
    fetch = Fetches(sems)
    q_hbms, o_hbms, i_hbms, f_hbms = (qo_hbm, qr_hbm), (oo_hbm, or_hbm), (io_hbm, ir_hbm), (fo_hbm, fr_hbm)

    for side in range(2):
        fetch.start(f"q{side}", q_hbms[side].at[0], w_ref.at[side, 0])

    block = 16 if tokens % 32 == 0 else tokens // 2

    def pieces():
        for start in range(0, tokens, block):
            rows = slice(start, start + block)
            yield rows, x_ref[rows, :].astype(F32)

    for index, (rows, values) in enumerate(pieces()):
        if index == tokens // (2 * block):
            for side in range(2):
                fetch.start(f"k{side}", q_hbms[side].at[1], w_ref.at[side, 1])
        normed = norm_rows(values) * (1.0 + mod[4:5, :]) + mod[3:4, :]
        n_ref[rows, :] = normed.astype(BF16)
    factor = math.log2(math.e) / math.sqrt(head_dim)
    columns = [column(gain[which : which + 1, :]) for which in range(2)]
    quarter = half // 2

    def project(side, which, target):
        for part in range(2):
            rows = slice(part * quarter * head_dim, (part + 1) * quarter * head_dim)
            projected = mm(w_ref[side, which, rows], n_ref[...], NT).reshape(quarter, head_dim, tokens)
            if which < 2:
                projected = head_norm(projected, columns[which] * factor if which == 0 else columns[which])
            else:
                projected = with_ones(projected)
            at = side * half + part * quarter
            target[at : at + quarter] = projected.astype(BF16)

    fetch.wait("q0", "q1")
    for side in range(2):
        fetch.start(f"v{side}", q_hbms[side].at[2], w_ref.at[side, 2])
        fetch.start(f"out{side}", o_hbms[side], o_ref.at[side])
    project(0, 0, q_ref)
    project(1, 0, q_ref)
    fetch.wait("k0", "k1")
    for side in range(2):
        fetch.start(f"in{side}", i_hbms[side], i_ref.at[side])
    project(0, 1, k_ref)
    project(1, 1, k_ref)
    for h in range(heads):
        for v in range(parts):
            cols = slice(v * each, (v + 1) * each)
            s_ref[h, v] = mm(k_ref[h, :, cols], q_ref[h, :, cols], TN)
    first = lax.broadcasted_iota(jnp.int32, (share, each), 0)
    second = lax.broadcasted_iota(jnp.int32, (share, each), 1)
    same = (first == lax.rem(second, share))[None]
    for h in range(heads):
        for v in range(parts):
            weights = jnp.exp2(s_ref[h, v]).reshape(frames, share, each)
            p_ref[h, v] = jnp.where(same, weights, 0.0).reshape(each, each).astype(BF16)
    fetch.wait("v0", "v1", "out0", "out1")
    for side in range(2):
        fetch.start(f"down{side}", f_hbms[side], f_ref.at[side])
    project(0, 2, v_ref)
    project(1, 2, v_ref)
    for h in range(0, heads, 2):
        for v in range(parts):
            cols = slice(v * each, (v + 1) * each)
            pair = [
                normalized(mm(v_ref[g, :, cols], p_ref[g, v], NN), head_dim) for g in (h, h + 1)
            ]
            a_ref[h * head_dim : (h + 2) * head_dim, cols] = jnp.concatenate(pair, axis=0).astype(BF16)
    r_ref[...] = mm(a_ref[:inner, :], o_ref[0], TN) + mm(a_ref[inner:, :], o_ref[1], TN)
    for rows, values in pieces():
        running = values + mod[5:6, :] * r_ref[rows, :].astype(BF16).astype(F32)
        r_ref[rows, :] = running
        normed = norm_rows(running) * (1.0 + mod[7:8, :]) + mod[6:7, :]
        n_ref[rows, :] = normed.astype(BF16)
    fetch.wait("in0", "in1")
    hidden_width = i_ref.shape[2]
    chunk = hidden_width // 3 if hidden_width % 384 == 0 else hidden_width
    for side in range(2):
        for start in range(0, hidden_width, chunk):
            u = mm(n_ref[...], i_ref[side, :, start : start + chunk], NN)
            h_ref[side, :, start : start + chunk] = jax.nn.gelu(u, approximate=True).astype(BF16)
    fetch.wait("down0", "down1")
    mlp = mm(h_ref[0], f_ref[0], NN) + mm(h_ref[1], f_ref[1], NN)
    mlp = mlp.astype(BF16).astype(F32)
    out_ref[...] = (r_ref[...] + mod[8:9, :] * mlp).astype(BF16)


def late(x, early, q_own, q_rem, o_own, o_rem, i_own, i_rem, f_own, f_rem, head_dim, parts, frames):
    tokens, width = x.shape
    inner = q_own.shape[1]
    heads = 2 * inner // head_dim
    return pl.pallas_call(
        functools.partial(late_kernel, head_dim, parts, frames),
        out_shape=jax.ShapeDtypeStruct(x.shape, BF16),
        in_specs=[VMEM] * 3 + [HBM] * 8,
        out_specs=VMEM,
        scratch_shapes=[
            pltpu.VMEM((2,) + q_own.shape, BF16),
            pltpu.VMEM((2,) + o_own.shape, BF16),
            pltpu.VMEM((2,) + i_own.shape, BF16),
            pltpu.VMEM((2,) + f_own.shape, BF16),
            pltpu.VMEM((tokens, width), BF16),
            pltpu.VMEM((tokens, width), F32),
            pltpu.VMEM((heads, head_dim, tokens), BF16),
            pltpu.VMEM((heads, head_dim, tokens), BF16),
            pltpu.VMEM((heads, padded_rows(head_dim), tokens), BF16),
            pltpu.VMEM((heads, parts, tokens // parts, tokens // parts), F32),
            pltpu.VMEM((heads, parts, tokens // parts, tokens // parts), BF16),
            pltpu.VMEM((2 * inner, tokens), BF16),
            pltpu.VMEM((2, tokens, i_own.shape[1]), BF16),
            pltpu.SemaphoreType.DMA((12,)),
        ],
        compiler_params=pltpu.CompilerParams(vmem_limit_bytes=52 * MIB),
        cost_estimate=pl.CostEstimate(flops=9 * 10**9, transcendentals=2 * 10**6, bytes_accessed=33 * 10**6),
        name="late",
    )(x, *early, *(hbm(v) for v in (q_own, q_rem, o_own, o_rem, i_own, i_rem, f_own, f_rem)))


def early_kernel(mod_hbm, gain_hbm, mod, gain, sems):
    fetch = Fetches(sems)
    fetch.start("mod", mod_hbm.at[lax.axis_index("tp")], mod)
    fetch.start("gain", gain_hbm, gain)
    fetch.wait("mod", "gain")


def early_loads(mod, gain):
    return pl.pallas_call(
        early_kernel,
        out_shape=[
            jax.ShapeDtypeStruct(mod.shape[1:], F32),
            jax.ShapeDtypeStruct(gain.shape, F32),
        ],
        in_specs=[HBM] * 2,
        out_specs=[VMEM] * 2,
        scratch_shapes=[pltpu.SemaphoreType.DMA((2,))],
        compiler_params=pltpu.CompilerParams(vmem_limit_bytes=4 * MIB),
        cost_estimate=pl.CostEstimate(flops=10**9, transcendentals=0, bytes_accessed=10**5),
        name="early",
    )(hbm(mod), hbm(gain))


def paired_body(
    seq_size,
    latent,
    modulation,
    qkv_spatial,
    gain_spatial,
    out_spatial,
    qkv_temporal,
    gain_temporal,
    out_temporal,
    fc_in,
    fc_out,
):
    head_dim = gain_spatial.shape[-1]
    videos, _, rows, width = latent.shape

    def swap(value):
        return lax.ppermute(value, "tp", [(0, 1), (1, 0)])

    x_own = latent.reshape(videos, rows, width)
    w_spatial = jnp.swapaxes(qkv_spatial, 1, 2)
    w_temporal = jnp.swapaxes(qkv_temporal, 1, 2)
    mod_rows = jnp.swapaxes(modulation, 0, 1)
    x_oth = swap(x_own)
    q_rem = swap(w_temporal)
    o_rem = swap(out_temporal)
    own, other, x_kept, gate = spatial(
        x_own, x_oth, mod_rows, w_spatial, gain_spatial, out_spatial, head_dim
    )
    other, i_sent, f_sent = lax.optimization_barrier((other, fc_in, fc_out))
    got = swap(other)
    i_rem = swap(i_sent)
    f_rem = swap(f_sent)
    mid = middle(x_kept, own, got, gate)
    both = ("tp", "seq")
    share = rows // seq_size
    moved = lax.all_to_all(mid.reshape(-1, share, width), both, 0, 0, tiled=True)
    early = early_loads(modulation, gain_temporal)
    done = late(
        moved.reshape(-1, width), early, w_temporal, q_rem, out_temporal, o_rem,
        fc_in, i_rem, fc_out, f_rem, head_dim, videos, seq_size,
    )
    back = lax.all_to_all(done.reshape(-1, share, width), both, 0, 0, tiled=True)
    return back.reshape(latent.shape)


def layer_norm(values):
    average = jnp.mean(values, axis=-1, keepdims=True)
    centred = values - average
    variance = jnp.mean(centred * centred, axis=-1, keepdims=True)
    return centred * lax.rsqrt(variance + epsilon)


def modulated(field, modulation, offset):
    shift_row = modulation[:, offset][:, None, None, :]
    scale_row = modulation[:, offset + 1][:, None, None, :]
    return (layer_norm(field) * (1.0 + scale_row) + shift_row).astype(jnp.bfloat16)


def project_heads(rows_piece, table, gains, head_dim):
    results = []
    for which_part in range(3):
        projected = jnp.einsum(
            "bfpd,de->bfpe", rows_piece, table[which_part], preferred_element_type=jnp.float32
        )
        if which_part < 2:
            shaped = projected.reshape(
                projected.shape[:-1] + (projected.shape[-1] // head_dim, head_dim)
            )
            shaped = (
                shaped
                * lax.rsqrt(jnp.mean(shaped * shaped, axis=-1, keepdims=True) + epsilon)
                * gains[which_part]
            )
            projected = shaped.reshape(projected.shape)
        results.append(projected.astype(jnp.bfloat16))
    return jnp.stack(results)


def attend(query_rows, key_rows, value_rows, head_dim):
    groups, length, feature_width = query_rows.shape
    head_count = feature_width // head_dim
    query_heads = query_rows.reshape(groups, length, head_count, head_dim)
    key_heads = key_rows.reshape(groups, length, head_count, head_dim)
    value_heads = value_rows.reshape(groups, length, head_count, head_dim)
    block_rows = min(length, 512)

    def one_block(first_row):
        query_block = lax.dynamic_slice_in_dim(query_heads, first_row, block_rows, 1)
        scores = jnp.einsum(
            "gqhe,gkhe->ghqk", query_block, key_heads, preferred_element_type=jnp.float32
        ) / math.sqrt(head_dim)
        weights = jnp.exp(scores)
        probabilities = (weights / jnp.sum(weights, axis=-1, keepdims=True)).astype(jnp.bfloat16)
        return jnp.einsum(
            "ghqk,gkhe->gqhe", probabilities, value_heads, preferred_element_type=jnp.float32
        ).astype(jnp.bfloat16)

    starts = jnp.arange(length // block_rows, dtype=jnp.int32) * block_rows
    pieces = lax.map(one_block, starts)
    return pieces.transpose(1, 0, 2, 3, 4).reshape(groups, length, feature_width)


def frame_attention(query_rows, key_rows, value_rows, head_dim):
    batches, frames, patches, feature_width = query_rows.shape
    members = [
        item.transpose(0, 2, 1, 3).reshape(batches * patches, frames, feature_width)
        for item in (query_rows, key_rows, value_rows)
    ]
    mixed_heads = attend(members[0], members[1], members[2], head_dim)
    return mixed_heads.reshape(batches, patches, frames, feature_width).transpose(0, 2, 1, 3)


def body(
    latent,
    modulation,
    qkv_spatial,
    gain_spatial,
    out_spatial,
    qkv_temporal,
    gain_temporal,
    out_temporal,
    fc_in,
    fc_out,
):
    head_dim = gain_spatial.shape[-1]
    running = latent.astype(jnp.float32)
    normed = modulated(running, modulation, 0)
    packed = project_heads(
        lax.all_gather(normed, "tp", axis=2, tiled=True), qkv_spatial, gain_spatial, head_dim
    )
    batches, frames, patches, local_width = packed.shape[1:]
    mixed_heads = attend(
        packed[0].reshape(batches * frames, patches, local_width),
        packed[1].reshape(batches * frames, patches, local_width),
        packed[2].reshape(batches * frames, patches, local_width),
        head_dim,
    )
    mixed_heads = mixed_heads.reshape(batches, frames, patches, local_width)
    partial_value = jnp.einsum(
        "bfpe,ed->bfpd", mixed_heads, out_spatial, preferred_element_type=jnp.float32
    )
    spatial_out = lax.psum_scatter(
        partial_value.astype(jnp.bfloat16), "tp", scatter_dimension=2, tiled=True
    )
    running = running + modulation[:, 2][:, None, None, :] * spatial_out.astype(jnp.float32)
    normed = modulated(running, modulation, 3)
    moved_rows = lax.all_to_all(normed, "seq", split_axis=2, concat_axis=1, tiled=True)
    packed = project_heads(
        lax.all_gather(moved_rows, "tp", axis=2, tiled=True), qkv_temporal, gain_temporal, head_dim
    )
    mixed_heads = frame_attention(packed[0], packed[1], packed[2], head_dim)
    partial_value = jnp.einsum(
        "bfpe,ed->bfpd", mixed_heads, out_temporal, preferred_element_type=jnp.float32
    )
    shares = lax.psum_scatter(
        partial_value.astype(jnp.bfloat16), "tp", scatter_dimension=2, tiled=True
    )
    temporal_out = lax.all_to_all(shares, "seq", split_axis=1, concat_axis=2, tiled=True)
    running = running + modulation[:, 5][:, None, None, :] * temporal_out.astype(jnp.float32)
    normed = modulated(running, modulation, 6)
    projected = jnp.einsum(
        "bfpd,de->bfpe",
        lax.all_gather(normed, "tp", axis=2, tiled=True),
        fc_in,
        preferred_element_type=jnp.float32,
    )
    hidden = jax.nn.gelu(projected, approximate=True).astype(jnp.bfloat16)
    partial_value = jnp.einsum("bfpe,ed->bfpd", hidden, fc_out, preferred_element_type=jnp.float32)
    mlp_out = lax.psum_scatter(
        partial_value.astype(jnp.bfloat16), "tp", scatter_dimension=2, tiled=True
    )
    return (running + modulation[:, 8][:, None, None, :] * mlp_out.astype(jnp.float32)).astype(
        jnp.bfloat16
    )


def fits(mesh, videos, local_frames, local_rows, heads_here):
    return (
        mesh.shape["tp"] == 2
        and videos == 2
        and local_frames == 1
        and local_rows % (8 * mesh.shape["seq"]) == 0
        and heads_here % 2 == 0
    )


def solution(mesh):
    placed = (
        P(None, "seq", "tp", None),
        P(),
        P(None, None, "tp"),
        P(),
        P("tp", None),
        P(None, None, "tp"),
        P(),
        P("tp", None),
        P(None, "tp"),
        P("tp", None),
    )

    def step(*args):
        latent, qkv, gain = args[0], args[2], args[3]
        if fits(mesh, latent.shape[0], latent.shape[1], latent.shape[2], qkv.shape[2] // gain.shape[1]):
            return paired_body(mesh.shape["seq"], *args)
        return body(*args)

    return jax.shard_map(
        step, mesh=mesh, in_specs=placed, out_specs=P(None, "seq", "tp", None), check_vma=False
    )
```

```python
import functools
import math

import jax
import jax.numpy as jnp
from jax import lax
from jax.experimental import pallas as pl
from jax.experimental.pallas import tpu as pltpu
from jax.sharding import PartitionSpec as P


epsilon = 1e-06
F32 = jnp.float32
BF16 = jnp.bfloat16
VMEM = pl.BlockSpec(memory_space=pltpu.VMEM)
HBM = pl.BlockSpec(memory_space=pltpu.HBM)

MIB = 1 << 20

NT = (((1,), (1,)), ((), ()))
TN = (((0,), (0,)), ((), ()))
NN = (((1,), (0,)), ((), ()))


def mm(a, b, dims):
    return lax.dot_general(a, b, dims, preferred_element_type=F32)


def hbm(value):
    return pltpu.with_memory_space_constraint(value, pltpu.HBM)


class Fetches:
    def __init__(self, sems):
        self.sems, self.made = sems, {}

    def start(self, name, source, target):
        copy = pltpu.make_async_copy(source, target, self.sems.at[len(self.made)])
        copy.start()
        self.made[name] = copy

    def wait(self, *names):
        for name in names:
            self.made[name].wait()


def norm_rows(values):
    average = jnp.mean(values, axis=-1, keepdims=True)
    centred = values - average
    variance = jnp.mean(centred * centred, axis=-1, keepdims=True)
    return centred * lax.rsqrt(variance + epsilon)


def column(row):
    n = row.shape[1]
    diagonal = lax.broadcasted_iota(jnp.int32, (n, n), 0) == lax.broadcasted_iota(jnp.int32, (n, n), 1)
    return jnp.sum(jnp.where(diagonal, row, 0.0), axis=1, keepdims=True)


def head_norm(projected, gain):
    mean_square = jnp.mean(projected * projected, axis=1, keepdims=True)
    return projected * lax.rsqrt(mean_square + epsilon) * gain[None]


def padded_rows(head_dim):
    return -(-(head_dim + 1) // 16) * 16


def with_ones(values):
    heads, head_dim, tokens = values.shape
    extra = padded_rows(head_dim) - head_dim
    place = lax.broadcasted_iota(jnp.int32, (heads, extra, tokens), 1)
    return jnp.concatenate([values, jnp.where(place == 0, 1.0, 0.0)], axis=1)


def normalized(mixed, head_dim):
    return mixed[:head_dim] * (1.0 / mixed[head_dim : head_dim + 1])


def spatial_kernel(
    head_dim, own_hbm, oth_hbm, mod_hbm, w_hbm, gain_hbm, o_hbm, part_own, part_oth, x_out, gate_out,
    x_own, x_oth, mod, gain, w_ref, o_ref, n_ref, q_ref, k_ref, v_ref, s_ref, p_ref, a_ref, sems,
):
    videos, rows, _ = part_own.shape
    patches = 2 * rows
    heads = w_ref.shape[1] // head_dim
    fetch = Fetches(sems)
    fetch.start("own", own_hbm, x_own)
    fetch.start("mod", mod_hbm, mod)
    fetch.start("oth", oth_hbm, x_oth)
    fetch.start("gain", gain_hbm, gain)
    for which in range(3):
        fetch.start(which, w_hbm.at[which], w_ref.at[which])
    fetch.start("out", o_hbm, o_ref)
    block = 16 if rows % 16 == 0 else rows
    fetch.wait("own", "mod", "gain")
    x_out[...] = x_own[...]
    gate_out[...] = mod[2]
    for v in range(videos):
        for place, source in enumerate((x_own, x_oth)):
            if v == 0 and place == 1:
                fetch.wait("oth")
            base = v * patches + place * rows
            for start in range(0, rows, block):
                normed = norm_rows(source[v, start : start + block].astype(F32))
                normed = normed * (1.0 + mod[1, v : v + 1, :]) + mod[0, v : v + 1, :]
                n_ref[base + start : base + start + block, :] = normed.astype(BF16)
    factor = math.log2(math.e) / math.sqrt(head_dim)
    for which, target in enumerate((q_ref, k_ref, v_ref)):
        if which == 0:
            fetch.wait(0)
        elif which == 1:
            fetch.wait(1, 2, "out")
        projected = mm(w_ref[which], n_ref[...], NT)
        projected = projected.reshape(heads, head_dim, videos * patches)
        if which < 2:
            gains = column(gain[which : which + 1, :])
            projected = head_norm(projected, gains * factor if which == 0 else gains)
        else:
            projected = with_ones(projected)
        target[...] = projected.astype(BF16)
    for v in range(videos):
        cols = slice(v * patches, (v + 1) * patches)
        for h in range(heads):
            s_ref[v, h] = mm(k_ref[h, :, cols], q_ref[h, :, cols], TN)
    for v in range(videos):
        for h in range(heads):
            p_ref[v, h] = jnp.exp2(s_ref[v, h]).astype(BF16)
    for v in range(videos):
        cols = slice(v * patches, (v + 1) * patches)
        for h in range(0, heads, 2):
            pair = [
                normalized(mm(v_ref[g, :, cols], p_ref[v, g], NN), head_dim) for g in (h, h + 1)
            ]
            a_ref[v, h * head_dim : (h + 2) * head_dim, :] = jnp.concatenate(pair, axis=0).astype(BF16)
    for v in range(videos):
        part = mm(a_ref[v], o_ref[...], TN).astype(BF16)
        part_own[v] = part[:rows]
        part_oth[v] = part[rows:]


def spatial(x_own, x_oth, mod, w, gain, w_out, head_dim):
    videos, rows, width = x_own.shape
    inner = w.shape[1]
    heads = inner // head_dim
    tokens = 2 * rows * videos
    return pl.pallas_call(
        functools.partial(spatial_kernel, head_dim),
        out_shape=[jax.ShapeDtypeStruct((videos, rows, width), BF16)] * 3
        + [jax.ShapeDtypeStruct((videos, width), F32)],
        in_specs=[HBM] * 6,
        out_specs=[VMEM] * 4,
        scratch_shapes=[
            pltpu.VMEM(x_own.shape, BF16),
            pltpu.VMEM(x_own.shape, BF16),
            pltpu.VMEM(mod.shape, F32),
            pltpu.VMEM(gain.shape, F32),
            pltpu.VMEM(w.shape, BF16),
            pltpu.VMEM(w_out.shape, BF16),
            pltpu.VMEM((tokens, width), BF16),
            pltpu.VMEM((heads, head_dim, tokens), BF16),
            pltpu.VMEM((heads, head_dim, tokens), BF16),
            pltpu.VMEM((heads, padded_rows(head_dim), tokens), BF16),
            pltpu.VMEM((videos, heads, 2 * rows, 2 * rows), F32),
            pltpu.VMEM((videos, heads, 2 * rows, 2 * rows), BF16),
            pltpu.VMEM((videos, inner, 2 * rows), BF16),
            pltpu.SemaphoreType.DMA((8,)),
        ],
        compiler_params=pltpu.CompilerParams(vmem_limit_bytes=28 * MIB),
        cost_estimate=pl.CostEstimate(flops=6 * 10**9, transcendentals=10**6, bytes_accessed=8 * 10**6),
        name="spatial",
    )(hbm(x_own), x_oth, hbm(mod), hbm(w), hbm(gain), hbm(w_out))


def middle_kernel(x_ref, own_ref, got_ref, gate_ref, out_ref):
    videos = x_ref.shape[0]
    peers, group, _ = out_ref.shape
    share = group // videos
    for d in range(peers):
        there = slice(d * share, (d + 1) * share)
        parts = []
        for v in range(videos):
            total = own_ref[v, there].astype(F32) + got_ref[v, there].astype(F32)
            total = total.astype(BF16).astype(F32)
            parts.append(x_ref[v, there].astype(F32) + gate_ref[v : v + 1, :] * total)
        out_ref[d] = jnp.concatenate(parts, axis=0).astype(BF16)


def middle(x_own, own, got, gate, peers):
    videos, rows, width = x_own.shape
    return pl.pallas_call(
        middle_kernel,
        out_shape=jax.ShapeDtypeStruct((peers, videos * rows // peers, width), BF16),
        in_specs=[VMEM] * 4,
        out_specs=VMEM,
        compiler_params=pltpu.CompilerParams(vmem_limit_bytes=16 * MIB),
        cost_estimate=pl.CostEstimate(flops=10**8, transcendentals=0, bytes_accessed=10**6),
        name="middle",
    )(x_own, own, got, gate)


def late_kernel(
    head_dim, parts, x_ref, mod, gain, qo_hbm, qr_hbm, oo_hbm, or_hbm, io_hbm, ir_hbm, fo_hbm, fr_hbm, out_ref,
    w_ref, o_ref, i_ref, f_ref, n_ref, r_ref, q_ref, k_ref, v_ref, s_ref, p_ref, a_ref, h_ref, sems,
):
    frames, group, _ = x_ref.shape
    share = group // parts
    tokens = frames * group
    heads = q_ref.shape[0]
    inner = w_ref.shape[2]
    half = heads // 2
    fetch = Fetches(sems)
    q_hbms, o_hbms, i_hbms, f_hbms = (qo_hbm, qr_hbm), (oo_hbm, or_hbm), (io_hbm, ir_hbm), (fo_hbm, fr_hbm)

    for side in range(2):
        fetch.start(f"q{side}", q_hbms[side].at[0], w_ref.at[side, 0])
    for side in range(2):
        fetch.start(f"k{side}", q_hbms[side].at[1], w_ref.at[side, 1])

    each = frames * share
    step = 2 if frames % 2 == 0 else 1

    def pieces():
        for v in range(parts):
            for f in range(0, frames, step):
                rows = [x_ref[f + i].astype(F32)[v * share : (v + 1) * share] for i in range(step)]
                start = v * each + f * share
                yield slice(start, start + step * share), jnp.concatenate(rows, axis=0)

    for index, (rows, values) in enumerate(pieces()):
        if index == tokens // (2 * step * share):
            for side in range(2):
                fetch.start(f"v{side}", q_hbms[side].at[2], w_ref.at[side, 2])
        normed = norm_rows(values) * (1.0 + mod[4:5, :]) + mod[3:4, :]
        n_ref[rows, :] = normed.astype(BF16)
    factor = math.log2(math.e) / math.sqrt(head_dim)
    columns = [column(gain[which : which + 1, :]) for which in range(2)]
    quarter = half // 2

    def project(side, which, target):
        for part in range(2):
            rows = slice(part * quarter * head_dim, (part + 1) * quarter * head_dim)
            projected = mm(w_ref[side, which, rows], n_ref[...], NT).reshape(quarter, head_dim, tokens)
            if which < 2:
                projected = head_norm(projected, columns[which] * factor if which == 0 else columns[which])
            else:
                projected = with_ones(projected)
            at = side * half + part * quarter
            target[at : at + quarter] = projected.astype(BF16)

    fetch.wait("q0", "q1")
    for side in range(2):
        fetch.start(f"out{side}", o_hbms[side], o_ref.at[side])
    project(0, 0, q_ref)
    project(1, 0, q_ref)
    fetch.wait("k0", "k1")
    for side in range(2):
        fetch.start(f"in{side}", i_hbms[side], i_ref.at[side])
    project(0, 1, k_ref)
    project(1, 1, k_ref)
    for h in range(heads):
        for v in range(parts):
            cols = slice(v * each, (v + 1) * each)
            s_ref[h, v] = mm(k_ref[h, :, cols], q_ref[h, :, cols], TN)
    first = lax.broadcasted_iota(jnp.int32, (share, each), 0)
    second = lax.broadcasted_iota(jnp.int32, (share, each), 1)
    same = (first == lax.rem(second, share))[None]
    for h in range(heads):
        for v in range(parts):
            weights = jnp.exp2(s_ref[h, v]).reshape(frames, share, each)
            p_ref[h, v] = jnp.where(same, weights, 0.0).reshape(each, each).astype(BF16)
    fetch.wait("v0", "v1", "out0", "out1")
    for side in range(2):
        fetch.start(f"down{side}", f_hbms[side], f_ref.at[side])
    project(0, 2, v_ref)
    project(1, 2, v_ref)
    for h in range(0, heads, 2):
        for v in range(parts):
            cols = slice(v * each, (v + 1) * each)
            pair = [
                normalized(mm(v_ref[g, :, cols], p_ref[g, v], NN), head_dim) for g in (h, h + 1)
            ]
            a_ref[h * head_dim : (h + 2) * head_dim, cols] = jnp.concatenate(pair, axis=0).astype(BF16)
    r_ref[...] = mm(a_ref[:inner, :], o_ref[0], TN) + mm(a_ref[inner:, :], o_ref[1], TN)
    for rows, values in pieces():
        running = values + mod[5:6, :] * r_ref[rows, :].astype(BF16).astype(F32)
        r_ref[rows, :] = running
        normed = norm_rows(running) * (1.0 + mod[7:8, :]) + mod[6:7, :]
        n_ref[rows, :] = normed.astype(BF16)
    fetch.wait("in0", "in1")
    hidden_width = i_ref.shape[2]
    chunk = hidden_width // 9 if hidden_width % 1152 == 0 else hidden_width
    for side in range(2):
        for start in range(0, hidden_width, chunk):
            u = mm(n_ref[...], i_ref[side, :, start : start + chunk], NN)
            h_ref[side, :, start : start + chunk] = jax.nn.gelu(u, approximate=True).astype(BF16)
    fetch.wait("down0", "down1")
    mlp = mm(h_ref[0], f_ref[0], NN) + mm(h_ref[1], f_ref[1], NN)
    mlp = mlp.astype(BF16).astype(F32)
    for f in range(frames):
        blocks = []
        for v in range(parts):
            rows = slice(v * each + f * share, v * each + (f + 1) * share)
            blocks.append(r_ref[rows, :] + mod[8:9, :] * mlp[rows])
        out_ref[f] = jnp.concatenate(blocks, axis=0).astype(BF16)


def late(x, early, q_own, q_rem, o_own, o_rem, i_own, i_rem, f_own, f_rem, head_dim, parts):
    frames, group, width = x.shape
    tokens = frames * group
    inner = q_own.shape[1]
    heads = 2 * inner // head_dim
    return pl.pallas_call(
        functools.partial(late_kernel, head_dim, parts),
        out_shape=jax.ShapeDtypeStruct(x.shape, BF16),
        in_specs=[VMEM] * 3 + [HBM] * 8,
        out_specs=VMEM,
        scratch_shapes=[
            pltpu.VMEM((2,) + q_own.shape, BF16),
            pltpu.VMEM((2,) + o_own.shape, BF16),
            pltpu.VMEM((2,) + i_own.shape, BF16),
            pltpu.VMEM((2,) + f_own.shape, BF16),
            pltpu.VMEM((tokens, width), BF16),
            pltpu.VMEM((tokens, width), F32),
            pltpu.VMEM((heads, head_dim, tokens), BF16),
            pltpu.VMEM((heads, head_dim, tokens), BF16),
            pltpu.VMEM((heads, padded_rows(head_dim), tokens), BF16),
            pltpu.VMEM((heads, parts, tokens // parts, tokens // parts), F32),
            pltpu.VMEM((heads, parts, tokens // parts, tokens // parts), BF16),
            pltpu.VMEM((2 * inner, tokens), BF16),
            pltpu.VMEM((2, tokens, i_own.shape[1]), BF16),
            pltpu.SemaphoreType.DMA((12,)),
        ],
        compiler_params=pltpu.CompilerParams(vmem_limit_bytes=52 * MIB),
        cost_estimate=pl.CostEstimate(flops=9 * 10**9, transcendentals=2 * 10**6, bytes_accessed=33 * 10**6),
        name="late",
    )(x, *early, *(hbm(v) for v in (q_own, q_rem, o_own, o_rem, i_own, i_rem, f_own, f_rem)))


def early_kernel(mod_hbm, gain_hbm, mod, gain, sems):
    fetch = Fetches(sems)
    fetch.start("mod", mod_hbm.at[lax.axis_index("tp")], mod)
    fetch.start("gain", gain_hbm, gain)
    fetch.wait("mod", "gain")


def early_loads(mod, gain):
    return pl.pallas_call(
        early_kernel,
        out_shape=[
            jax.ShapeDtypeStruct(mod.shape[1:], F32),
            jax.ShapeDtypeStruct(gain.shape, F32),
        ],
        in_specs=[HBM] * 2,
        out_specs=[VMEM] * 2,
        scratch_shapes=[pltpu.SemaphoreType.DMA((2,))],
        compiler_params=pltpu.CompilerParams(vmem_limit_bytes=4 * MIB),
        cost_estimate=pl.CostEstimate(flops=10**9, transcendentals=0, bytes_accessed=10**5),
        name="early",
    )(hbm(mod), hbm(gain))


def paired_body(
    seq_size,
    latent,
    modulation,
    qkv_spatial,
    gain_spatial,
    out_spatial,
    qkv_temporal,
    gain_temporal,
    out_temporal,
    fc_in,
    fc_out,
):
    head_dim = gain_spatial.shape[-1]
    videos, _, rows, width = latent.shape

    def swap(value):
        return lax.ppermute(value, "tp", [(0, 1), (1, 0)])

    x_own = latent.reshape(videos, rows, width)
    w_spatial = jnp.swapaxes(qkv_spatial, 1, 2)
    w_temporal = jnp.swapaxes(qkv_temporal, 1, 2)
    mod_rows = jnp.swapaxes(modulation, 0, 1)
    x_oth = swap(x_own)
    q_rem = swap(w_temporal)
    o_rem = swap(out_temporal)
    own, other, x_kept, gate = spatial(
        x_own, x_oth, mod_rows, w_spatial, gain_spatial, out_spatial, head_dim
    )
    other, i_sent, f_sent = lax.optimization_barrier((other, fc_in, fc_out))
    got = swap(other)
    i_rem = swap(i_sent)
    f_rem = swap(f_sent)
    mid = middle(x_kept, own, got, gate, seq_size)
    both = ("seq", "tp")
    share = rows // seq_size
    moved = lax.all_to_all(mid.reshape(-1, share, width), both, 0, 0, tiled=True)
    early = early_loads(modulation, gain_temporal)
    done = late(
        moved.reshape(mid.shape), early, w_temporal, q_rem, out_temporal, o_rem,
        fc_in, i_rem, fc_out, f_rem, head_dim, mid.shape[1] // share,
    )
    back = lax.all_to_all(done.reshape(-1, share, width), both, 0, 0, tiled=True)
    back = back.reshape(seq_size, videos, share, width).transpose(1, 0, 2, 3)
    return back.reshape(latent.shape)


def layer_norm(values):
    average = jnp.mean(values, axis=-1, keepdims=True)
    centred = values - average
    variance = jnp.mean(centred * centred, axis=-1, keepdims=True)
    return centred * lax.rsqrt(variance + epsilon)


def modulated(field, modulation, offset):
    shift_row = modulation[:, offset][:, None, None, :]
    scale_row = modulation[:, offset + 1][:, None, None, :]
    return (layer_norm(field) * (1.0 + scale_row) + shift_row).astype(jnp.bfloat16)


def project_heads(rows_piece, table, gains, head_dim):
    results = []
    for which_part in range(3):
        projected = jnp.einsum(
            "bfpd,de->bfpe", rows_piece, table[which_part], preferred_element_type=jnp.float32
        )
        if which_part < 2:
            shaped = projected.reshape(
                projected.shape[:-1] + (projected.shape[-1] // head_dim, head_dim)
            )
            shaped = (
                shaped
                * lax.rsqrt(jnp.mean(shaped * shaped, axis=-1, keepdims=True) + epsilon)
                * gains[which_part]
            )
            projected = shaped.reshape(projected.shape)
        results.append(projected.astype(jnp.bfloat16))
    return jnp.stack(results)


def attend(query_rows, key_rows, value_rows, head_dim):
    groups, length, feature_width = query_rows.shape
    head_count = feature_width // head_dim
    query_heads = query_rows.reshape(groups, length, head_count, head_dim)
    key_heads = key_rows.reshape(groups, length, head_count, head_dim)
    value_heads = value_rows.reshape(groups, length, head_count, head_dim)
    block_rows = min(length, 512)

    def one_block(first_row):
        query_block = lax.dynamic_slice_in_dim(query_heads, first_row, block_rows, 1)
        scores = jnp.einsum(
            "gqhe,gkhe->ghqk", query_block, key_heads, preferred_element_type=jnp.float32
        ) / math.sqrt(head_dim)
        weights = jnp.exp(scores)
        probabilities = (weights / jnp.sum(weights, axis=-1, keepdims=True)).astype(jnp.bfloat16)
        return jnp.einsum(
            "ghqk,gkhe->gqhe", probabilities, value_heads, preferred_element_type=jnp.float32
        ).astype(jnp.bfloat16)

    starts = jnp.arange(length // block_rows, dtype=jnp.int32) * block_rows
    pieces = lax.map(one_block, starts)
    return pieces.transpose(1, 0, 2, 3, 4).reshape(groups, length, feature_width)


def frame_attention(query_rows, key_rows, value_rows, head_dim):
    batches, frames, patches, feature_width = query_rows.shape
    members = [
        item.transpose(0, 2, 1, 3).reshape(batches * patches, frames, feature_width)
        for item in (query_rows, key_rows, value_rows)
    ]
    mixed_heads = attend(members[0], members[1], members[2], head_dim)
    return mixed_heads.reshape(batches, patches, frames, feature_width).transpose(0, 2, 1, 3)


def body(
    latent,
    modulation,
    qkv_spatial,
    gain_spatial,
    out_spatial,
    qkv_temporal,
    gain_temporal,
    out_temporal,
    fc_in,
    fc_out,
):
    head_dim = gain_spatial.shape[-1]
    running = latent.astype(jnp.float32)
    normed = modulated(running, modulation, 0)
    packed = project_heads(
        lax.all_gather(normed, "tp", axis=2, tiled=True), qkv_spatial, gain_spatial, head_dim
    )
    batches, frames, patches, local_width = packed.shape[1:]
    mixed_heads = attend(
        packed[0].reshape(batches * frames, patches, local_width),
        packed[1].reshape(batches * frames, patches, local_width),
        packed[2].reshape(batches * frames, patches, local_width),
        head_dim,
    )
    mixed_heads = mixed_heads.reshape(batches, frames, patches, local_width)
    partial_value = jnp.einsum(
        "bfpe,ed->bfpd", mixed_heads, out_spatial, preferred_element_type=jnp.float32
    )
    spatial_out = lax.psum_scatter(
        partial_value.astype(jnp.bfloat16), "tp", scatter_dimension=2, tiled=True
    )
    running = running + modulation[:, 2][:, None, None, :] * spatial_out.astype(jnp.float32)
    normed = modulated(running, modulation, 3)
    moved_rows = lax.all_to_all(normed, "seq", split_axis=2, concat_axis=1, tiled=True)
    packed = project_heads(
        lax.all_gather(moved_rows, "tp", axis=2, tiled=True), qkv_temporal, gain_temporal, head_dim
    )
    mixed_heads = frame_attention(packed[0], packed[1], packed[2], head_dim)
    partial_value = jnp.einsum(
        "bfpe,ed->bfpd", mixed_heads, out_temporal, preferred_element_type=jnp.float32
    )
    shares = lax.psum_scatter(
        partial_value.astype(jnp.bfloat16), "tp", scatter_dimension=2, tiled=True
    )
    temporal_out = lax.all_to_all(shares, "seq", split_axis=1, concat_axis=2, tiled=True)
    running = running + modulation[:, 5][:, None, None, :] * temporal_out.astype(jnp.float32)
    normed = modulated(running, modulation, 6)
    projected = jnp.einsum(
        "bfpd,de->bfpe",
        lax.all_gather(normed, "tp", axis=2, tiled=True),
        fc_in,
        preferred_element_type=jnp.float32,
    )
    hidden = jax.nn.gelu(projected, approximate=True).astype(jnp.bfloat16)
    partial_value = jnp.einsum("bfpe,ed->bfpd", hidden, fc_out, preferred_element_type=jnp.float32)
    mlp_out = lax.psum_scatter(
        partial_value.astype(jnp.bfloat16), "tp", scatter_dimension=2, tiled=True
    )
    return (running + modulation[:, 8][:, None, None, :] * mlp_out.astype(jnp.float32)).astype(
        jnp.bfloat16
    )


def fits(mesh, videos, local_frames, local_rows, heads_here):
    return (
        mesh.shape["tp"] == 2
        and videos == 2
        and local_frames == 1
        and local_rows % (8 * mesh.shape["seq"]) == 0
        and heads_here % 2 == 0
    )


def solution(mesh):
    placed = (
        P(None, "seq", "tp", None),
        P(),
        P(None, None, "tp"),
        P(),
        P("tp", None),
        P(None, None, "tp"),
        P(),
        P("tp", None),
        P(None, "tp"),
        P("tp", None),
    )

    def step(*args):
        latent, qkv, gain = args[0], args[2], args[3]
        if fits(mesh, latent.shape[0], latent.shape[1], latent.shape[2], qkv.shape[2] // gain.shape[1]):
            return paired_body(mesh.shape["seq"], *args)
        return body(*args)

    return jax.shard_map(
        step, mesh=mesh, in_specs=placed, out_specs=P(None, "seq", "tp", None), check_vma=False
    )
```

```python
import functools
import math

import jax
import jax.numpy as jnp
from jax import lax
from jax.experimental import pallas as pl
from jax.experimental.pallas import tpu as pltpu
from jax.sharding import PartitionSpec as P


epsilon = 1e-06
F32 = jnp.float32
BF16 = jnp.bfloat16
VMEM = pl.BlockSpec(memory_space=pltpu.VMEM)
HBM = pl.BlockSpec(memory_space=pltpu.HBM)

MIB = 1 << 20

NT = (((1,), (1,)), ((), ()))
TN = (((0,), (0,)), ((), ()))
NN = (((1,), (0,)), ((), ()))


def mm(a, b, dims):
    return lax.dot_general(a, b, dims, preferred_element_type=F32)


def hbm(value):
    return pltpu.with_memory_space_constraint(value, pltpu.HBM)


class Fetches:
    def __init__(self, sems):
        self.sems, self.made = sems, {}

    def start(self, name, source, target):
        copy = pltpu.make_async_copy(source, target, self.sems.at[len(self.made)])
        copy.start()
        self.made[name] = copy

    def wait(self, *names):
        for name in names:
            self.made[name].wait()


def norm_rows(values):
    average = jnp.mean(values, axis=-1, keepdims=True)
    centred = values - average
    variance = jnp.mean(centred * centred, axis=-1, keepdims=True)
    return centred * lax.rsqrt(variance + epsilon)


def column(row):
    n = row.shape[1]
    diagonal = lax.broadcasted_iota(jnp.int32, (n, n), 0) == lax.broadcasted_iota(jnp.int32, (n, n), 1)
    return jnp.sum(jnp.where(diagonal, row, 0.0), axis=1, keepdims=True)


def head_norm(projected, gain):
    mean_square = jnp.mean(projected * projected, axis=1, keepdims=True)
    return projected * lax.rsqrt(mean_square + epsilon) * gain[None]


def padded_rows(head_dim):
    return -(-(head_dim + 1) // 16) * 16


def with_ones(values):
    heads, head_dim, tokens = values.shape
    extra = padded_rows(head_dim) - head_dim
    place = lax.broadcasted_iota(jnp.int32, (heads, extra, tokens), 1)
    return jnp.concatenate([values, jnp.where(place == 0, 1.0, 0.0)], axis=1)


def normalized(mixed, head_dim):
    return mixed[:head_dim] * (1.0 / mixed[head_dim : head_dim + 1])


def spatial_kernel(
    head_dim, own_hbm, oth_hbm, mod_hbm, w_hbm, gain_hbm, o_hbm, part_own, part_oth, x_out, gate_out,
    x_own, x_oth, mod, gain, w_ref, o_ref, n_ref, q_ref, k_ref, v_ref, s_ref, p_ref, a_ref, sems,
):
    videos, rows, _ = part_own.shape
    patches = 2 * rows
    heads = w_ref.shape[1] // head_dim
    fetch = Fetches(sems)
    fetch.start("own", own_hbm, x_own)
    fetch.start("mod", mod_hbm, mod)
    fetch.start("oth", oth_hbm, x_oth)
    fetch.start("gain", gain_hbm, gain)
    for which in range(3):
        fetch.start(which, w_hbm.at[which], w_ref.at[which])
    fetch.start("out", o_hbm, o_ref)
    block = 16 if rows % 16 == 0 else rows
    fetch.wait("own", "mod", "gain")
    x_out[...] = x_own[...]
    gate_out[...] = mod[2]
    for v in range(videos):
        for place, source in enumerate((x_own, x_oth)):
            if v == 0 and place == 1:
                fetch.wait("oth")
            base = v * patches + place * rows
            for start in range(0, rows, block):
                normed = norm_rows(source[v, start : start + block].astype(F32))
                normed = normed * (1.0 + mod[1, v : v + 1, :]) + mod[0, v : v + 1, :]
                n_ref[base + start : base + start + block, :] = normed.astype(BF16)
    factor = math.log2(math.e) / math.sqrt(head_dim)
    for which, target in enumerate((q_ref, k_ref, v_ref)):
        if which == 0:
            fetch.wait(0)
        elif which == 1:
            fetch.wait(1, 2, "out")
        projected = mm(w_ref[which], n_ref[...], NT)
        projected = projected.reshape(heads, head_dim, videos * patches)
        if which < 2:
            gains = column(gain[which : which + 1, :])
            projected = head_norm(projected, gains * factor if which == 0 else gains)
        else:
            projected = with_ones(projected)
        target[...] = projected.astype(BF16)
    for v in range(videos):
        cols = slice(v * patches, (v + 1) * patches)
        for h in range(heads):
            s_ref[v, h] = mm(k_ref[h, :, cols], q_ref[h, :, cols], TN)
    for v in range(videos):
        for h in range(heads):
            p_ref[v, h] = jnp.exp2(s_ref[v, h]).astype(BF16)
    for v in range(videos):
        cols = slice(v * patches, (v + 1) * patches)
        for h in range(0, heads, 2):
            pair = [
                normalized(mm(v_ref[g, :, cols], p_ref[v, g], NN), head_dim) for g in (h, h + 1)
            ]
            a_ref[v, h * head_dim : (h + 2) * head_dim, :] = jnp.concatenate(pair, axis=0).astype(BF16)
    for v in range(videos):
        part = mm(a_ref[v], o_ref[...], TN).astype(BF16)
        part_own[v] = part[:rows]
        part_oth[v] = part[rows:]


def spatial(x_own, x_oth, mod, w, gain, w_out, head_dim):
    videos, rows, width = x_own.shape
    inner = w.shape[1]
    heads = inner // head_dim
    tokens = 2 * rows * videos
    return pl.pallas_call(
        functools.partial(spatial_kernel, head_dim),
        out_shape=[jax.ShapeDtypeStruct((videos, rows, width), BF16)] * 3
        + [jax.ShapeDtypeStruct((videos, width), F32)],
        in_specs=[HBM] * 6,
        out_specs=[VMEM] * 4,
        scratch_shapes=[
            pltpu.VMEM(x_own.shape, BF16),
            pltpu.VMEM(x_own.shape, BF16),
            pltpu.VMEM(mod.shape, F32),
            pltpu.VMEM(gain.shape, F32),
            pltpu.VMEM(w.shape, BF16),
            pltpu.VMEM(w_out.shape, BF16),
            pltpu.VMEM((tokens, width), BF16),
            pltpu.VMEM((heads, head_dim, tokens), BF16),
            pltpu.VMEM((heads, head_dim, tokens), BF16),
            pltpu.VMEM((heads, padded_rows(head_dim), tokens), BF16),
            pltpu.VMEM((videos, heads, 2 * rows, 2 * rows), F32),
            pltpu.VMEM((videos, heads, 2 * rows, 2 * rows), BF16),
            pltpu.VMEM((videos, inner, 2 * rows), BF16),
            pltpu.SemaphoreType.DMA((8,)),
        ],
        compiler_params=pltpu.CompilerParams(vmem_limit_bytes=28 * MIB),
        cost_estimate=pl.CostEstimate(flops=6 * 10**9, transcendentals=10**6, bytes_accessed=8 * 10**6),
        name="spatial",
    )(hbm(x_own), x_oth, hbm(mod), hbm(w), hbm(gain), hbm(w_out))


def middle_kernel(x_ref, own_ref, got_ref, gate_ref, out_ref):
    videos = x_ref.shape[0]
    peers, group, _ = out_ref.shape
    share = group // videos
    for d in range(peers):
        there = slice(d * share, (d + 1) * share)
        parts = []
        for v in range(videos):
            total = own_ref[v, there].astype(F32) + got_ref[v, there].astype(F32)
            total = total.astype(BF16).astype(F32)
            parts.append(x_ref[v, there].astype(F32) + gate_ref[v : v + 1, :] * total)
        out_ref[d] = jnp.concatenate(parts, axis=0).astype(BF16)


def middle(x_own, own, got, gate, peers):
    videos, rows, width = x_own.shape
    return pl.pallas_call(
        middle_kernel,
        out_shape=jax.ShapeDtypeStruct((peers, videos * rows // peers, width), BF16),
        in_specs=[VMEM] * 4,
        out_specs=VMEM,
        compiler_params=pltpu.CompilerParams(vmem_limit_bytes=16 * MIB),
        cost_estimate=pl.CostEstimate(flops=10**8, transcendentals=0, bytes_accessed=10**6),
        name="middle",
    )(x_own, own, got, gate)


def late_kernel(
    head_dim, parts, x_ref, mod, gain, qo_hbm, qr_hbm, oo_hbm, or_hbm, io_hbm, ir_hbm, fo_hbm, fr_hbm, out_ref,
    w_ref, o_ref, i_ref, f_ref, n_ref, r_ref, q_ref, k_ref, v_ref, s_ref, p_ref, a_ref, h_ref, sems,
):
    frames, group, _ = x_ref.shape
    share = group // parts
    tokens = frames * group
    heads = q_ref.shape[0]
    inner = w_ref.shape[2]
    half = heads // 2
    fetch = Fetches(sems)
    q_hbms, o_hbms, i_hbms, f_hbms = (qo_hbm, qr_hbm), (oo_hbm, or_hbm), (io_hbm, ir_hbm), (fo_hbm, fr_hbm)

    for side in range(2):
        fetch.start(f"q{side}", q_hbms[side].at[0], w_ref.at[side, 0])
    for side in range(2):
        fetch.start(f"k{side}", q_hbms[side].at[1], w_ref.at[side, 1])

    each = frames * share
    step = 2 if frames % 2 == 0 else 1

    def pieces():
        for v in range(parts):
            for f in range(0, frames, step):
                rows = [x_ref[f + i].astype(F32)[v * share : (v + 1) * share] for i in range(step)]
                start = v * each + f * share
                yield slice(start, start + step * share), jnp.concatenate(rows, axis=0)

    for index, (rows, values) in enumerate(pieces()):
        if index == tokens // (2 * step * share):
            for side in range(2):
                fetch.start(f"v{side}", q_hbms[side].at[2], w_ref.at[side, 2])
        normed = norm_rows(values) * (1.0 + mod[4:5, :]) + mod[3:4, :]
        n_ref[rows, :] = normed.astype(BF16)
    factor = math.log2(math.e) / math.sqrt(head_dim)
    columns = [column(gain[which : which + 1, :]) for which in range(2)]
    quarter = half // 2

    def project(side, which, target):
        for part in range(2):
            rows = slice(part * quarter * head_dim, (part + 1) * quarter * head_dim)
            projected = mm(w_ref[side, which, rows], n_ref[...], NT).reshape(quarter, head_dim, tokens)
            if which < 2:
                projected = head_norm(projected, columns[which] * factor if which == 0 else columns[which])
            else:
                projected = with_ones(projected)
            at = side * half + part * quarter
            target[at : at + quarter] = projected.astype(BF16)

    fetch.wait("q0", "q1")
    for side in range(2):
        fetch.start(f"out{side}", o_hbms[side], o_ref.at[side])
    project(0, 0, q_ref)
    project(1, 0, q_ref)
    fetch.wait("k0", "k1")
    for side in range(2):
        fetch.start(f"in{side}", i_hbms[side], i_ref.at[side])
    project(0, 1, k_ref)
    project(1, 1, k_ref)
    for h in range(heads):
        for v in range(parts):
            cols = slice(v * each, (v + 1) * each)
            s_ref[h, v] = mm(k_ref[h, :, cols], q_ref[h, :, cols], TN)
    first = lax.broadcasted_iota(jnp.int32, (share, each), 0)
    second = lax.broadcasted_iota(jnp.int32, (share, each), 1)
    same = (first == lax.rem(second, share))[None]
    for h in range(heads):
        for v in range(parts):
            weights = jnp.exp2(s_ref[h, v]).reshape(frames, share, each)
            p_ref[h, v] = jnp.where(same, weights, 0.0).reshape(each, each).astype(BF16)
    fetch.wait("v0", "v1", "out0", "out1")
    for side in range(2):
        fetch.start(f"down{side}", f_hbms[side], f_ref.at[side])
    project(0, 2, v_ref)
    project(1, 2, v_ref)
    for h in range(0, heads, 2):
        for v in range(parts):
            cols = slice(v * each, (v + 1) * each)
            pair = [
                normalized(mm(v_ref[g, :, cols], p_ref[g, v], NN), head_dim) for g in (h, h + 1)
            ]
            a_ref[h * head_dim : (h + 2) * head_dim, cols] = jnp.concatenate(pair, axis=0).astype(BF16)
    r_ref[...] = mm(a_ref[:inner, :], o_ref[0], TN) + mm(a_ref[inner:, :], o_ref[1], TN)
    for rows, values in pieces():
        running = values + mod[5:6, :] * r_ref[rows, :].astype(BF16).astype(F32)
        r_ref[rows, :] = running
        normed = norm_rows(running) * (1.0 + mod[7:8, :]) + mod[6:7, :]
        n_ref[rows, :] = normed.astype(BF16)
    fetch.wait("in0", "in1")
    hidden_width = i_ref.shape[2]
    chunk = hidden_width // 9 if hidden_width % 1152 == 0 else hidden_width
    for side in range(2):
        for start in range(0, hidden_width, chunk):
            u = mm(n_ref[...], i_ref[side, :, start : start + chunk], NN)
            h_ref[side, :, start : start + chunk] = jax.nn.gelu(u, approximate=True).astype(BF16)
    fetch.wait("down0", "down1")
    mlp = mm(h_ref[0], f_ref[0], NN) + mm(h_ref[1], f_ref[1], NN)
    mlp = mlp.astype(BF16).astype(F32)
    out_ref[...] = (r_ref[...] + mod[8:9, :] * mlp).astype(BF16)


def late(x, early, q_own, q_rem, o_own, o_rem, i_own, i_rem, f_own, f_rem, head_dim, parts):
    frames, group, width = x.shape
    tokens = frames * group
    inner = q_own.shape[1]
    heads = 2 * inner // head_dim
    return pl.pallas_call(
        functools.partial(late_kernel, head_dim, parts),
        out_shape=jax.ShapeDtypeStruct((tokens, width), BF16),
        in_specs=[VMEM] * 3 + [HBM] * 8,
        out_specs=VMEM,
        scratch_shapes=[
            pltpu.VMEM((2,) + q_own.shape, BF16),
            pltpu.VMEM((2,) + o_own.shape, BF16),
            pltpu.VMEM((2,) + i_own.shape, BF16),
            pltpu.VMEM((2,) + f_own.shape, BF16),
            pltpu.VMEM((tokens, width), BF16),
            pltpu.VMEM((tokens, width), F32),
            pltpu.VMEM((heads, head_dim, tokens), BF16),
            pltpu.VMEM((heads, head_dim, tokens), BF16),
            pltpu.VMEM((heads, padded_rows(head_dim), tokens), BF16),
            pltpu.VMEM((heads, parts, tokens // parts, tokens // parts), F32),
            pltpu.VMEM((heads, parts, tokens // parts, tokens // parts), BF16),
            pltpu.VMEM((2 * inner, tokens), BF16),
            pltpu.VMEM((2, tokens, i_own.shape[1]), BF16),
            pltpu.SemaphoreType.DMA((12,)),
        ],
        compiler_params=pltpu.CompilerParams(vmem_limit_bytes=52 * MIB),
        cost_estimate=pl.CostEstimate(flops=9 * 10**9, transcendentals=2 * 10**6, bytes_accessed=33 * 10**6),
        name="late",
    )(x, *early, *(hbm(v) for v in (q_own, q_rem, o_own, o_rem, i_own, i_rem, f_own, f_rem)))


def early_kernel(mod_hbm, gain_hbm, mod, gain, sems):
    fetch = Fetches(sems)
    fetch.start("mod", mod_hbm.at[lax.axis_index("tp")], mod)
    fetch.start("gain", gain_hbm, gain)
    fetch.wait("mod", "gain")


def early_loads(mod, gain):
    return pl.pallas_call(
        early_kernel,
        out_shape=[
            jax.ShapeDtypeStruct(mod.shape[1:], F32),
            jax.ShapeDtypeStruct(gain.shape, F32),
        ],
        in_specs=[HBM] * 2,
        out_specs=[VMEM] * 2,
        scratch_shapes=[pltpu.SemaphoreType.DMA((2,))],
        compiler_params=pltpu.CompilerParams(vmem_limit_bytes=4 * MIB),
        cost_estimate=pl.CostEstimate(flops=10**9, transcendentals=0, bytes_accessed=10**5),
        name="early",
    )(hbm(mod), hbm(gain))


def paired_body(
    seq_size,
    latent,
    modulation,
    qkv_spatial,
    gain_spatial,
    out_spatial,
    qkv_temporal,
    gain_temporal,
    out_temporal,
    fc_in,
    fc_out,
):
    head_dim = gain_spatial.shape[-1]
    videos, _, rows, width = latent.shape

    def swap(value):
        return lax.ppermute(value, "tp", [(0, 1), (1, 0)])

    x_own = latent.reshape(videos, rows, width)
    w_spatial = jnp.swapaxes(qkv_spatial, 1, 2)
    w_temporal = jnp.swapaxes(qkv_temporal, 1, 2)
    mod_rows = jnp.swapaxes(modulation, 0, 1)
    x_oth = swap(x_own)
    q_rem = swap(w_temporal)
    o_rem = swap(out_temporal)
    own, other, x_kept, gate = spatial(
        x_own, x_oth, mod_rows, w_spatial, gain_spatial, out_spatial, head_dim
    )
    other, i_sent, f_sent = lax.optimization_barrier((other, fc_in, fc_out))
    got = swap(other)
    i_rem = swap(i_sent)
    f_rem = swap(f_sent)
    mid = middle(x_kept, own, got, gate, seq_size)
    both = ("seq", "tp")
    share = rows // seq_size
    moved = lax.all_to_all(mid.reshape(-1, share, width), both, 0, 0, tiled=True)
    early = early_loads(modulation, gain_temporal)
    done = late(
        moved.reshape(mid.shape), early, w_temporal, q_rem, out_temporal, o_rem,
        fc_in, i_rem, fc_out, f_rem, head_dim, mid.shape[1] // share,
    )
    back = lax.all_to_all(done.reshape(-1, share, width), ("tp", "seq"), 0, 0, tiled=True)
    return back.reshape(latent.shape)


def layer_norm(values):
    average = jnp.mean(values, axis=-1, keepdims=True)
    centred = values - average
    variance = jnp.mean(centred * centred, axis=-1, keepdims=True)
    return centred * lax.rsqrt(variance + epsilon)


def modulated(field, modulation, offset):
    shift_row = modulation[:, offset][:, None, None, :]
    scale_row = modulation[:, offset + 1][:, None, None, :]
    return (layer_norm(field) * (1.0 + scale_row) + shift_row).astype(jnp.bfloat16)


def project_heads(rows_piece, table, gains, head_dim):
    results = []
    for which_part in range(3):
        projected = jnp.einsum(
            "bfpd,de->bfpe", rows_piece, table[which_part], preferred_element_type=jnp.float32
        )
        if which_part < 2:
            shaped = projected.reshape(
                projected.shape[:-1] + (projected.shape[-1] // head_dim, head_dim)
            )
            shaped = (
                shaped
                * lax.rsqrt(jnp.mean(shaped * shaped, axis=-1, keepdims=True) + epsilon)
                * gains[which_part]
            )
            projected = shaped.reshape(projected.shape)
        results.append(projected.astype(jnp.bfloat16))
    return jnp.stack(results)


def attend(query_rows, key_rows, value_rows, head_dim):
    groups, length, feature_width = query_rows.shape
    head_count = feature_width // head_dim
    query_heads = query_rows.reshape(groups, length, head_count, head_dim)
    key_heads = key_rows.reshape(groups, length, head_count, head_dim)
    value_heads = value_rows.reshape(groups, length, head_count, head_dim)
    block_rows = min(length, 512)

    def one_block(first_row):
        query_block = lax.dynamic_slice_in_dim(query_heads, first_row, block_rows, 1)
        scores = jnp.einsum(
            "gqhe,gkhe->ghqk", query_block, key_heads, preferred_element_type=jnp.float32
        ) / math.sqrt(head_dim)
        weights = jnp.exp(scores)
        probabilities = (weights / jnp.sum(weights, axis=-1, keepdims=True)).astype(jnp.bfloat16)
        return jnp.einsum(
            "ghqk,gkhe->gqhe", probabilities, value_heads, preferred_element_type=jnp.float32
        ).astype(jnp.bfloat16)

    starts = jnp.arange(length // block_rows, dtype=jnp.int32) * block_rows
    pieces = lax.map(one_block, starts)
    return pieces.transpose(1, 0, 2, 3, 4).reshape(groups, length, feature_width)


def frame_attention(query_rows, key_rows, value_rows, head_dim):
    batches, frames, patches, feature_width = query_rows.shape
    members = [
        item.transpose(0, 2, 1, 3).reshape(batches * patches, frames, feature_width)
        for item in (query_rows, key_rows, value_rows)
    ]
    mixed_heads = attend(members[0], members[1], members[2], head_dim)
    return mixed_heads.reshape(batches, patches, frames, feature_width).transpose(0, 2, 1, 3)


def body(
    latent,
    modulation,
    qkv_spatial,
    gain_spatial,
    out_spatial,
    qkv_temporal,
    gain_temporal,
    out_temporal,
    fc_in,
    fc_out,
):
    head_dim = gain_spatial.shape[-1]
    running = latent.astype(jnp.float32)
    normed = modulated(running, modulation, 0)
    packed = project_heads(
        lax.all_gather(normed, "tp", axis=2, tiled=True), qkv_spatial, gain_spatial, head_dim
    )
    batches, frames, patches, local_width = packed.shape[1:]
    mixed_heads = attend(
        packed[0].reshape(batches * frames, patches, local_width),
        packed[1].reshape(batches * frames, patches, local_width),
        packed[2].reshape(batches * frames, patches, local_width),
        head_dim,
    )
    mixed_heads = mixed_heads.reshape(batches, frames, patches, local_width)
    partial_value = jnp.einsum(
        "bfpe,ed->bfpd", mixed_heads, out_spatial, preferred_element_type=jnp.float32
    )
    spatial_out = lax.psum_scatter(
        partial_value.astype(jnp.bfloat16), "tp", scatter_dimension=2, tiled=True
    )
    running = running + modulation[:, 2][:, None, None, :] * spatial_out.astype(jnp.float32)
    normed = modulated(running, modulation, 3)
    moved_rows = lax.all_to_all(normed, "seq", split_axis=2, concat_axis=1, tiled=True)
    packed = project_heads(
        lax.all_gather(moved_rows, "tp", axis=2, tiled=True), qkv_temporal, gain_temporal, head_dim
    )
    mixed_heads = frame_attention(packed[0], packed[1], packed[2], head_dim)
    partial_value = jnp.einsum(
        "bfpe,ed->bfpd", mixed_heads, out_temporal, preferred_element_type=jnp.float32
    )
    shares = lax.psum_scatter(
        partial_value.astype(jnp.bfloat16), "tp", scatter_dimension=2, tiled=True
    )
    temporal_out = lax.all_to_all(shares, "seq", split_axis=1, concat_axis=2, tiled=True)
    running = running + modulation[:, 5][:, None, None, :] * temporal_out.astype(jnp.float32)
    normed = modulated(running, modulation, 6)
    projected = jnp.einsum(
        "bfpd,de->bfpe",
        lax.all_gather(normed, "tp", axis=2, tiled=True),
        fc_in,
        preferred_element_type=jnp.float32,
    )
    hidden = jax.nn.gelu(projected, approximate=True).astype(jnp.bfloat16)
    partial_value = jnp.einsum("bfpe,ed->bfpd", hidden, fc_out, preferred_element_type=jnp.float32)
    mlp_out = lax.psum_scatter(
        partial_value.astype(jnp.bfloat16), "tp", scatter_dimension=2, tiled=True
    )
    return (running + modulation[:, 8][:, None, None, :] * mlp_out.astype(jnp.float32)).astype(
        jnp.bfloat16
    )


def fits(mesh, videos, local_frames, local_rows, heads_here):
    return (
        mesh.shape["tp"] == 2
        and videos == 2
        and local_frames == 1
        and local_rows % (8 * mesh.shape["seq"]) == 0
        and heads_here % 2 == 0
    )


def solution(mesh):
    placed = (
        P(None, "seq", "tp", None),
        P(),
        P(None, None, "tp"),
        P(),
        P("tp", None),
        P(None, None, "tp"),
        P(),
        P("tp", None),
        P(None, "tp"),
        P("tp", None),
    )

    def step(*args):
        latent, qkv, gain = args[0], args[2], args[3]
        if fits(mesh, latent.shape[0], latent.shape[1], latent.shape[2], qkv.shape[2] // gain.shape[1]):
            return paired_body(mesh.shape["seq"], *args)
        return body(*args)

    return jax.shard_map(
        step, mesh=mesh, in_specs=placed, out_specs=P(None, "seq", "tp", None), check_vma=False
    )
```
